32 devices in a mesh: fsdp: 32 (over z, y, x, core).
Axes of the slice: x: 2, y: 2, z: 4, core: 2. Of those that a mesh axis runs over, the one named last changes fastest.
Arguments:
- hidden_in: bfloat16 [64, 320, 768], P('fsdp'), may hold values from -16 to 16
- encoder_states: bfloat16 [64, 128, 768], P('fsdp'), may hold values from -16 to 16
- lengths: int32 [64], P('fsdp'), may hold values from 60 to 320, as said below
- out_grad: bfloat16 [64, 320, 768], P('fsdp'), may hold values from -6 to 6
- attn_in: bfloat16 [6, 768, 768], P(None, 'fsdp'), may hold values from -0.21875 to 0.21875
- attn_out: bfloat16 [2, 768, 768], P(None, 'fsdp'), may hold values from -0.875 to 0.875
- fc_in: bfloat16 [768, 3072], P('fsdp'), may hold values from -0.21875 to 0.21875
- fc_out: bfloat16 [3072, 768], P('fsdp'), may hold values from -0.109375 to 0.109375
- gains: bfloat16 [3, 768], P(None, 'fsdp'), may hold values from 0.5 to 1.5
- biases: bfloat16 [10, 768], P(None, 'fsdp'), may hold values from -2 to 2
- ffn_bias: bfloat16 [3072], P('fsdp'), may hold values from -2 to 2
Outputs:
- layer_out: bfloat16 [64, 320, 768], P('fsdp')
- grad_in: bfloat16 [64, 320, 768], P('fsdp')
- grad_encoder: bfloat16 [64, 128, 768], P('fsdp')
- grad_attn_in: float32 [6, 768, 768], P(None, 'fsdp')
- grad_attn_out: float32 [2, 768, 768], P(None, 'fsdp')
- grad_fc_in: float32 [768, 3072], P('fsdp')
- grad_fc_out: float32 [3072, 768], P('fsdp')
- grad_gains: float32 [3, 768], P(None, 'fsdp')
- grad_biases: float32 [10, 768], P(None, 'fsdp')
- grad_ffn_bias: float32 [3072], P('fsdp')
- rms: float32 [4], replicated
The draws below stay inside these ranges and needn't reach their ends.
Inputs may be any that keep to these rules, and one draw needn't show every extreme that they name: `lengths`: each transcript has 60 to 320 valid tokens, its first ones; some transcript has exactly 320.
All inputs are finite; a program needn't handle non-finite values.
Results may differ from the reference program's by a relative error of at most 0.017.
Values may be sent and summed in bfloat16 or wider, within the bound.
No kernel may reach another device: no remote copies, remote signals or barrier semaphores. Data moves between devices by JAX's collectives and lax.ppermute only.
A program may use at most 256 MiB of HBM per device.

```python
import math
import jax
import jax.numpy as jnp
from jax import lax

D = 768
HEADS = 12
FF = 3072
HEAD_FEATURES = 64
LEN = 320
MIN_LEN = 60
FRAMES = 128
SEQS = 64


def sequence_scale(key, count):
    trend = 0.6 * 3.0 ** (jnp.arange(count, dtype=jnp.float32) / max(count - 1, 1))
    wobble = jnp.exp(jax.random.uniform(key, (count,), jnp.float32, -0.2, 0.2))
    return trend * wobble


def scaled_rows(key, rows):
    scales = sequence_scale(jax.random.fold_in(key, 11), SEQS)
    base = jax.random.normal(jax.random.fold_in(key, 12), (SEQS, rows, D), jnp.float32)
    return (base * scales[:, None, None]).astype(jnp.bfloat16)


def draw_hidden_in(key, part):
    return scaled_rows(jax.random.fold_in(key, 1), LEN)


def draw_encoder_states(key, part):
    return scaled_rows(jax.random.fold_in(key, 2), FRAMES)


def draw_lengths(key, part):
    raw_counts = jax.random.randint(jax.random.fold_in(key, 3), (SEQS,), MIN_LEN, LEN + 1, jnp.int32)
    chosen = jax.random.randint(jax.random.fold_in(key, 4), (), 0, SEQS, jnp.int32)
    return jnp.where(jnp.arange(SEQS, dtype=jnp.int32) == chosen, LEN, raw_counts).astype(jnp.int32)


def block_scale(key, shape, cuts, least, top_value):
    loudness = 1.0
    for position, shards_of in cuts:
        draws = jax.random.uniform(jax.random.fold_in(jax.random.fold_in(key, 6), position), (shards_of,), jnp.float32, least / len(cuts), top_value / len(cuts))
        loudness = loudness * jnp.repeat(jnp.exp(draws), shape[position] // shards_of).reshape((-1,) + (1,) * (len(shape) - 1 - position))
    return loudness


def centred(stream_key, dims, width, bound, shards=(), kind=jnp.bfloat16):
    values = width * jax.random.normal(stream_key, dims, jnp.float32)
    if shards:
        values = values * block_scale(stream_key, dims, shards, -0.22, 0.18)
    return jnp.clip(values, -bound, bound).astype(kind)


def setup_inputs(seed: int = 0) -> dict:
    splits = jax.random.split(jax.random.key(seed), 12)
    hidden_in = draw_hidden_in(jax.random.fold_in(splits[11], 71), 0)
    encoder_states = draw_encoder_states(jax.random.fold_in(splits[11], 71), 0)
    lengths = draw_lengths(jax.random.fold_in(splits[11], 71), 0)
    out_grad = centred(splits[3], (SEQS, LEN, D), 1.0, 6.0, ((0, 32),))
    attn_in = centred(splits[4], (6, D, D), D ** -0.5, 0.21875, ((1, 32),))
    attn_out = centred(splits[5], (2, D, D), (D // 16) ** -0.5, 0.875, ((1, 32),))
    fc_in = centred(splits[6], (D, FF), D ** -0.5, 0.21875, ((0, 32),))
    fc_out = centred(splits[7], (FF, D), FF ** -0.5, 0.109375, ((0, 32),))
    gains = jnp.clip(1.0 + 0.1 * jax.random.normal(splits[8], (3, D), jnp.float32), 0.5, 1.5).astype(jnp.bfloat16)
    biases = centred(splits[9], (10, D), 0.3, 2.0, ((1, 32),))
    ffn_bias = centred(splits[10], (FF,), 0.3, 2.0, ((0, 32),))
    return dict(hidden_in=hidden_in, encoder_states=encoder_states, lengths=lengths, out_grad=out_grad, attn_in=attn_in, attn_out=attn_out, fc_in=fc_in, fc_out=fc_out, gains=gains, biases=biases, ffn_bias=ffn_bias)


@jax.custom_vjp
def low(v):
    return lax.optimization_barrier(v.astype(jnp.bfloat16)).astype(jnp.float32)

@jax.custom_vjp
def low_back(v):
    return v

def low_keep(v):
    return (low(v), None)

def low_pass(kept, grad):
    return (grad,)

def back_keep(v):
    return (v, None)

def back_low(kept, grad):
    return (low(grad),)
low.defvjp(low_keep, low_pass)
low_back.defvjp(back_keep, back_low)
norm_eps = 1e-05
masked_score = -1e+30
highest_mode = lax.Precision.HIGHEST

def layer_norm(inputs, gain_row, shift_row):
    center = inputs - lax.optimization_barrier(jnp.mean(inputs, -1, keepdims=True))
    spread = lax.optimization_barrier(jnp.mean(center * center, -1, keepdims=True))
    return center * lax.rsqrt(spread + norm_eps) * gain_row + shift_row

def project(left, right):
    return jnp.dot(left, right, precision=highest_mode)

def attend(query_matrix, key_matrix, value_matrix, causal):
    length = query_matrix.shape[0]
    frames = key_matrix.shape[0]
    per_head_queries = query_matrix.reshape(length, HEADS, HEAD_FEATURES)
    per_head_keys = key_matrix.reshape(frames, HEADS, HEAD_FEATURES)
    per_head_values = value_matrix.reshape(frames, HEADS, HEAD_FEATURES)
    logit_scores = jnp.einsum('sxc,oxc->xso', per_head_queries, per_head_keys, precision=highest_mode) * (1.0 / math.sqrt(HEAD_FEATURES))
    logit_scores = low_back(logit_scores)
    if causal:
        allowed = jnp.arange(frames)[None, :] <= jnp.arange(length)[:, None]
        logit_scores = jnp.where(allowed[None], logit_scores, masked_score)
    attention_weight = low(jax.nn.softmax(logit_scores, axis=-1))
    attended_rows = jnp.einsum('opi,ioz->poz', attention_weight, per_head_values, precision=highest_mode)
    return attended_rows.reshape(length, HEADS * HEAD_FEATURES)

def decoder_layer(stream, frames_in, attn_in, attn_out, fc_in, fc_out, gains, biases, ffn_bias):
    norm_one = low(layer_norm(stream, gains[0], biases[7]))
    query_matrix = low_back(low(project(norm_one, attn_in[0]) + biases[0]))
    key_matrix = low_back(low(project(norm_one, attn_in[1])))
    value_matrix = low_back(low(project(norm_one, attn_in[2]) + biases[1]))
    attended_rows = low_back(low(attend(query_matrix, key_matrix, value_matrix, True)))
    self_out = low_back(project(attended_rows, attn_out[0]) + biases[2])
    stream_mid = stream + self_out
    norm_two = low(layer_norm(stream_mid, gains[1], biases[8]))
    cross_query = low_back(low(project(norm_two, attn_in[3]) + biases[3]))
    cross_key = low_back(low(project(frames_in, attn_in[4])))
    cross_value = low_back(low(project(frames_in, attn_in[5]) + biases[4]))
    cross_attended = low_back(low(attend(cross_query, cross_key, cross_value, False)))
    cross_out = low_back(project(cross_attended, attn_out[1]) + biases[5])
    stream_late = stream_mid + cross_out
    norm_three = low(layer_norm(stream_late, gains[2], biases[9]))
    ffn_input = low_back(project(norm_three, fc_in) + ffn_bias)
    ffn_hidden = low(jax.nn.gelu(ffn_input, approximate=False))
    ffn_out = low_back(project(ffn_hidden, fc_out) + biases[6])
    result = stream_late + ffn_out
    return (result, (self_out, cross_out, ffn_out))

def reference(hidden_in, encoder_states, lengths, out_grad, attn_in, attn_out, fc_in, fc_out, gains, biases, ffn_bias):
    weights_f32 = tuple((w.astype(jnp.float32) for w in (attn_in, attn_out, fc_in, fc_out, gains, biases, ffn_bias)))
    group_size = 8
    group_count = SEQS // group_size

    def shaped(array):
        return array.reshape((group_count, group_size) + array.shape[1:])

    def per_sequence(stream, frames_in, valid_count, cotangent):
        stream = stream.astype(jnp.float32)
        frames_in = frames_in.astype(jnp.float32)
        valid_rows = (jnp.arange(LEN) < valid_count).astype(jnp.float32)[:, None]
        result, pullback, branches = jax.vjp(decoder_layer, stream, frames_in, *weights_f32, has_aux=True)
        grad_terms = pullback(cotangent.astype(jnp.float32) * valid_rows)
        square_sums = jnp.stack([jnp.sum(valid_rows * result * result)] + [jnp.sum(valid_rows * branch * branch) for branch in branches])
        return (result.astype(jnp.bfloat16), grad_terms[0].astype(jnp.bfloat16), grad_terms[1].astype(jnp.bfloat16), grad_terms[2:], square_sums)

    def scan_step(carry, inputs):
        totals, square_sums = carry
        result, grad_stream, grad_frames, grad_terms, sums_now = jax.vmap(per_sequence)(*inputs)
        totals = tuple((total + lax.optimization_barrier(jnp.sum(term, 0)) for total, term in zip(totals, grad_terms)))
        return ((totals, square_sums + lax.optimization_barrier(jnp.sum(sums_now, 0))), (result, grad_stream, grad_frames))
    start = (tuple((jnp.zeros(w.shape, jnp.float32) for w in weights_f32)), jnp.zeros((4,), jnp.float32))
    (totals, square_sums), (results, grad_streams, grad_frames) = lax.scan(scan_step, start, (shaped(hidden_in), shaped(encoder_states), shaped(lengths), shaped(out_grad)))
    valid_total = jnp.sum(lengths).astype(jnp.float32)
    rms = jnp.sqrt(square_sums / (valid_total * D))
    return (results.reshape(SEQS, LEN, D), grad_streams.reshape(SEQS, LEN, D), grad_frames.reshape(SEQS, FRAMES, D), totals[0], totals[1], totals[2], totals[3], totals[4], totals[5], totals[6], rms)
```

```python
import functools
import math

import jax
import jax.numpy as jnp
from jax import lax
from jax.experimental import pallas as pl
from jax.experimental.pallas import tpu as pltpu
from jax.sharding import PartitionSpec as P

NORM_EPS = 1e-05
LOW = jnp.bfloat16
WIDE = jnp.float32
HEADS = 12
PAIR = 128
HALF_PAIR = 64
SCALE = 0.125


def dot_nn(left, right):
    return lax.dot_general(left, right, (((1,), (0,)), ((), ())), preferred_element_type=WIDE)


def dot_nt(left, right):
    return lax.dot_general(left, right, (((1,), (1,)), ((), ())), preferred_element_type=WIDE)


def dot_tn(left, right):
    return lax.dot_general(left, right, (((0,), (0,)), ((), ())), preferred_element_type=WIDE)


def spec(block, index, once=False):
    if once:
        return pl.BlockSpec(block, index, pipeline_mode=pl.Buffered(1))
    return pl.BlockSpec(block, index)


def run(body, name, grid, operands, in_specs, outs, scratch=(), flops=0, exps=0, limit=40):
    moved = sum(o.size * o.dtype.itemsize for o in operands)
    moved += sum(math.prod(s) * jnp.dtype(d).itemsize for s, d, _ in outs)
    return pl.pallas_call(
        body,
        name=name,
        grid=grid,
        in_specs=in_specs,
        out_specs=[o[2] for o in outs],
        out_shape=[jax.ShapeDtypeStruct(o[0], o[1]) for o in outs],
        scratch_shapes=list(scratch),
        compiler_params=pltpu.CompilerParams(
            dimension_semantics=("arbitrary",) * len(grid), vmem_limit_bytes=limit << 20
        ),
        cost_estimate=pl.CostEstimate(flops=flops, transcendentals=exps, bytes_accessed=moved),
    )(*operands)


def normalised(values):
    center = values - jnp.mean(values, -1, keepdims=True)
    spread = jnp.mean(center * center, -1, keepdims=True)
    scale = lax.rsqrt(spread + NORM_EPS)
    return center * scale, scale


def norm_backward(values, grad, gain):
    unit, scale = normalised(values)
    inner = grad * gain
    mean_inner = jnp.mean(inner, -1, keepdims=True)
    mean_unit = jnp.mean(inner * unit, -1, keepdims=True)
    return scale * (inner - mean_inner - unit * mean_unit), grad * unit


def col_sum(values):
    return jnp.sum(values.astype(WIDE), 0, keepdims=True)


def add_rows(ref, first, rows):
    @pl.when(first)
    def _():
        ref[...] = jnp.zeros_like(ref)

    for place, row in enumerate(rows):
        ref[place : place + 1, :] += row


def masked_squares(values, length_ref, step, per_seq):
    rows = values.shape[0]
    start = (step % per_seq) * rows
    index = start + lax.broadcasted_iota(jnp.int32, (rows, 1), 0)
    inside = index < length_ref[step // per_seq]
    return col_sum(jnp.where(inside, values * values, 0.0))


def qkv_body(x_ref, vec_ref, wq, wk, wv, n_ref, q_ref, k_ref, v_ref):
    unit, _ = normalised(x_ref[...].astype(WIDE))
    norm = (unit * vec_ref[0:1, :] + vec_ref[10:11, :]).astype(LOW)
    n_ref[...] = norm
    query = (dot_nn(norm, wq[0]) + vec_ref[3:4, :]).astype(LOW)
    q_ref[...] = query * jnp.asarray(SCALE, LOW)
    k_ref[...] = dot_nn(norm, wk[0]).astype(LOW)
    v_ref[...] = (dot_nn(norm, wv[0]) + vec_ref[4:5, :]).astype(LOW)


def whole(shape):
    return spec(shape, lambda *_: (0,) * len(shape), once=True)


def qkv(x, vec, self_a, self_b, block):
    rows, width = x.shape
    row = lambda i: (i, 0)
    weight = lambda which: spec((1, width, width), lambda i: (which, 0, 0), once=True)
    return run(
        qkv_body,
        "qkv",
        (rows // block,),
        (x, vec, self_a, self_a, self_b),
        [spec((block, width), row), whole(vec.shape), weight(0), weight(1), weight(0)],
        [((rows, width), LOW, spec((block, width), row))] * 4,
        flops=6 * rows * width * width,
    )


def head_lanes(values, head):
    lane = lax.broadcasted_iota(jnp.int32, (1, PAIR), 1)
    inside = lane < HALF_PAIR if head == 0 else lane >= HALF_PAIR
    return jnp.where(inside, values, jnp.zeros_like(values))


def attend_body(causal, pairs, step_rows, q_ref, k_ref, v_ref, o_ref):
    length = q_ref.shape[0]
    frames = k_ref.shape[0]
    for pair in range(pairs):
        lanes = slice(pair * PAIR, (pair + 1) * PAIR)
        values = v_ref[:, lanes]
        by_head = [head_lanes(values, head) for head in (0, 1)]
        for start in range(0, length, step_rows):
            stop = min(start + step_rows, length)
            seen = stop if causal else frames
            keys = k_ref[0:seen, lanes]
            queries = q_ref[start:stop, lanes]
            total = None
            for head in (0, 1):
                scores = dot_nt(head_lanes(queries, head), keys)
                if causal:
                    shape = scores.shape
                    key_at = lax.broadcasted_iota(jnp.int32, shape, 1)
                    query_at = lax.broadcasted_iota(jnp.int32, shape, 0) + start
                    scores = jnp.where(key_at <= query_at, scores, -1e30)
                top = jnp.max(scores, -1, keepdims=True)
                exps = jnp.exp(scores - top)
                probs = exps * (1.0 / jnp.sum(exps, -1, keepdims=True))
                part = dot_nn(probs.astype(LOW), by_head[head][0:seen])
                total = part if total is None else total + part
            o_ref[start:stop, lanes] = total.astype(LOW)


def attend(q, k, v, batch, causal, pairs=2, step_rows=128):
    rows, width = q.shape
    length, frames = rows // batch, k.shape[0] // batch
    lanes = pairs * PAIR
    at = lambda b, p: (b, p)
    return run(
        functools.partial(attend_body, causal, pairs, step_rows),
        "attend_self" if causal else "attend_cross",
        (batch, width // lanes),
        (q, k, v),
        [spec((length, lanes), at), spec((frames, lanes), at), spec((frames, lanes), at)],
        [((rows, width), LOW, spec((length, lanes), at))],
        flops=4 * rows * frames * width,
        exps=rows * frames * HEADS,
    )[0]


def attend_back_body(causal, pairs, step_rows, q_ref, k_ref, v_ref, g_ref, gq_ref, gk_ref, gv_ref, dk, dv):
    length = q_ref.shape[0]
    frames = k_ref.shape[0]
    for pair in range(pairs):
        lanes = slice(pair * PAIR, (pair + 1) * PAIR)
        for start in range(0, length, step_rows):
            stop = min(start + step_rows, length)
            seen = stop if causal else frames
            keys = k_ref[0:seen, lanes]
            values = v_ref[0:seen, lanes]
            queries = q_ref[start:stop, lanes]
            grads = g_ref[start:stop, lanes]
            grad_q = grad_k = grad_v = None
            for head in (0, 1):
                head_keys = head_lanes(keys, head)
                scores = dot_nt(head_keys, queries)
                if causal:
                    shape = scores.shape
                    key_at = lax.broadcasted_iota(jnp.int32, shape, 0)
                    query_at = lax.broadcasted_iota(jnp.int32, shape, 1) + start
                    scores = jnp.where(key_at <= query_at, scores, -1e30)
                top = jnp.max(scores, 0, keepdims=True)
                exps = jnp.exp(scores - top)
                probs = exps * (1.0 / jnp.sum(exps, 0, keepdims=True))
                grad_probs = dot_nt(head_lanes(values, head), grads)
                weighted = probs * grad_probs
                inner = jnp.sum(weighted, 0, keepdims=True)
                grad_scores = (weighted - probs * inner).astype(LOW)
                part_v = dot_nn(probs.astype(LOW), head_lanes(grads, head))
                part_k = dot_nn(grad_scores, head_lanes(queries, head))
                part_q = dot_tn(grad_scores, head_keys)
                grad_v = part_v if grad_v is None else grad_v + part_v
                grad_k = part_k if grad_k is None else grad_k + part_k
                grad_q = part_q if grad_q is None else grad_q + part_q
            gq_ref[start:stop, lanes] = (grad_q * SCALE).astype(LOW)
            if causal:
                old = 0 if start == 0 else start
                if old:
                    dk[0:old, :] += grad_k[0:old]
                    dv[0:old, :] += grad_v[0:old]
                dk[old:seen, :] = grad_k[old:]
                dv[old:seen, :] = grad_v[old:]
            elif start == 0:
                dk[...] = grad_k
                dv[...] = grad_v
            else:
                dk[...] += grad_k
                dv[...] += grad_v
        gk_ref[:, lanes] = dk[...].astype(LOW)
        gv_ref[:, lanes] = dv[...].astype(LOW)


def attend_back(q, k, v, grad, batch, causal, pairs=2, step_rows=128):
    rows, width = q.shape
    length, frames = rows // batch, k.shape[0] // batch
    lanes = pairs * PAIR
    at = lambda b, p: (b, p)
    long, short = spec((length, lanes), at), spec((frames, lanes), at)
    return run(
        functools.partial(attend_back_body, causal, pairs, step_rows),
        "attend_self_back" if causal else "attend_cross_back",
        (batch, width // lanes),
        (q, k, v, grad),
        [long, short, short, long],
        [((rows, width), LOW, long), (k.shape, LOW, short), (k.shape, LOW, short)],
        [pltpu.VMEM((frames, PAIR), WIDE)] * 2,
        flops=10 * rows * frames * width,
        exps=rows * frames * HEADS,
    )


def mid_body(per_seq, len_ref, a_ref, x_ref, vec_ref, wo, wq, mid_ref, n_ref, q_ref, s_ref):
    step = pl.program_id(0)
    branch = dot_nn(a_ref[...], wo[0]) + vec_ref[5:6, :]
    mid = x_ref[...].astype(WIDE) + branch
    mid_ref[...] = mid
    unit, _ = normalised(mid)
    norm = (unit * vec_ref[1:2, :] + vec_ref[11:12, :]).astype(LOW)
    n_ref[...] = norm
    query = (dot_nn(norm, wq[0]) + vec_ref[6:7, :]).astype(LOW)
    q_ref[...] = query * jnp.asarray(SCALE, LOW)
    add_rows(s_ref, step == 0, [masked_squares(branch, len_ref, step, per_seq)])


def smem():
    return pl.BlockSpec(memory_space=pltpu.SMEM)


def mid_stage(lengths, attended, x, vec, self_b, cross_a, batch, block):
    rows, width = x.shape
    row = lambda i: (i, 0)
    weight = lambda which: spec((1, width, width), lambda i: (which, 0, 0), once=True)
    tile = spec((block, width), row)
    return run(
        functools.partial(mid_body, rows // batch // block),
        "mid_stage",
        (rows // block,),
        (lengths, attended, x, vec, self_b, cross_a),
        [smem(), tile, tile, whole(vec.shape), weight(1), weight(0)],
        [
            ((rows, width), WIDE, tile),
            ((rows, width), LOW, tile),
            ((rows, width), LOW, tile),
            ((8, width), WIDE, spec((8, width), lambda i: (0, 0))),
        ],
        flops=4 * rows * width * width,
    )


def frames_body(f_ref, vec_ref, wk, wv, k_ref, v_ref):
    frames = f_ref[...]
    k_ref[...] = dot_nn(frames, wk[0]).astype(LOW)
    v_ref[...] = (dot_nn(frames, wv[0]) + vec_ref[7:8, :]).astype(LOW)


def frames_stage(frames, vec, cross_b, block):
    rows, width = frames.shape
    tile = spec((block, width), lambda i: (i, 0))
    weight = lambda which: spec((1, width, width), lambda i: (which, 0, 0), once=True)
    return run(
        frames_body,
        "frames_stage",
        (rows // block,),
        (frames, vec, cross_b, cross_b),
        [tile, whole(vec.shape), weight(0), weight(1)],
        [((rows, width), LOW, tile)] * 2,
        flops=4 * rows * width * width,
    )


def late_body(per_seq, len_ref, a_ref, mid_ref, vec_ref, wo, late_ref, n_ref, s_ref):
    step = pl.program_id(0)
    branch = dot_nn(a_ref[...], wo[0]) + vec_ref[8:9, :]
    late = mid_ref[...] + branch
    late_ref[...] = late
    unit, _ = normalised(late)
    n_ref[...] = (unit * vec_ref[2:3, :] + vec_ref[12:13, :]).astype(LOW)
    add_rows(s_ref, step == 0, [masked_squares(branch, len_ref, step, per_seq)])


def late_stage(lengths, attended, mid, vec, cross_a, batch, block):
    rows, width = mid.shape
    tile = spec((block, width), lambda i: (i, 0))
    return run(
        functools.partial(late_body, rows // batch // block),
        "late_stage",
        (rows // block,),
        (lengths, attended, mid, vec, cross_a),
        [smem(), tile, tile, whole(vec.shape), spec((1, width, width), lambda i: (1, 0, 0), once=True)],
        [
            ((rows, width), WIDE, tile),
            ((rows, width), LOW, tile),
            ((8, width), WIDE, spec((8, width), lambda i: (0, 0))),
        ],
        flops=2 * rows * width * width,
    )


def ffn_in_body(n_ref, b_ref, w_ref, h_ref, d_ref):
    pre = dot_nn(n_ref[...], w_ref[0]) + b_ref[0]
    below = 0.5 + 0.5 * lax.erf(pre * (0.5**0.5))
    density = jnp.exp(-0.5 * pre * pre) * (1.0 / math.sqrt(2.0 * math.pi))
    h_ref[...] = (pre * below).astype(LOW)
    d_ref[...] = (below + pre * density).astype(LOW)


def ffn_in(norm, bias, weight, block):
    rows, width = norm.shape
    mats = weight.shape[0]
    tile = spec((block, width), lambda j, i: (i, j))
    return run(
        ffn_in_body,
        "ffn_in",
        (mats, rows // block),
        (norm, bias, weight),
        [
            spec((block, width), lambda j, i: (i, 0)),
            spec((1, 1, width), lambda j, i: (j, 0, 0)),
            spec((1, width, width), lambda j, i: (j, 0, 0)),
        ],
        [((rows, mats * width), LOW, tile)] * 2,
        flops=2 * rows * width * width * mats,
        exps=2 * rows * width * mats,
    )


def ffn_out_body(per_seq, len_ref, ha, hb, late_ref, vec_ref, oa, ob, r_ref, s_ref):
    step = pl.program_id(0)
    parts = [dot_nn(ha[...], w[0]) + dot_nn(hb[...], w[1]) for w in (oa, ob)]
    branch = jnp.concatenate(parts, -1) + vec_ref[9:10, :]
    result = late_ref[...] + branch
    r_ref[...] = result.astype(LOW)
    sums = [masked_squares(v, len_ref, step, per_seq) for v in (result, branch)]
    add_rows(s_ref, step == 0, sums)


def ffn_out(lengths, ha, hb, late, vec, out_a, out_b, batch, block):
    rows, width = late.shape
    inner = ha.shape[1]
    half = out_a.shape[2]
    tile = spec((block, width), lambda i: (i, 0))
    wide = spec((block, inner), lambda i: (i, 0))
    return run(
        functools.partial(ffn_out_body, rows // batch // block),
        "ffn_out",
        (rows // block,),
        (lengths, ha, hb, late, vec, out_a, out_b),
        [smem(), wide, wide, tile, whole(vec.shape), whole((2, inner, half)), whole((2, inner, half))],
        [((rows, width), LOW, tile), ((8, width), WIDE, spec((8, width), lambda i: (0, 0)))],
        flops=8 * rows * inner * half,
    )


def d_out_body(ha, hb, g_ref, da, db, s_ref):
    half = da.shape[2]
    grad = g_ref[...]
    for place, hidden in enumerate((ha, hb)):
        part = dot_tn(hidden[...], grad)
        da[place] = part[:, :half].astype(LOW)
        db[place] = part[:, half:].astype(LOW)
    add_rows(s_ref, pl.program_id(0) == 0, [])

    @pl.when(pl.program_id(0) == 0)
    def _():
        s_ref[0:1, :] = col_sum(grad)


def d_out(ha, hb, grad, block):
    rows, inner = ha.shape
    width = grad.shape[1]
    half = width // 2
    tile = spec((rows, block), lambda j: (0, j))
    return run(
        d_out_body,
        "d_out",
        (inner // block,),
        (ha, hb, grad),
        [tile, tile, whole(grad.shape)],
        [((2, inner, half), LOW, spec((2, block, half), lambda j: (0, j, 0)))] * 2
        + [((8, width), WIDE, spec((8, width), lambda j: (0, 0)))],
        flops=4 * rows * inner * width,
    )


def ffn_back_body(g_ref, d_ref, oa, ob, n_ref, p_ref, dw_ref, s_ref):
    half = oa.shape[2]
    grad = dot_nt(g_ref[:, :half], oa[0]) + dot_nt(g_ref[:, half:], ob[0])
    pre = (grad * d_ref[...].astype(WIDE)).astype(LOW)
    p_ref[...] = pre
    s_ref[0] = col_sum(pre)
    dw_ref[0] = dot_tn(n_ref[...], pre).astype(LOW)


def ffn_back(grad, slope, out_a, out_b, norm, which, width_step):
    rows, inner = slope.shape
    width = grad.shape[1]
    half = out_a.shape[2]
    steps = inner // width_step
    per = width // width_step
    assert per * width_step == width
    weight = spec((1, width_step, half), lambda j: (which, j, 0))
    tile = spec((rows, width_step), lambda j: (0, j))
    return run(
        ffn_back_body,
        "ffn_back",
        (steps,),
        (grad, slope, out_a, out_b, norm),
        [whole(grad.shape), tile, weight, weight, whole(norm.shape)],
        [
            ((rows, inner), LOW, tile),
            ((inner // width, width, width), LOW, spec((1, width, width_step), lambda j: (j // per, 0, j % per))),
            ((steps, 1, width_step), WIDE, spec((1, 1, width_step), lambda j: (j, 0, 0))),
        ],
        flops=4 * rows * inner * width,
    )


def late_back_body(pa, pb, wa, wb, late_ref, og_ref, vec_ref, wo, gl_ref, gc_ref, ga_ref, s_ref):
    width = wa.shape[1]
    grad = None
    for pre, weight in ((pa, wa), (pb, wb)):
        for mat in range(weight.shape[0]):
            part = dot_nt(pre[:, mat * width : (mat + 1) * width], weight[mat])
            grad = part if grad is None else grad + part
    through, for_gain = norm_backward(late_ref[...], grad, vec_ref[2:3, :])
    total = og_ref[...].astype(WIDE) + through
    gl_ref[...] = total
    low = total.astype(LOW)
    gc_ref[...] = low
    ga_ref[...] = dot_nt(low, wo[0]).astype(LOW)
    add_rows(s_ref, pl.program_id(0) == 0, [col_sum(for_gain), col_sum(grad), col_sum(low)])


def late_back(pa, pb, in_a, in_b, late, grad, vec, cross_a, block):
    rows, width = late.shape
    inner = pa.shape[1]
    tile = spec((block, width), lambda i: (i, 0))
    wide = spec((block, inner), lambda i: (i, 0))
    return run(
        late_back_body,
        "late_back",
        (rows // block,),
        (pa, pb, in_a, in_b, late, grad, vec, cross_a),
        [
            wide,
            wide,
            whole(in_a.shape),
            whole(in_b.shape),
            tile,
            tile,
            whole(vec.shape),
            spec((1, width, width), lambda i: (1, 0, 0), once=True),
        ],
        [
            ((rows, width), WIDE, tile),
            ((rows, width), LOW, tile),
            ((rows, width), LOW, tile),
            ((8, width), WIDE, spec((8, width), lambda i: (0, 0))),
        ],
        flops=4 * rows * inner * width + 2 * rows * width * width,
    )


def weights_body(count, *refs):
    out = refs[-1]
    for place in range(count):
        out[place] = dot_tn(refs[2 * place][...], refs[2 * place + 1][...]).astype(LOW)


def weight_grads(pairs, block):
    width = pairs[0][0].shape[1]
    operands, specs = [], []
    for left, right in pairs:
        operands += [left, right]
        specs += [spec((left.shape[0], block), lambda j: (0, j)), whole(right.shape)]
    return run(
        functools.partial(weights_body, len(pairs)),
        "weight_grads",
        (width // block,),
        tuple(operands),
        specs,
        [((len(pairs), width, width), LOW, spec((len(pairs), block, width), lambda j: (0, j, 0)))],
        flops=sum(2 * left.shape[0] * width * width for left, _ in pairs),
    )[0]


def mid_back_body(gq, wq, mid_ref, gl_ref, vec_ref, wo, gm_ref, gs_ref, ga_ref, s_ref):
    query = gq[...]
    grad = dot_nt(query, wq[0])
    through, for_gain = norm_backward(mid_ref[...], grad, vec_ref[1:2, :])
    total = gl_ref[...] + through
    gm_ref[...] = total
    low = total.astype(LOW)
    gs_ref[...] = low
    ga_ref[...] = dot_nt(low, wo[0]).astype(LOW)
    add_rows(
        s_ref,
        pl.program_id(0) == 0,
        [col_sum(for_gain), col_sum(grad), col_sum(low), col_sum(query)],
    )


def mid_back(grad_q, cross_a, mid, grad_late, vec, self_b, block):
    rows, width = mid.shape
    tile = spec((block, width), lambda i: (i, 0))
    weight = lambda which: spec((1, width, width), lambda i: (which, 0, 0), once=True)
    return run(
        mid_back_body,
        "mid_back",
        (rows // block,),
        (grad_q, cross_a, mid, grad_late, vec, self_b),
        [tile, weight(0), tile, tile, whole(vec.shape), weight(1)],
        [
            ((rows, width), WIDE, tile),
            ((rows, width), LOW, tile),
            ((rows, width), LOW, tile),
            ((8, width), WIDE, spec((8, width), lambda i: (0, 0))),
        ],
        flops=4 * rows * width * width,
    )


def frames_back_body(gk, gv, wk, wv, ge_ref, s_ref):
    grad_v = gv[...]
    ge_ref[...] = (dot_nt(gk[...], wk[0]) + dot_nt(grad_v, wv[0])).astype(LOW)
    add_rows(s_ref, pl.program_id(0) == 0, [col_sum(grad_v)])


def frames_back(grad_k, grad_v, cross_b, block):
    rows, width = grad_k.shape
    tile = spec((block, width), lambda i: (i, 0))
    weight = lambda which: spec((1, width, width), lambda i: (which, 0, 0), once=True)
    return run(
        frames_back_body,
        "frames_back",
        (rows // block,),
        (grad_k, grad_v, cross_b, cross_b),
        [tile, tile, weight(0), weight(1)],
        [((rows, width), LOW, tile), ((8, width), WIDE, spec((8, width), lambda i: (0, 0)))],
        flops=4 * rows * width * width,
    )


def in_back_body(gq, gk, gv, wq, wk, wv, x_ref, gm_ref, vec_ref, gi_ref, s_ref):
    query, value = gq[...], gv[...]
    grad = dot_nt(query, wq[0]) + dot_nt(gk[...], wk[0]) + dot_nt(value, wv[0])
    through, for_gain = norm_backward(x_ref[...].astype(WIDE), grad, vec_ref[0:1, :])
    gi_ref[...] = (gm_ref[...] + through).astype(LOW)
    add_rows(
        s_ref,
        pl.program_id(0) == 0,
        [col_sum(for_gain), col_sum(grad), col_sum(query), col_sum(value)],
    )


def in_back(grad_q, grad_k, grad_v, self_a, self_b, x, grad_mid, vec, block):
    rows, width = x.shape
    tile = spec((block, width), lambda i: (i, 0))
    weight = lambda which: spec((1, width, width), lambda i: (which, 0, 0), once=True)
    return run(
        in_back_body,
        "in_back",
        (rows // block,),
        (grad_q, grad_k, grad_v, self_a, self_a, self_b, x, grad_mid, vec),
        [tile, tile, tile, weight(0), weight(1), weight(0), tile, tile, whole(vec.shape)],
        [((rows, width), LOW, tile), ((8, width), WIDE, spec((8, width), lambda i: (0, 0)))],
        flops=6 * rows * width * width,
    )


def layer(vec, ffn_bias, weights, x, frames, lengths, grad, batch):
    self_a, self_b, cross_a, cross_b, in_a, in_b, out_a, out_b = weights
    rows, width = x.shape
    block = rows // batch // 2
    inner = in_a.shape[0] * width
    half = width // 2
    out_a, out_b = (w.reshape(2, inner, half) for w in (out_a, out_b))
    norm_one, query, key, value = qkv(x, vec, self_a, self_b, block)
    attended = attend(query, key, value, batch, True)
    mid, norm_two, cross_q, square_self = mid_stage(lengths, attended, x, vec, self_b, cross_a, batch, block)
    cross_k, cross_v = frames_stage(frames, vec, cross_b, frames.shape[0] // batch)
    cross_attended = attend(cross_q, cross_k, cross_v, batch, False)
    late, norm_three, square_cross = late_stage(lengths, cross_attended, mid, vec, cross_a, batch, block)
    hidden_a, slope_a = ffn_in(norm_three, ffn_bias[: in_a.shape[0]], in_a, block)
    hidden_b, slope_b = ffn_in(norm_three, ffn_bias[in_a.shape[0] :], in_b, block)
    d_out_a, d_out_b, sums_out = d_out(hidden_a, hidden_b, grad, width)
    result, square_rest = ffn_out(lengths, hidden_a, hidden_b, late, vec, out_a, out_b, batch, block)
    pre_a, d_in_a, sums_in_a = ffn_back(grad, slope_a, out_a, out_b, norm_three, 0, width)
    pre_b, d_in_b, sums_in_b = ffn_back(grad, slope_b, out_a, out_b, norm_three, 1, width)
    grad_late, grad_cross, grad_cross_att, sums_late = late_back(
        pre_a, pre_b, in_a, in_b, late, grad, vec, cross_a, block
    )
    grad_cq, grad_ck, grad_cv = attend_back(cross_q, cross_k, cross_v, grad_cross_att, batch, False)
    d_cross_a = weight_grads([(norm_two, grad_cq), (cross_attended, grad_cross)], width // 3)
    d_cross_b = weight_grads([(frames, grad_ck), (frames, grad_cv)], width // 3)
    grad_mid, grad_self, grad_att, sums_mid = mid_back(grad_cq, cross_a, mid, grad_late, vec, self_b, block)
    grad_frames, sums_frames = frames_back(grad_ck, grad_cv, cross_b, frames.shape[0] // batch)
    grad_q, grad_k, grad_v = attend_back(query, key, value, grad_att, batch, True)
    d_self_a = weight_grads([(norm_one, grad_q), (norm_one, grad_k)], width // 3)
    d_self_b = weight_grads([(norm_one, grad_v), (attended, grad_self)], width // 3)
    grad_in, sums_one = in_back(grad_q, grad_k, grad_v, self_a, self_b, x, grad_mid, vec, block)
    squares = jnp.stack([square_rest[0], square_self[0], square_cross[0], square_rest[1]])
    sum_rows = (
        [sums_one[0], sums_mid[0], sums_late[0]]
        + [sums_one[2], sums_one[3], sums_mid[2], sums_mid[3], sums_frames[0], sums_late[2], sums_out[0]]
        + [sums_one[1], sums_mid[1], sums_late[1]]
    )
    sums_ff = jnp.concatenate([sums_in_a, sums_in_b], 0).reshape(-1, width)
    grads = (d_self_a, d_self_b, d_cross_a, d_cross_b, d_in_a, d_in_b, d_out_a, d_out_b)
    return (result, grad_in, grad_frames), grads, jnp.concatenate([jnp.stack(sum_rows), sums_ff]), squares


def bit_orders(count):
    bits = count.bit_length() - 1
    assert 1 << bits == count
    each = (bits - 1) // 3
    x_bits = list(range(1, 1 + each))
    y_bits = list(range(1 + each, 1 + 2 * each))
    z_bits = list(range(1 + 2 * each, bits))
    return ([0] + x_bits + y_bits + z_bits, [0] + y_bits + x_bits + z_bits)


def swap(values, bit, count):
    return lax.ppermute(values, "fsdp", [(i, i ^ (1 << bit)) for i in range(count)])


def own_bit(bit):
    return (lax.axis_index("fsdp") >> bit) & 1


def gather_piece(piece, order, count):
    mats, rows, width = piece.shape
    bits = count.bit_length() - 1
    held = piece.reshape((mats,) + (1,) * bits + (rows, width))
    for bit in reversed(order):
        other = swap(held, bit, count)
        axis = 1 + (bits - 1 - bit)
        first = own_bit(bit) == 0
        held = jnp.where(
            first,
            jnp.concatenate([held, other], axis),
            jnp.concatenate([other, held], axis),
        )
    return held.reshape(mats, count * rows, width)


def scatter_piece(partial, order, count):
    mats, rows, width = partial.shape
    bits = count.bit_length() - 1
    rows = rows // count
    held = partial.reshape((mats,) + (2,) * bits + (rows, width))
    for step, bit in enumerate(order):
        axis = 1 + (bits - 1 - bit)
        mine = own_bit(bit)
        send = lax.dynamic_slice_in_dim(held, 1 - mine, 1, axis)
        keep = lax.dynamic_slice_in_dim(held, mine, 1, axis)
        other = swap(send, bit, count)
        held = keep.astype(jnp.float32) + other.astype(jnp.float32)
        if step < bits - 1:
            held = held.astype(partial.dtype)
    return held.reshape(mats, rows, width)


def sum_all(values, count):
    for bit in range(count.bit_length() - 1):
        values = values + swap(values, bit, count)
    return values


def shards(
    count,
    hidden_in,
    encoder_states,
    lengths,
    out_grad,
    attn_in,
    attn_out,
    fc_in,
    fc_out,
    gains,
    biases,
    ffn_bias,
):
    batch, length, width = hidden_in.shape
    half = width // 2
    order_a, order_b = bit_orders(count)
    share = gains.shape[1]
    small = jnp.concatenate([gains.reshape(-1), biases.reshape(-1), ffn_bias.reshape(-1)])
    small_count = small.shape[0]
    small_rows = -(-small_count // 128)
    small = jnp.pad(small, (0, small_rows * 128 - small_count)).reshape(1, small_rows, 128)
    small = gather_piece(small, order_a, count).reshape(count, small_rows * 128)
    vec = small[:, : 13 * share].reshape(count, 13, share).transpose(1, 0, 2).reshape(13, width)
    vec = jnp.pad(vec.astype(jnp.float32), ((0, 3), (0, 0)))
    ffn_bias_all = small[:, 13 * share : small_count].astype(jnp.float32).reshape(-1)
    ff = ffn_bias_all.shape[0]
    blocks = ff // width
    fc_in_blocks = fc_in.reshape(-1, blocks, width).transpose(1, 0, 2)
    self_a = gather_piece(attn_in[0:2], order_a, count)
    self_b = gather_piece(jnp.stack([attn_in[2], attn_out[0]]), order_b, count)
    cross_a = gather_piece(jnp.stack([attn_in[3], attn_out[1]]), order_a, count)
    cross_b = gather_piece(attn_in[4:6], order_b, count)
    in_a = gather_piece(fc_in_blocks[: blocks // 2], order_a, count)
    in_b = gather_piece(fc_in_blocks[blocks // 2 :], order_b, count)
    out_a = gather_piece(fc_out[None, :, :half], order_a, count)
    out_b = gather_piece(fc_out[None, :, half:], order_b, count)
    valid = jnp.arange(length)[None, :, None] < lengths[:, None, None]
    grad = jnp.where(valid, out_grad, jnp.zeros_like(out_grad))
    results, grads, rows, squares = layer(
        vec,
        ffn_bias_all.reshape(blocks, 1, width),
        (self_a, self_b, cross_a, cross_b, in_a, in_b, out_a, out_b),
        hidden_in.reshape(batch * length, width),
        encoder_states.reshape(-1, width),
        lengths,
        grad.reshape(batch * length, width),
        batch,
    )
    g_self_a, g_self_b, g_cross_a, g_cross_b, g_in_a, g_in_b, g_out_a, g_out_b = grads
    d_out_a = scatter_piece(g_out_a.reshape(1, ff, half), order_a, count)
    d_out_b = scatter_piece(g_out_b.reshape(1, ff, half), order_b, count)
    d_in_a = scatter_piece(g_in_a, order_a, count)
    d_in_b = scatter_piece(g_in_b, order_b, count)
    d_cross_a = scatter_piece(g_cross_a, order_a, count)
    d_cross_b = scatter_piece(g_cross_b, order_b, count)
    d_self_a = scatter_piece(g_self_a, order_a, count)
    d_self_b = scatter_piece(g_self_b, order_b, count)
    stats = jnp.concatenate([jnp.sum(squares, -1), jnp.sum(lengths).astype(jnp.float32)[None]])
    stats = jnp.pad(stats, (0, 123)).reshape(1, 128)
    stats = sum_all(stats, count)[0]
    rms = jnp.sqrt(stats[:4] / (stats[4] * width))
    rows = jnp.pad(rows, ((0, -rows.shape[0] % 8), (0, 0)))
    rows = sum_all(rows, count)
    me = lax.axis_index("fsdp")
    mine = lax.dynamic_slice_in_dim(rows[:13], me * share, share, 1)
    ff_share = ff // count
    mine_ff = lax.dynamic_slice_in_dim(rows[13 : 13 + blocks].reshape(-1), me * ff_share, ff_share)
    return (
        results[0].reshape(hidden_in.shape),
        results[1].reshape(hidden_in.shape),
        results[2].reshape(encoder_states.shape),
        jnp.stack([d_self_a[0], d_self_a[1], d_self_b[0], d_cross_a[0], d_cross_b[0], d_cross_b[1]]),
        jnp.stack([d_self_b[1], d_cross_a[1]]),
        jnp.concatenate([d_in_a, d_in_b]).transpose(1, 0, 2).reshape(-1, ff),
        jnp.concatenate([d_out_a[0], d_out_b[0]], 1),
        mine[:3],
        mine[3:13],
        mine_ff,
        rms,
    )


def solution(mesh):
    placed = (
        P("fsdp", None, None),
        P("fsdp", None, None),
        P("fsdp"),
        P("fsdp", None, None),
        P(None, "fsdp", None),
        P(None, "fsdp", None),
        P("fsdp", None),
        P("fsdp", None),
        P(None, "fsdp"),
        P(None, "fsdp"),
        P("fsdp"),
    )
    return jax.shard_map(
        functools.partial(shards, mesh.shape["fsdp"]),
        mesh=mesh,
        in_specs=placed,
        out_specs=(
            P("fsdp", None, None),
            P("fsdp", None, None),
            P("fsdp", None, None),
            P(None, "fsdp", None),
            P(None, "fsdp", None),
            P("fsdp", None),
            P("fsdp", None),
            P(None, "fsdp"),
            P(None, "fsdp"),
            P("fsdp"),
            P(),
        ),
        check_vma=False,
    )
```

```python
import functools
import math

import jax
import jax.numpy as jnp
from jax import lax
from jax.experimental import pallas as pl
from jax.experimental.pallas import tpu as pltpu
from jax.sharding import PartitionSpec as P

NORM_EPS = 1e-05
LOW = jnp.bfloat16
WIDE = jnp.float32
HEADS = 12
PAIR = 128
HALF_PAIR = 64
SCALE = 0.125


def dot_nn(left, right):
    return lax.dot_general(left, right, (((1,), (0,)), ((), ())), preferred_element_type=WIDE)


def dot_nt(left, right):
    return lax.dot_general(left, right, (((1,), (1,)), ((), ())), preferred_element_type=WIDE)


def dot_tn(left, right):
    return lax.dot_general(left, right, (((0,), (0,)), ((), ())), preferred_element_type=WIDE)


def spec(block, index, once=False):
    if once:
        return pl.BlockSpec(block, index, pipeline_mode=pl.Buffered(1))
    return pl.BlockSpec(block, index)


def run(body, name, grid, operands, in_specs, outs, scratch=(), flops=0, exps=0, limit=40):
    moved = sum(o.size * o.dtype.itemsize for o in operands)
    moved += sum(math.prod(s) * jnp.dtype(d).itemsize for s, d, _ in outs)
    return pl.pallas_call(
        body,
        name=name,
        grid=grid,
        in_specs=in_specs,
        out_specs=[o[2] for o in outs],
        out_shape=[jax.ShapeDtypeStruct(o[0], o[1]) for o in outs],
        scratch_shapes=list(scratch),
        compiler_params=pltpu.CompilerParams(
            dimension_semantics=("arbitrary",) * len(grid), vmem_limit_bytes=limit << 20
        ),
        cost_estimate=pl.CostEstimate(flops=flops, transcendentals=exps, bytes_accessed=moved),
    )(*operands)


def normalised(values):
    center = values - jnp.mean(values, -1, keepdims=True)
    spread = jnp.mean(center * center, -1, keepdims=True)
    scale = lax.rsqrt(spread + NORM_EPS)
    return center * scale, scale


def norm_backward(values, grad, gain):
    unit, scale = normalised(values)
    inner = grad * gain
    mean_inner = jnp.mean(inner, -1, keepdims=True)
    mean_unit = jnp.mean(inner * unit, -1, keepdims=True)
    return scale * (inner - mean_inner - unit * mean_unit), grad * unit


def col_sum(values):
    return jnp.sum(values.astype(WIDE), 0, keepdims=True)


def add_rows(ref, first, rows):
    @pl.when(first)
    def _():
        ref[...] = jnp.zeros_like(ref)

    for place, row in enumerate(rows):
        ref[place : place + 1, :] += row


def masked_squares(values, length_ref, step, per_seq):
    rows = values.shape[0]
    start = (step % per_seq) * rows
    index = start + lax.broadcasted_iota(jnp.int32, (rows, 1), 0)
    inside = index < length_ref[step // per_seq]
    return col_sum(jnp.where(inside, values * values, 0.0))


def qkv_body(x_ref, vec_ref, wq, wk, wv, n_ref, q_ref, k_ref, v_ref):
    unit, _ = normalised(x_ref[...].astype(WIDE))
    norm = (unit * vec_ref[0:1, :] + vec_ref[10:11, :]).astype(LOW)
    n_ref[...] = norm
    query = (dot_nn(norm, wq[0]) + vec_ref[3:4, :]).astype(LOW)
    q_ref[...] = query * jnp.asarray(SCALE, LOW)
    k_ref[...] = dot_nn(norm, wk[0]).astype(LOW)
    v_ref[...] = (dot_nn(norm, wv[0]) + vec_ref[4:5, :]).astype(LOW)


def whole(shape):
    return spec(shape, lambda *_: (0,) * len(shape), once=True)


def qkv(x, vec, self_a, self_b, block):
    rows, width = x.shape
    row = lambda i: (i, 0)
    weight = lambda which: spec((1, width, width), lambda i: (which, 0, 0), once=True)
    return run(
        qkv_body,
        "qkv",
        (rows // block,),
        (x, vec, self_a, self_a, self_b),
        [spec((block, width), row), whole(vec.shape), weight(0), weight(1), weight(0)],
        [((rows, width), LOW, spec((block, width), row))] * 4,
        flops=6 * rows * width * width,
    )


def head_lanes(values, head):
    lane = lax.broadcasted_iota(jnp.int32, (1, PAIR), 1)
    inside = lane < HALF_PAIR if head == 0 else lane >= HALF_PAIR
    return jnp.where(inside, values, jnp.zeros_like(values))


def attend_body(causal, pairs, step_rows, q_ref, k_ref, v_ref, o_ref):
    length = q_ref.shape[0]
    frames = k_ref.shape[0]
    for pair in range(pairs):
        lanes = slice(pair * PAIR, (pair + 1) * PAIR)
        values = v_ref[:, lanes]
        by_head = [head_lanes(values, head) for head in (0, 1)]
        for start in range(0, length, step_rows):
            stop = min(start + step_rows, length)
            seen = stop if causal else frames
            keys = k_ref[0:seen, lanes]
            queries = q_ref[start:stop, lanes]
            total = None
            for head in (0, 1):
                scores = dot_nt(head_lanes(queries, head), keys)
                if causal:
                    shape = scores.shape
                    key_at = lax.broadcasted_iota(jnp.int32, shape, 1)
                    query_at = lax.broadcasted_iota(jnp.int32, shape, 0) + start
                    scores = jnp.where(key_at <= query_at, scores, -1e30)
                top = jnp.max(scores, -1, keepdims=True)
                exps = jnp.exp(scores - top)
                probs = exps * (1.0 / jnp.sum(exps, -1, keepdims=True))
                part = dot_nn(probs.astype(LOW), by_head[head][0:seen])
                total = part if total is None else total + part
            o_ref[start:stop, lanes] = total.astype(LOW)


def attend(q, k, v, batch, causal, pairs=2, step_rows=128):
    rows, width = q.shape
    length, frames = rows // batch, k.shape[0] // batch
    lanes = pairs * PAIR
    at = lambda b, p: (b, p)
    return run(
        functools.partial(attend_body, causal, pairs, step_rows),
        "attend_self" if causal else "attend_cross",
        (batch, width // lanes),
        (q, k, v),
        [spec((length, lanes), at), spec((frames, lanes), at), spec((frames, lanes), at)],
        [((rows, width), LOW, spec((length, lanes), at))],
        flops=4 * rows * frames * width,
        exps=rows * frames * HEADS,
    )[0]


def attend_back_body(causal, pairs, step_rows, q_ref, k_ref, v_ref, g_ref, gq_ref, gk_ref, gv_ref, dk, dv):
    length = q_ref.shape[0]
    frames = k_ref.shape[0]
    for pair in range(pairs):
        lanes = slice(pair * PAIR, (pair + 1) * PAIR)
        for start in range(0, length, step_rows):
            stop = min(start + step_rows, length)
            seen = stop if causal else frames
            keys = k_ref[0:seen, lanes]
            values = v_ref[0:seen, lanes]
            queries = q_ref[start:stop, lanes]
            grads = g_ref[start:stop, lanes]
            grad_q = grad_k = grad_v = None
            for head in (0, 1):
                head_keys = head_lanes(keys, head)
                scores = dot_nt(head_keys, queries)
                if causal:
                    shape = scores.shape
                    key_at = lax.broadcasted_iota(jnp.int32, shape, 0)
                    query_at = lax.broadcasted_iota(jnp.int32, shape, 1) + start
                    scores = jnp.where(key_at <= query_at, scores, -1e30)
                top = jnp.max(scores, 0, keepdims=True)
                exps = jnp.exp(scores - top)
                probs = exps * (1.0 / jnp.sum(exps, 0, keepdims=True))
                grad_probs = dot_nt(head_lanes(values, head), grads)
                weighted = probs * grad_probs
                inner = jnp.sum(weighted, 0, keepdims=True)
                grad_scores = (weighted - probs * inner).astype(LOW)
                part_v = dot_nn(probs.astype(LOW), head_lanes(grads, head))
                part_k = dot_nn(grad_scores, head_lanes(queries, head))
                part_q = dot_tn(grad_scores, head_keys)
                grad_v = part_v if grad_v is None else grad_v + part_v
                grad_k = part_k if grad_k is None else grad_k + part_k
                grad_q = part_q if grad_q is None else grad_q + part_q
            gq_ref[start:stop, lanes] = (grad_q * SCALE).astype(LOW)
            if causal:
                old = 0 if start == 0 else start
                if old:
                    dk[0:old, :] += grad_k[0:old]
                    dv[0:old, :] += grad_v[0:old]
                dk[old:seen, :] = grad_k[old:]
                dv[old:seen, :] = grad_v[old:]
            elif start == 0:
                dk[...] = grad_k
                dv[...] = grad_v
            else:
                dk[...] += grad_k
                dv[...] += grad_v
        gk_ref[:, lanes] = dk[...].astype(LOW)
        gv_ref[:, lanes] = dv[...].astype(LOW)


def attend_back(q, k, v, grad, batch, causal, pairs=2, step_rows=128):
    rows, width = q.shape
    length, frames = rows // batch, k.shape[0] // batch
    lanes = pairs * PAIR
    at = lambda b, p: (b, p)
    long, short = spec((length, lanes), at), spec((frames, lanes), at)
    return run(
        functools.partial(attend_back_body, causal, pairs, step_rows),
        "attend_self_back" if causal else "attend_cross_back",
        (batch, width // lanes),
        (q, k, v, grad),
        [long, short, short, long],
        [((rows, width), LOW, long), (k.shape, LOW, short), (k.shape, LOW, short)],
        [pltpu.VMEM((frames, PAIR), WIDE)] * 2,
        flops=10 * rows * frames * width,
        exps=rows * frames * HEADS,
    )


def mid_body(per_seq, len_ref, a_ref, x_ref, vec_ref, wo, mid_ref, n_ref, s_ref):
    step = pl.program_id(0)
    branch = dot_nn(a_ref[...], wo[0]) + vec_ref[5:6, :]
    mid = x_ref[...].astype(WIDE) + branch
    mid_ref[...] = mid
    unit, _ = normalised(mid)
    n_ref[...] = (unit * vec_ref[1:2, :] + vec_ref[11:12, :]).astype(LOW)
    add_rows(s_ref, step == 0, [masked_squares(branch, len_ref, step, per_seq)])


def smem():
    return pl.BlockSpec(memory_space=pltpu.SMEM)


def mid_stage(lengths, attended, x, vec, self_b, batch, block):
    rows, width = x.shape
    weight = spec((1, width, width), lambda i: (1, 0, 0), once=True)
    tile = spec((block, width), lambda i: (i, 0))
    return run(
        functools.partial(mid_body, rows // batch // block),
        "mid_stage",
        (rows // block,),
        (lengths, attended, x, vec, self_b),
        [smem(), tile, tile, whole(vec.shape), weight],
        [
            ((rows, width), WIDE, tile),
            ((rows, width), LOW, tile),
            ((8, width), WIDE, spec((8, width), lambda i: (0, 0))),
        ],
        flops=2 * rows * width * width,
    )


def cross_body(n_ref, f_ref, vec_ref, wq, wk, wv, q_ref, k_ref, v_ref):
    query = (dot_nn(n_ref[...], wq[0]) + vec_ref[6:7, :]).astype(LOW)
    q_ref[...] = query * jnp.asarray(SCALE, LOW)
    frames = f_ref[...]
    k_ref[...] = dot_nn(frames, wk[0]).astype(LOW)
    v_ref[...] = (dot_nn(frames, wv[0]) + vec_ref[7:8, :]).astype(LOW)


def cross_stage(norm, frames, vec, cross_a, cross_b, batch):
    width = norm.shape[1]
    rows, frame_rows = norm.shape[0], frames.shape[0]
    long = spec((rows // batch, width), lambda i: (i, 0))
    short = spec((frame_rows // batch, width), lambda i: (i, 0))
    weight = lambda which: spec((1, width, width), lambda i: (which, 0, 0), once=True)
    return run(
        cross_body,
        "cross_stage",
        (batch,),
        (norm, frames, vec, cross_a, cross_b, cross_b),
        [long, short, whole(vec.shape), weight(0), weight(0), weight(1)],
        [((rows, width), LOW, long), ((frame_rows, width), LOW, short), ((frame_rows, width), LOW, short)],
        flops=(2 * rows + 4 * frame_rows) * width * width,
    )


def late_body(per_seq, len_ref, a_ref, mid_ref, vec_ref, wo, late_ref, n_ref, s_ref):
    step = pl.program_id(0)
    branch = dot_nn(a_ref[...], wo[0]) + vec_ref[8:9, :]
    late = mid_ref[...] + branch
    late_ref[...] = late
    unit, _ = normalised(late)
    n_ref[...] = (unit * vec_ref[2:3, :] + vec_ref[12:13, :]).astype(LOW)
    add_rows(s_ref, step == 0, [masked_squares(branch, len_ref, step, per_seq)])


def late_stage(lengths, attended, mid, vec, cross_a, batch, block):
    rows, width = mid.shape
    tile = spec((block, width), lambda i: (i, 0))
    return run(
        functools.partial(late_body, rows // batch // block),
        "late_stage",
        (rows // block,),
        (lengths, attended, mid, vec, cross_a),
        [smem(), tile, tile, whole(vec.shape), spec((1, width, width), lambda i: (1, 0, 0), once=True)],
        [
            ((rows, width), WIDE, tile),
            ((rows, width), LOW, tile),
            ((8, width), WIDE, spec((8, width), lambda i: (0, 0))),
        ],
        flops=2 * rows * width * width,
    )


def ffn_in_body(n_ref, b_ref, w_ref, h_ref, d_ref):
    pre = dot_nn(n_ref[...], w_ref[0]) + b_ref[0]
    below = 0.5 + 0.5 * lax.erf(pre * (0.5**0.5))
    density = jnp.exp(-0.5 * pre * pre) * (1.0 / math.sqrt(2.0 * math.pi))
    h_ref[...] = (pre * below).astype(LOW)
    d_ref[...] = (below + pre * density).astype(LOW)


def ffn_in(norm, bias, weight, block):
    rows, width = norm.shape
    mats = weight.shape[0]
    tile = spec((block, width), lambda j, i: (i, j))
    return run(
        ffn_in_body,
        "ffn_in",
        (mats, rows // block),
        (norm, bias, weight),
        [
            spec((block, width), lambda j, i: (i, 0)),
            spec((1, 1, width), lambda j, i: (j, 0, 0)),
            spec((1, width, width), lambda j, i: (j, 0, 0)),
        ],
        [((rows, mats * width), LOW, tile)] * 2,
        flops=2 * rows * width * width * mats,
        exps=2 * rows * width * mats,
    )


def ffn_out_body(per_seq, len_ref, ha, hb, late_ref, vec_ref, oa, ob, r_ref, s_ref):
    step = pl.program_id(0)
    width = oa.shape[2]
    branch = vec_ref[9:10, :]
    for hidden, weight in ((ha, oa), (hb, ob)):
        for mat in range(weight.shape[0]):
            branch = branch + dot_nn(hidden[:, mat * width : (mat + 1) * width], weight[mat])
    result = late_ref[...] + branch
    r_ref[...] = result.astype(LOW)
    sums = [masked_squares(v, len_ref, step, per_seq) for v in (result, branch)]
    add_rows(s_ref, step == 0, sums)


def ffn_out(lengths, ha, hb, late, vec, out_a, out_b, batch, block):
    rows, width = late.shape
    inner = ha.shape[1]
    tile = spec((block, width), lambda i: (i, 0))
    wide = spec((block, inner), lambda i: (i, 0))
    return run(
        functools.partial(ffn_out_body, rows // batch // block),
        "ffn_out",
        (rows // block,),
        (lengths, ha, hb, late, vec, out_a, out_b),
        [smem(), wide, wide, tile, whole(vec.shape), whole(out_a.shape), whole(out_b.shape)],
        [((rows, width), LOW, tile), ((8, width), WIDE, spec((8, width), lambda i: (0, 0)))],
        flops=4 * rows * inner * width,
    )


def d_out_body(hidden, g_ref, dw_ref, s_ref):
    grad = g_ref[...]
    dw_ref[0] = dot_tn(hidden[...], grad).astype(LOW)
    add_rows(s_ref, pl.program_id(0) == 0, [])

    @pl.when(pl.program_id(0) == 0)
    def _():
        s_ref[0:1, :] = col_sum(grad)


def d_out(hidden, grad):
    rows, inner = hidden.shape
    width = grad.shape[1]
    mats = inner // width
    return run(
        d_out_body,
        "d_out",
        (mats,),
        (hidden, grad),
        [spec((rows, width), lambda j: (0, j)), whole(grad.shape)],
        [
            ((mats, width, width), LOW, spec((1, width, width), lambda j: (j, 0, 0))),
            ((8, width), WIDE, spec((8, width), lambda j: (0, 0))),
        ],
        flops=2 * rows * inner * width,
    )


def ffn_back_body(g_ref, d_ref, o_ref, n_ref, p_ref, dw_ref, s_ref):
    grad = dot_nt(g_ref[...], o_ref[0])
    pre = (grad * d_ref[...].astype(WIDE)).astype(LOW)
    p_ref[...] = pre
    s_ref[0] = col_sum(pre)
    dw_ref[0] = dot_tn(n_ref[...], pre).astype(LOW)


def ffn_back(grad, slope, weight, norm):
    rows, inner = slope.shape
    width = grad.shape[1]
    mats = inner // width
    mat = spec((1, width, width), lambda j: (j, 0, 0))
    tile = spec((rows, width), lambda j: (0, j))
    return run(
        ffn_back_body,
        "ffn_back",
        (mats,),
        (grad, slope, weight, norm),
        [whole(grad.shape), tile, mat, whole(norm.shape)],
        [
            ((rows, inner), LOW, tile),
            ((mats, width, width), LOW, mat),
            ((mats, 1, width), WIDE, spec((1, 1, width), lambda j: (j, 0, 0))),
        ],
        flops=4 * rows * inner * width,
    )


def late_back_body(pa, pb, wa, wb, late_ref, og_ref, vec_ref, wo, gl_ref, gc_ref, ga_ref, s_ref):
    width = wa.shape[1]
    grad = None
    for pre, weight in ((pa, wa), (pb, wb)):
        for mat in range(weight.shape[0]):
            part = dot_nt(pre[:, mat * width : (mat + 1) * width], weight[mat])
            grad = part if grad is None else grad + part
    through, for_gain = norm_backward(late_ref[...], grad, vec_ref[2:3, :])
    total = og_ref[...].astype(WIDE) + through
    gl_ref[...] = total
    low = total.astype(LOW)
    gc_ref[...] = low
    ga_ref[...] = dot_nt(low, wo[0]).astype(LOW)
    add_rows(s_ref, pl.program_id(0) == 0, [col_sum(for_gain), col_sum(grad), col_sum(low)])


def late_back(pa, pb, in_a, in_b, late, grad, vec, cross_a, block):
    rows, width = late.shape
    inner = pa.shape[1]
    tile = spec((block, width), lambda i: (i, 0))
    wide = spec((block, inner), lambda i: (i, 0))
    return run(
        late_back_body,
        "late_back",
        (rows // block,),
        (pa, pb, in_a, in_b, late, grad, vec, cross_a),
        [
            wide,
            wide,
            whole(in_a.shape),
            whole(in_b.shape),
            tile,
            tile,
            whole(vec.shape),
            spec((1, width, width), lambda i: (1, 0, 0), once=True),
        ],
        [
            ((rows, width), WIDE, tile),
            ((rows, width), LOW, tile),
            ((rows, width), LOW, tile),
            ((8, width), WIDE, spec((8, width), lambda i: (0, 0))),
        ],
        flops=4 * rows * inner * width + 2 * rows * width * width,
    )


def weights_body(count, *refs):
    out = refs[-1]
    for place in range(count):
        out[place] = dot_tn(refs[2 * place][...], refs[2 * place + 1][...]).astype(LOW)


def weight_grads(pairs, block):
    width = pairs[0][0].shape[1]
    operands, specs = [], []
    for left, right in pairs:
        operands += [left, right]
        specs += [spec((left.shape[0], block), lambda j: (0, j)), whole(right.shape)]
    return run(
        functools.partial(weights_body, len(pairs)),
        "weight_grads",
        (width // block,),
        tuple(operands),
        specs,
        [((len(pairs), width, width), LOW, spec((len(pairs), block, width), lambda j: (0, j, 0)))],
        flops=sum(2 * left.shape[0] * width * width for left, _ in pairs),
    )[0]


def mid_back_body(gq, wq, mid_ref, gl_ref, vec_ref, wo, gm_ref, gs_ref, ga_ref, s_ref):
    query = gq[...]
    grad = dot_nt(query, wq[0])
    through, for_gain = norm_backward(mid_ref[...], grad, vec_ref[1:2, :])
    total = gl_ref[...] + through
    gm_ref[...] = total
    low = total.astype(LOW)
    gs_ref[...] = low
    ga_ref[...] = dot_nt(low, wo[0]).astype(LOW)
    add_rows(
        s_ref,
        pl.program_id(0) == 0,
        [col_sum(for_gain), col_sum(grad), col_sum(low), col_sum(query)],
    )


def mid_back(grad_q, cross_a, mid, grad_late, vec, self_b, block):
    rows, width = mid.shape
    tile = spec((block, width), lambda i: (i, 0))
    weight = lambda which: spec((1, width, width), lambda i: (which, 0, 0), once=True)
    return run(
        mid_back_body,
        "mid_back",
        (rows // block,),
        (grad_q, cross_a, mid, grad_late, vec, self_b),
        [tile, weight(0), tile, tile, whole(vec.shape), weight(1)],
        [
            ((rows, width), WIDE, tile),
            ((rows, width), LOW, tile),
            ((rows, width), LOW, tile),
            ((8, width), WIDE, spec((8, width), lambda i: (0, 0))),
        ],
        flops=4 * rows * width * width,
    )


def frames_back_body(gk, gv, wk, wv, ge_ref, s_ref):
    grad_v = gv[...]
    ge_ref[...] = (dot_nt(gk[...], wk[0]) + dot_nt(grad_v, wv[0])).astype(LOW)
    add_rows(s_ref, pl.program_id(0) == 0, [col_sum(grad_v)])


def frames_back(grad_k, grad_v, cross_b, block):
    rows, width = grad_k.shape
    tile = spec((block, width), lambda i: (i, 0))
    weight = lambda which: spec((1, width, width), lambda i: (which, 0, 0), once=True)
    return run(
        frames_back_body,
        "frames_back",
        (rows // block,),
        (grad_k, grad_v, cross_b, cross_b),
        [tile, tile, weight(0), weight(1)],
        [((rows, width), LOW, tile), ((8, width), WIDE, spec((8, width), lambda i: (0, 0)))],
        flops=4 * rows * width * width,
    )


def in_back_body(gq, gk, gv, wq, wk, wv, x_ref, gm_ref, vec_ref, gi_ref, s_ref):
    query, value = gq[...], gv[...]
    grad = dot_nt(query, wq[0]) + dot_nt(gk[...], wk[0]) + dot_nt(value, wv[0])
    through, for_gain = norm_backward(x_ref[...].astype(WIDE), grad, vec_ref[0:1, :])
    gi_ref[...] = (gm_ref[...] + through).astype(LOW)
    add_rows(
        s_ref,
        pl.program_id(0) == 0,
        [col_sum(for_gain), col_sum(grad), col_sum(query), col_sum(value)],
    )


def in_back(grad_q, grad_k, grad_v, self_a, self_b, x, grad_mid, vec, block):
    rows, width = x.shape
    tile = spec((block, width), lambda i: (i, 0))
    weight = lambda which: spec((1, width, width), lambda i: (which, 0, 0), once=True)
    return run(
        in_back_body,
        "in_back",
        (rows // block,),
        (grad_q, grad_k, grad_v, self_a, self_a, self_b, x, grad_mid, vec),
        [tile, tile, tile, weight(0), weight(1), weight(0), tile, tile, whole(vec.shape)],
        [((rows, width), LOW, tile), ((8, width), WIDE, spec((8, width), lambda i: (0, 0)))],
        flops=6 * rows * width * width,
    )


def axis_bits(count):
    bits = count.bit_length() - 1
    assert 1 << bits == count
    each = (bits - 1) // 3
    x_bits = list(range(1, 1 + each))
    y_bits = list(range(1 + each, 1 + 2 * each))
    z_bits = list(range(1 + 2 * each, bits))
    return x_bits, y_bits, z_bits


def gather_stages(count, parts):
    x_bits, y_bits, z_bits = (list(reversed(b)) for b in axis_bits(count))
    if parts == 1:
        return [[(b,) for b in bits] for bits in (z_bits[:1], z_bits[1:], y_bits, x_bits, [0])]
    return [
        [(z_bits[0],)],
        [(b,) for b in z_bits[1:]],
        list(zip(y_bits, x_bits)),
        list(zip(x_bits, y_bits)),
        [(0, 0)],
    ]


def scatter_stages(count, parts):
    return [list(reversed(stage)) for stage in reversed(gather_stages(count, parts))]


def swap(values, bit, count):
    return lax.ppermute(values, "fsdp", [(i, i ^ (1 << bit)) for i in range(count)])


def own_bit(bit):
    return (lax.axis_index("fsdp") >> bit) & 1


def halves(parts):
    if len(parts) == 2:
        return parts
    middle = parts[0].shape[0] // 2
    return [parts[0][:middle], parts[0][middle:]]


class Gather:
    def __init__(self, piece, count, parts=2):
        self.count = count
        self.bits = count.bit_length() - 1
        mats, rows, width = piece.shape
        self.shape = (rows, width)
        self.parts = [piece.reshape((mats,) + (1,) * self.bits + (rows, width))]
        self.stages = gather_stages(count, parts)
        self.flight = None

    def axis(self, bit):
        return self.bits - bit

    def land(self):
        if self.flight is not None:
            parts = []
            for held, (bit, other) in zip(self.parts, self.flight):
                axis = self.axis(bit)
                parts.append(
                    jnp.where(
                        own_bit(bit) == 0,
                        jnp.concatenate([held, other], axis),
                        jnp.concatenate([other, held], axis),
                    )
                )
            self.parts = parts
            self.flight = None

    def ready(self):
        self.land()
        if len(self.stages[0][0]) == 2:
            self.parts = halves(self.parts)
        return self.parts

    def launch(self, parts):
        self.parts = parts
        for place, step in enumerate(self.stages.pop(0)):
            if place:
                self.land()
            self.flight = [(bit, swap(part, bit, self.count)) for bit, part in zip(step, self.parts)]

    def result(self):
        self.land()
        rows, width = self.shape
        return [part.reshape(part.shape[0], self.count * rows, width) for part in self.parts]


class Scatter:
    def __init__(self, parts, count):
        self.count = count
        self.bits = count.bit_length() - 1
        self.pairs = []
        for part in parts:
            mats, rows, width = part.shape
            self.shape = (rows // count, width)
            self.pairs.append((part.reshape((mats,) + (2,) * self.bits + (rows // count, width)), None))
        self.stages = scatter_stages(count, len(parts))
        self.kind = parts[0].dtype

    def pick(self, pair, bit, side):
        axis = self.bits - bit
        values = [
            lax.dynamic_slice_in_dim(v, side, 1, axis) for v in pair if v is not None
        ]
        if len(values) == 1:
            return values[0]
        return (values[0].astype(jnp.float32) + values[1].astype(jnp.float32)).astype(self.kind)

    def prepare(self):
        step = self.stages[0][0]
        if len(step) == 1 and len(self.pairs) == 2:
            self.pairs = [
                (jnp.concatenate([self.total(p, self.kind) for p in self.pairs]), None)
            ]
        return [self.pick(pair, bit, 1 - own_bit(bit)) for bit, pair in zip(step, self.pairs)]

    def ready(self):
        return self.prepare()

    def total(self, pair, kind):
        if pair[1] is None:
            return pair[0]
        return (pair[0].astype(jnp.float32) + pair[1].astype(jnp.float32)).astype(kind)

    def launch(self, sends):
        steps = self.stages.pop(0)
        for place, step in enumerate(steps):
            if place:
                self.stages.insert(0, [step])
                sends = self.prepare()
                self.stages.pop(0)
            flight = [swap(v, bit, self.count) for bit, v in zip(step, sends)]
            self.pairs = [
                (self.pick(pair, bit, own_bit(bit)), other)
                for bit, pair, other in zip(step, self.pairs, flight)
            ]

    def result(self):
        total = jnp.concatenate([self.total(p, jnp.float32) for p in self.pairs])
        return total.astype(jnp.float32).reshape((total.shape[0],) + self.shape)


def tick(chains, values=()):
    ready = [chain.ready() for chain in chains]
    ready, values = lax.optimization_barrier((ready, values))
    for chain, parts in zip(chains, ready):
        chain.launch(parts)
    return values


def shards(
    count,
    hidden_in,
    encoder_states,
    lengths,
    out_grad,
    attn_in,
    attn_out,
    fc_in,
    fc_out,
    gains,
    biases,
    ffn_bias,
):
    batch, length, width = hidden_in.shape
    rows = batch * length
    block = length // 2
    frame_rows = encoder_states.shape[1]
    share = gains.shape[1]
    ff_share = ffn_bias.shape[0]
    mats = ff_share // share
    middle = mats // 2

    small = jnp.concatenate([gains.reshape(-1), biases.reshape(-1), ffn_bias])
    small_count = small.shape[0]
    small_rows = -(-(small_count + 5) // 128)
    small_size = small_rows * 128
    small = jnp.pad(small, (0, small_size - small_count)).reshape(1, small_rows, 128)
    fc_in_mats = fc_in.reshape(share, count, mats, share).transpose(2, 0, 1, 3).reshape(mats, share, width)
    fc_out_mats = fc_out.reshape(mats, share, width)
    g_small = Gather(small, count, 1)
    g_self = Gather(jnp.concatenate([attn_in[0:3], attn_out[0:1]]), count)
    g_cross = Gather(jnp.concatenate([attn_in[3:4], attn_out[1:2], attn_in[4:6]]), count)
    g_in = Gather(fc_in_mats, count)
    g_out = Gather(fc_out_mats, count)

    x = hidden_in.reshape(rows, width)
    frames = encoder_states.reshape(-1, width)
    valid = jnp.arange(length)[None, :, None] < lengths[:, None, None]
    grad = jnp.where(valid, out_grad, jnp.zeros_like(out_grad)).reshape(rows, width)

    tick([g_self, g_small])
    tick([g_self, g_small])
    tick([g_self, g_small, g_cross])
    tick([g_self, g_small, g_cross, g_in])
    tick([g_self, g_small, g_cross, g_in])
    small = g_small.result()[0].astype(jnp.float32).reshape(count, small_size)
    vec = small[:, : 13 * share].reshape(count, 13, share).transpose(1, 0, 2).reshape(13, width)
    vec = jnp.pad(vec, ((0, 3), (0, 0)))
    bias = small[:, 13 * share : small_count].reshape(count, mats, share)
    bias = bias.transpose(1, 0, 2).reshape(mats, 1, width)
    self_a, self_b = g_self.result()
    norm_one, query, key, value = qkv(x, vec, self_a, self_b, block)
    query, key, value = tick([g_cross, g_in, g_out], (query, key, value))
    attended = attend(query, key, value, batch, True)
    mid, norm_two, square_self = mid_stage(lengths, attended, x, vec, self_b, batch, block)
    norm_two = tick([g_cross, g_in, g_out], norm_two)
    cross_a, cross_b = g_cross.result()
    cross_q, cross_k, cross_v = cross_stage(norm_two, frames, vec, cross_a, cross_b, batch)
    cross_attended = attend(cross_q, cross_k, cross_v, batch, False)
    cross_attended = tick([g_in, g_out], cross_attended)
    late, norm_three, square_cross = late_stage(lengths, cross_attended, mid, vec, cross_a, batch, block)
    in_a, in_b = g_in.result()
    hidden_a, slope_a = ffn_in(norm_three, bias[:middle], in_a, block)
    hidden_b, slope_b = ffn_in(norm_three, bias[middle:], in_b, block)
    hidden_a, hidden_b = tick([g_out], (hidden_a, hidden_b))
    d_out_a, sums_out = d_out(hidden_a, grad)
    d_out_b, _ = d_out(hidden_b, grad)
    s_out = Scatter([d_out_a, d_out_b], count)
    grad = tick([g_out, s_out], grad)
    out_a, out_b = g_out.result()
    pre_a, d_in_a, sums_in_a = ffn_back(grad, slope_a, out_a, norm_three)
    hidden_a, hidden_b, grad = tick([s_out], (hidden_a, hidden_b, grad))
    pre_b, d_in_b, sums_in_b = ffn_back(grad, slope_b, out_b, norm_three)
    result, square_rest = ffn_out(lengths, hidden_a, hidden_b, late, vec, out_a, out_b, batch, block)
    s_in = Scatter([d_in_a, d_in_b], count)
    pre_a, pre_b = tick([s_in], (pre_a, pre_b))
    grad_late, grad_cross, grad_cross_att, sums_late = late_back(
        pre_a, pre_b, in_a, in_b, late, grad, vec, cross_a, block
    )
    grad_cross_att = tick([s_in, s_out], grad_cross_att)
    grad_cq, grad_ck, grad_cv = attend_back(
        cross_q, cross_k, cross_v, grad_cross_att, batch, False
    )
    d_cross_a = weight_grads([(norm_two, grad_cq), (cross_attended, grad_cross)], width // 3)
    d_cross_b = weight_grads([(frames, grad_ck), (frames, grad_cv)], width // 3)
    s_cross = Scatter([d_cross_a, d_cross_b], count)
    grad_cq = tick([s_cross, s_in, s_out], grad_cq)
    grad_mid, grad_self, grad_att, sums_mid = mid_back(
        grad_cq, cross_a, mid, grad_late, vec, self_b, block
    )
    grad_att = tick([s_cross, s_in, s_out], grad_att)
    grad_q, grad_k, grad_v = attend_back(query, key, value, grad_att, batch, True)
    grad_q, grad_k, grad_v = tick([s_cross, s_in], (grad_q, grad_k, grad_v))
    d_self_a = weight_grads([(norm_one, grad_q), (norm_one, grad_k)], width // 3)
    d_self_b = weight_grads([(norm_one, grad_v), (attended, grad_self)], width // 3)
    s_self = Scatter([d_self_a, d_self_b], count)
    grad_q, grad_k, grad_v = tick([s_self, s_cross], (grad_q, grad_k, grad_v))
    grad_in, sums_one = in_back(grad_q, grad_k, grad_v, self_a, self_b, x, grad_mid, vec, block)
    grad_ck, grad_cv = tick([s_self, s_cross], (grad_ck, grad_cv))
    grad_frames, sums_frames = frames_back(grad_ck, grad_cv, cross_b, frame_rows)

    sum_rows = jnp.stack(
        [sums_one[0], sums_mid[0], sums_late[0]]
        + [sums_one[2], sums_one[3], sums_mid[2], sums_mid[3], sums_frames[0], sums_late[2], sums_out[0]]
        + [sums_one[1], sums_mid[1], sums_late[1]]
    )
    squares = jnp.stack([square_rest[0], square_self[0], square_cross[0], square_rest[1]])
    stats = jnp.concatenate([jnp.sum(squares, -1), jnp.sum(lengths).astype(WIDE)[None]])
    sums_ff = jnp.concatenate([sums_in_a, sums_in_b]).reshape(mats, count, share)
    sums = jnp.concatenate(
        [
            sum_rows.reshape(13, count, share).transpose(1, 0, 2).reshape(count, 13 * share),
            sums_ff.transpose(1, 0, 2).reshape(count, ff_share),
            jnp.broadcast_to(stats[None], (count, 5)),
        ],
        1,
    )
    sums = jnp.pad(sums, ((0, 0), (0, small_size - sums.shape[1])))
    s_small = Scatter([sums.reshape(1, count * small_rows, 128)], count)
    tick([s_self, s_small])
    tick([s_self, s_small])
    tick([s_self, s_small])
    tick([s_small])
    tick([s_small])
    d_out_all = s_out.result()
    d_in_all = s_in.result()
    d_cross = s_cross.result()
    d_self = s_self.result()
    small = s_small.result().reshape(-1)
    stats = small[small_count : small_count + 5]
    rms = jnp.sqrt(stats[:4] / (stats[4] * width))
    return (
        result.reshape(hidden_in.shape),
        grad_in.reshape(hidden_in.shape),
        grad_frames.reshape(encoder_states.shape),
        jnp.concatenate([d_self[:3], d_cross[:1], d_cross[2:]]),
        jnp.concatenate([d_self[3:], d_cross[1:2]]),
        d_in_all.reshape(mats, share, count, share).transpose(1, 2, 0, 3).reshape(share, -1),
        d_out_all.reshape(ff_share, width),
        small[: 3 * share].reshape(3, share),
        small[3 * share : 13 * share].reshape(10, share),
        small[13 * share : small_count],
        rms,
    )


def solution(mesh):
    placed = (
        P("fsdp", None, None),
        P("fsdp", None, None),
        P("fsdp"),
        P("fsdp", None, None),
        P(None, "fsdp", None),
        P(None, "fsdp", None),
        P("fsdp", None),
        P("fsdp", None),
        P(None, "fsdp"),
        P(None, "fsdp"),
        P("fsdp"),
    )
    return jax.shard_map(
        functools.partial(shards, mesh.shape["fsdp"]),
        mesh=mesh,
        in_specs=placed,
        out_specs=(
            P("fsdp", None, None),
            P("fsdp", None, None),
            P("fsdp", None, None),
            P(None, "fsdp", None),
            P(None, "fsdp", None),
            P("fsdp", None),
            P("fsdp", None),
            P(None, "fsdp"),
            P(None, "fsdp"),
            P("fsdp"),
            P(),
        ),
        check_vma=False,
    )
```

```python
import functools
import math

import jax
import jax.numpy as jnp
from jax import lax
from jax.experimental import pallas as pl
from jax.experimental.pallas import tpu as pltpu
from jax.sharding import PartitionSpec as P

NORM_EPS = 1e-05
LOW = jnp.bfloat16
WIDE = jnp.float32
HEADS = 12
PAIR = 128
HALF_PAIR = 64
SCALE = 0.125


def dot_nn(left, right):
    return lax.dot_general(left, right, (((1,), (0,)), ((), ())), preferred_element_type=WIDE)


def dot_nt(left, right):
    return lax.dot_general(left, right, (((1,), (1,)), ((), ())), preferred_element_type=WIDE)


def dot_tn(left, right):
    return lax.dot_general(left, right, (((0,), (0,)), ((), ())), preferred_element_type=WIDE)


def spec(block, index, once=False):
    if once:
        return pl.BlockSpec(block, index, pipeline_mode=pl.Buffered(1))
    return pl.BlockSpec(block, index)


def run(body, name, grid, operands, in_specs, outs, scratch=(), flops=0, exps=0, limit=20):
    moved = sum(o.size * o.dtype.itemsize for o in operands)
    moved += sum(math.prod(s) * jnp.dtype(d).itemsize for s, d, _ in outs)
    return pl.pallas_call(
        body,
        name=name,
        grid=grid,
        in_specs=in_specs,
        out_specs=[o[2] for o in outs],
        out_shape=[jax.ShapeDtypeStruct(o[0], o[1]) for o in outs],
        scratch_shapes=list(scratch),
        compiler_params=pltpu.CompilerParams(
            dimension_semantics=("arbitrary",) * len(grid), vmem_limit_bytes=limit << 20
        ),
        cost_estimate=pl.CostEstimate(flops=flops, transcendentals=exps, bytes_accessed=moved),
    )(*operands)


def normalised(values):
    center = values - jnp.mean(values, -1, keepdims=True)
    spread = jnp.mean(center * center, -1, keepdims=True)
    scale = lax.rsqrt(spread + NORM_EPS)
    return center * scale, scale


def norm_backward(values, grad, gain):
    unit, scale = normalised(values)
    inner = grad * gain
    mean_inner = jnp.mean(inner, -1, keepdims=True)
    mean_unit = jnp.mean(inner * unit, -1, keepdims=True)
    return scale * (inner - mean_inner - unit * mean_unit), grad * unit


def col_sum(values):
    return jnp.sum(values.astype(WIDE), 0, keepdims=True)


def add_rows(ref, first, rows):
    @pl.when(first)
    def _():
        ref[...] = jnp.zeros_like(ref)

    for place, row in enumerate(rows):
        ref[place : place + 1, :] += row


def masked_squares(values, length_ref, step, per_seq):
    rows = values.shape[0]
    start = (step % per_seq) * rows
    index = start + lax.broadcasted_iota(jnp.int32, (rows, 1), 0)
    inside = index < length_ref[step // per_seq]
    return col_sum(jnp.where(inside, values * values, 0.0))


def qkv_body(x_ref, vec_ref, wq, wk, wv, n_ref, q_ref, k_ref, v_ref):
    unit, _ = normalised(x_ref[...].astype(WIDE))
    norm = (unit * vec_ref[0:1, :] + vec_ref[10:11, :]).astype(LOW)
    n_ref[...] = norm
    query = (dot_nn(norm, wq[0]) + vec_ref[3:4, :]).astype(LOW)
    q_ref[...] = query * jnp.asarray(SCALE, LOW)
    k_ref[...] = dot_nn(norm, wk[0]).astype(LOW)
    v_ref[...] = (dot_nn(norm, wv[0]) + vec_ref[4:5, :]).astype(LOW)


def whole(shape):
    return spec(shape, lambda *_: (0,) * len(shape), once=True)


def qkv(x, vec, self_a, self_b, block):
    rows, width = x.shape
    row = lambda i: (i, 0)
    weight = lambda which: spec((1, width, width), lambda i: (which, 0, 0), once=True)
    return run(
        qkv_body,
        "qkv",
        (rows // block,),
        (x, vec, self_a, self_a, self_b),
        [spec((block, width), row), whole(vec.shape), weight(0), weight(1), weight(0)],
        [((rows, width), LOW, spec((block, width), row))] * 4,
        flops=6 * rows * width * width,
    )


def head_lanes(values, head):
    lane = lax.broadcasted_iota(jnp.int32, (1, PAIR), 1)
    inside = lane < HALF_PAIR if head == 0 else lane >= HALF_PAIR
    return jnp.where(inside, values, jnp.zeros_like(values))


def attend_cross_body(pairs, q_ref, k_ref, v_ref, o_ref):
    for pair in range(pairs):
        lanes = slice(pair * PAIR, (pair + 1) * PAIR)
        values, keys, queries = v_ref[:, lanes], k_ref[:, lanes], q_ref[:, lanes]
        total = None
        for head in (0, 1):
            scores = dot_nt(head_lanes(queries, head), keys)
            exps = jnp.exp(scores - jnp.max(scores, -1, keepdims=True))
            probs = exps * (1.0 / jnp.sum(exps, -1, keepdims=True))
            part = dot_nn(probs.astype(LOW), head_lanes(values, head))
            total = part if total is None else total + part
        o_ref[:, lanes] = total.astype(LOW)


def attend_body(pairs, step_rows, q_ref, k_ref, v_ref, o_ref):
    length = q_ref.shape[0]
    starts = list(range(0, length, step_rows))
    for pair in range(pairs):
        lanes = slice(pair * PAIR, (pair + 1) * PAIR)
        turned = v_ref[:, lanes].T
        keys = [head_lanes(k_ref[:, lanes], head) for head in (0, 1)]
        work = []
        for start in starts:
            stop = min(start + step_rows, length)
            queries = q_ref[start:stop, lanes]
            cuts = ([(0, start)] if start else []) + [(start, stop)]
            for head in (0, 1):
                parts = []
                for low, high in cuts:
                    scores = dot_nt(keys[head][low:high], queries)
                    if low == start:
                        key_at = lax.broadcasted_iota(jnp.int32, scores.shape, 0)
                        query_at = lax.broadcasted_iota(jnp.int32, scores.shape, 1)
                        scores = jnp.where(key_at <= query_at, scores, -1e30)
                    parts.append(scores)
                work.append((start, stop, head, cuts, parts))
        tops = []
        for start, stop, head, cuts, parts in work:
            top = jnp.max(parts[0], 0, keepdims=True)
            for scores in parts[1:]:
                top = jnp.maximum(top, jnp.max(scores, 0, keepdims=True))
            tops.append(top)
        exps = [[jnp.exp(s - top) for s in item[4]] for item, top in zip(work, tops)]
        totals = [sum(jnp.sum(e, 0, keepdims=True) for e in group) for group in exps]
        outs = []
        for (start, stop, head, cuts, _), group, total in zip(work, exps, totals):
            out = None
            for (low, high), e in zip(cuts, group):
                part = dot_nn(turned[head * HALF_PAIR : (head + 1) * HALF_PAIR, low:high], e.astype(LOW))
                out = part if out is None else out + part
            outs.append(out * (1.0 / total))
        for place, start in enumerate(starts):
            stop = min(start + step_rows, length)
            both = jnp.concatenate(outs[2 * place : 2 * place + 2], 0)
            o_ref[start:stop, lanes] = both.T.astype(LOW)


def attend(q, k, v, batch, causal, pairs=6, step_rows=128):
    rows, width = q.shape
    length, frames = rows // batch, k.shape[0] // batch
    lanes = pairs * PAIR
    at = lambda b, p: (b, p)
    return run(
        functools.partial(attend_body, pairs, step_rows) if causal else functools.partial(attend_cross_body, pairs),
        "attend_self" if causal else "attend_cross",
        (batch, width // lanes),
        (q, k, v),
        [spec((length, lanes), at), spec((frames, lanes), at), spec((frames, lanes), at)],
        [((rows, width), LOW, spec((length, lanes), at))],
        flops=4 * rows * frames * width,
        exps=rows * frames * HEADS,
    )[0]


def attend_back_body(causal, pairs, step_rows, q_ref, k_ref, v_ref, g_ref, gq_ref, gk_ref, gv_ref, dk, dv):
    length = q_ref.shape[0]
    frames = k_ref.shape[0]
    starts = list(range(0, length, step_rows))
    for pair in range(pairs):
        lanes = slice(pair * PAIR, (pair + 1) * PAIR)
        keys = [head_lanes(k_ref[:, lanes], head) for head in (0, 1)]
        values = [head_lanes(v_ref[:, lanes], head) for head in (0, 1)]
        work = []
        for start in starts:
            stop = min(start + step_rows, length)
            cuts = ([(0, start)] if start else []) + [(start, stop)] if causal else [(0, frames)]
            for head in (0, 1):
                queries, grads = q_ref[start:stop, lanes], g_ref[start:stop, lanes]
                parts = []
                for low, high in cuts:
                    scores = dot_nt(keys[head][low:high], queries)
                    if causal and low == start:
                        key_at = lax.broadcasted_iota(jnp.int32, scores.shape, 0)
                        query_at = lax.broadcasted_iota(jnp.int32, scores.shape, 1)
                        scores = jnp.where(key_at <= query_at, scores, -1e30)
                    parts.append(scores)
                grad_parts = [dot_nt(values[head][low:high], grads) for low, high in cuts]
                work.append((start, stop, head, cuts, parts, grad_parts))
        probs = []
        for item in work:
            parts = item[4]
            top = jnp.max(parts[0], 0, keepdims=True)
            for scores in parts[1:]:
                top = jnp.maximum(top, jnp.max(scores, 0, keepdims=True))
            exps = [jnp.exp(scores - top) for scores in parts]
            total = 1.0 / sum(jnp.sum(e, 0, keepdims=True) for e in exps)
            probs.append([e * total for e in exps])
        scores = []
        for item, group in zip(work, probs):
            weighted = [p * g for p, g in zip(group, item[5])]
            inner = sum(jnp.sum(w, 0, keepdims=True) for w in weighted)
            scores.append([(w - p * inner).astype(LOW) for w, p in zip(weighted, group)])
        grad_q = {}
        for (start, stop, head, cuts, _, _), group, low_scores in zip(work, probs, scores):
            queries = head_lanes(q_ref[start:stop, lanes], head)
            grads = head_lanes(g_ref[start:stop, lanes], head)
            for (low, high), p, s in zip(cuts, group, low_scores):
                part_v = dot_nn(p.astype(LOW), grads)
                part_k = dot_nn(s, queries)
                part_q = dot_tn(s, keys[head][low:high])
                grad_q[start] = part_q if start not in grad_q else grad_q[start] + part_q
                if head == 0 and (low == start or not causal and start == 0):
                    dv[low:high, :] = part_v
                    dk[low:high, :] = part_k
                else:
                    dv[low:high, :] += part_v
                    dk[low:high, :] += part_k
        for start, total in grad_q.items():
            gq_ref[start : start + total.shape[0], lanes] = (total * SCALE).astype(LOW)
        gk_ref[:, lanes] = dk[...].astype(LOW)
        gv_ref[:, lanes] = dv[...].astype(LOW)


def attend_back(q, k, v, grad, batch, causal, pairs=6):
    rows, width = q.shape
    length, frames = rows // batch, k.shape[0] // batch
    lanes = pairs * PAIR
    at = lambda b, p: (b, p)
    long, short = spec((length, lanes), at), spec((frames, lanes), at)
    return run(
        functools.partial(attend_back_body, causal, pairs, 128 if causal else length),
        "attend_self_back" if causal else "attend_cross_back",
        (batch, width // lanes),
        (q, k, v, grad),
        [long, short, short, long],
        [((rows, width), LOW, long), (k.shape, LOW, short), (k.shape, LOW, short)],
        [pltpu.VMEM((frames, PAIR), WIDE)] * 2,
        flops=10 * rows * frames * width,
        exps=rows * frames * HEADS,
    )


def mid_body(per_seq, len_ref, a_ref, x_ref, vec_ref, wo, mid_ref, n_ref, s_ref):
    step = pl.program_id(0)
    branch = dot_nn(a_ref[...], wo[0]) + vec_ref[5:6, :]
    mid = x_ref[...].astype(WIDE) + branch
    mid_ref[...] = mid
    unit, _ = normalised(mid)
    n_ref[...] = (unit * vec_ref[1:2, :] + vec_ref[11:12, :]).astype(LOW)
    add_rows(s_ref, step == 0, [masked_squares(branch, len_ref, step, per_seq)])


def smem():
    return pl.BlockSpec(memory_space=pltpu.SMEM)


def mid_stage(lengths, attended, x, vec, self_b, batch, block):
    rows, width = x.shape
    weight = spec((1, width, width), lambda i: (1, 0, 0), once=True)
    tile = spec((block, width), lambda i: (i, 0))
    return run(
        functools.partial(mid_body, rows // batch // block),
        "mid_stage",
        (rows // block,),
        (lengths, attended, x, vec, self_b),
        [smem(), tile, tile, whole(vec.shape), weight],
        [
            ((rows, width), WIDE, tile),
            ((rows, width), LOW, tile),
            ((8, width), WIDE, spec((8, width), lambda i: (0, 0))),
        ],
        flops=2 * rows * width * width,
    )


def cross_body(n_ref, f_ref, vec_ref, wq, wk, wv, q_ref, k_ref, v_ref):
    query = (dot_nn(n_ref[...], wq[0]) + vec_ref[6:7, :]).astype(LOW)
    q_ref[...] = query * jnp.asarray(SCALE, LOW)
    frames = f_ref[...]
    k_ref[...] = dot_nn(frames, wk[0]).astype(LOW)
    v_ref[...] = (dot_nn(frames, wv[0]) + vec_ref[7:8, :]).astype(LOW)


def cross_stage(norm, frames, vec, cross_a, cross_b, batch):
    width = norm.shape[1]
    rows, frame_rows = norm.shape[0], frames.shape[0]
    long = spec((rows // batch, width), lambda i: (i, 0))
    short = spec((frame_rows // batch, width), lambda i: (i, 0))
    weight = lambda which: spec((1, width, width), lambda i: (which, 0, 0), once=True)
    return run(
        cross_body,
        "cross_stage",
        (batch,),
        (norm, frames, vec, cross_a, cross_b, cross_b),
        [long, short, whole(vec.shape), weight(0), weight(0), weight(1)],
        [((rows, width), LOW, long), ((frame_rows, width), LOW, short), ((frame_rows, width), LOW, short)],
        flops=(2 * rows + 4 * frame_rows) * width * width,
    )


def late_body(per_seq, len_ref, a_ref, mid_ref, vec_ref, wo, late_ref, n_ref, s_ref):
    step = pl.program_id(0)
    branch = dot_nn(a_ref[...], wo[0]) + vec_ref[8:9, :]
    late = mid_ref[...] + branch
    late_ref[...] = late
    unit, _ = normalised(late)
    n_ref[...] = (unit * vec_ref[2:3, :] + vec_ref[12:13, :]).astype(LOW)
    add_rows(s_ref, step == 0, [masked_squares(branch, len_ref, step, per_seq)])


def late_stage(lengths, attended, mid, vec, cross_a, batch, block):
    rows, width = mid.shape
    tile = spec((block, width), lambda i: (i, 0))
    return run(
        functools.partial(late_body, rows // batch // block),
        "late_stage",
        (rows // block,),
        (lengths, attended, mid, vec, cross_a),
        [smem(), tile, tile, whole(vec.shape), spec((1, width, width), lambda i: (1, 0, 0), once=True)],
        [
            ((rows, width), WIDE, tile),
            ((rows, width), LOW, tile),
            ((8, width), WIDE, spec((8, width), lambda i: (0, 0))),
        ],
        flops=2 * rows * width * width,
    )


def ffn_body(first, last, batch, block, len_ref, n_ref, g_ref, b_ref, wi_ref, wo_ref, *refs):
    refs = list(refs)
    before = [] if first else [refs.pop(0), refs.pop(0)]
    late_ref, vec_ref = (refs.pop(0), refs.pop(0)) if last else (None, None)
    gn_ref, di_ref, do_ref, sf_ref, f_ref = refs[:5]
    rest = refs[5:]
    s_ref = rest.pop(0) if last else None
    hidden_ref, pre_ref = rest[:2]
    acc_ref = rest[2] if last else f_ref
    step = pl.program_id(0)
    rows = n_ref.shape[0]

    @pl.when(step == 0)
    def _():
        if first:
            acc_ref[...] = jnp.zeros_like(acc_ref)
            gn_ref[...] = jnp.zeros_like(gn_ref)
        else:
            acc_ref[...] = before[0][...]
            gn_ref[...] = before[1][...]

    def chunk(place, carry):
        at = pl.ds(pl.multiple_of(place * block, block), block)
        pre = dot_nn(n_ref[at, :], wi_ref[0]) + b_ref[0]
        below = 0.5 + 0.5 * lax.erf(pre * (0.5**0.5))
        density = jnp.exp(-0.5 * pre * pre) * (1.0 / math.sqrt(2.0 * math.pi))
        hidden = (pre * below).astype(LOW)
        hidden_ref[at, :] = hidden
        acc_ref[at, :] += dot_nn(hidden, wo_ref[0])
        grad = dot_nt(g_ref[at, :], wo_ref[0])
        grad = (grad * (below + pre * density)).astype(LOW)
        pre_ref[at, :] = grad
        gn_ref[at, :] += dot_nt(grad, wi_ref[0])
        return carry

    lax.fori_loop(0, rows // block, chunk, 0)
    sf_ref[0] = col_sum(pre_ref[...])
    di_ref[0] = dot_tn(n_ref[...], pre_ref[...]).astype(LOW)
    do_ref[0] = dot_tn(hidden_ref[...], g_ref[...]).astype(LOW)
    if last:
        @pl.when(step == pl.num_programs(0) - 1)
        def _():
            s_ref[...] = jnp.zeros_like(s_ref)

            def finish(place, carry):
                at = pl.ds(pl.multiple_of(place * block, block), block)
                branch = acc_ref[at, :] + vec_ref[9:10, :]
                result = late_ref[at, :] + branch
                f_ref[at, :] = result.astype(LOW)
                per_seq = rows // batch // block
                s_ref[0:1, :] += masked_squares(result, len_ref, place, per_seq)
                s_ref[1:2, :] += masked_squares(branch, len_ref, place, per_seq)
                s_ref[2:3, :] += col_sum(g_ref[at, :])
                return carry

            lax.fori_loop(0, rows // block, finish, 0)


def ffn_stage(lengths, norm, grad, bias, w_in, w_out, before, late, vec, batch, block):
    rows, width = norm.shape
    mats = w_in.shape[0]
    first, last = before is None, late is not None
    mat = spec((1, width, width), lambda j: (j, 0, 0))
    line = spec((1, 1, width), lambda j: (j, 0, 0))
    operands = [lengths, norm, grad, bias, w_in, w_out]
    specs = [smem(), whole(norm.shape), whole(grad.shape), line, mat, mat]
    if not first:
        operands += list(before)
        specs += [whole((rows, width))] * 2
    if last:
        operands += [late, vec]
        specs += [whole((rows, width)), whole(vec.shape)]
    fixed = whole((rows, width))
    outs = [
        ((rows, width), WIDE, fixed),
        ((mats, width, width), LOW, mat),
        ((mats, width, width), LOW, mat),
        ((mats, 1, width), WIDE, line),
        ((rows, width), LOW if last else WIDE, fixed),
    ]
    scratch = [pltpu.VMEM((rows, width), LOW)] * 2
    if last:
        outs.append(((8, width), WIDE, whole((8, width))))
        scratch.append(pltpu.VMEM((rows, width), WIDE))
    return run(
        functools.partial(ffn_body, first, last, batch, block),
        "ffn_stage",
        (mats,),
        tuple(operands),
        specs,
        outs,
        scratch,
        flops=12 * rows * width * width * mats,
        exps=2 * rows * width * mats,
        limit=44,
    )


def late_back_body(gn_ref, late_ref, og_ref, vec_ref, wo, gl_ref, gc_ref, ga_ref, s_ref):
    grad = gn_ref[...]
    through, for_gain = norm_backward(late_ref[...], grad, vec_ref[2:3, :])
    total = og_ref[...].astype(WIDE) + through
    gl_ref[...] = total
    low = total.astype(LOW)
    gc_ref[...] = low
    ga_ref[...] = dot_nt(low, wo[0]).astype(LOW)
    add_rows(s_ref, pl.program_id(0) == 0, [col_sum(for_gain), col_sum(grad), col_sum(low)])


def late_back(grad_norm, late, grad, vec, cross_a, block):
    rows, width = late.shape
    tile = spec((block, width), lambda i: (i, 0))
    return run(
        late_back_body,
        "late_back",
        (rows // block,),
        (grad_norm, late, grad, vec, cross_a),
        [
            tile,
            tile,
            tile,
            whole(vec.shape),
            spec((1, width, width), lambda i: (1, 0, 0), once=True),
        ],
        [
            ((rows, width), WIDE, tile),
            ((rows, width), LOW, tile),
            ((rows, width), LOW, tile),
            ((8, width), WIDE, spec((8, width), lambda i: (0, 0))),
        ],
        flops=2 * rows * width * width,
    )


def weights_body(count, *refs):
    out = refs[-1]
    for place in range(count):
        out[place] = dot_tn(refs[2 * place][...], refs[2 * place + 1][...]).astype(LOW)


def weight_grads(pairs, block):
    width = pairs[0][0].shape[1]
    operands, specs = [], []
    for left, right in pairs:
        operands += [left, right]
        specs += [spec((left.shape[0], block), lambda j: (0, j)), whole(right.shape)]
    return run(
        functools.partial(weights_body, len(pairs)),
        "weight_grads",
        (width // block,),
        tuple(operands),
        specs,
        [((len(pairs), width, width), LOW, spec((len(pairs), block, width), lambda j: (0, j, 0)))],
        flops=sum(2 * left.shape[0] * width * width for left, _ in pairs),
    )[0]


def mid_back_body(gq, wq, mid_ref, gl_ref, vec_ref, wo, gm_ref, gs_ref, ga_ref, s_ref):
    query = gq[...]
    grad = dot_nt(query, wq[0])
    through, for_gain = norm_backward(mid_ref[...], grad, vec_ref[1:2, :])
    total = gl_ref[...] + through
    gm_ref[...] = total
    low = total.astype(LOW)
    gs_ref[...] = low
    ga_ref[...] = dot_nt(low, wo[0]).astype(LOW)
    add_rows(
        s_ref,
        pl.program_id(0) == 0,
        [col_sum(for_gain), col_sum(grad), col_sum(low), col_sum(query)],
    )


def mid_back(grad_q, cross_a, mid, grad_late, vec, self_b, block):
    rows, width = mid.shape
    tile = spec((block, width), lambda i: (i, 0))
    weight = lambda which: spec((1, width, width), lambda i: (which, 0, 0), once=True)
    return run(
        mid_back_body,
        "mid_back",
        (rows // block,),
        (grad_q, cross_a, mid, grad_late, vec, self_b),
        [tile, weight(0), tile, tile, whole(vec.shape), weight(1)],
        [
            ((rows, width), WIDE, tile),
            ((rows, width), LOW, tile),
            ((rows, width), LOW, tile),
            ((8, width), WIDE, spec((8, width), lambda i: (0, 0))),
        ],
        flops=4 * rows * width * width,
    )


def frames_back_body(gk, gv, wk, wv, ge_ref, s_ref):
    grad_v = gv[...]
    ge_ref[...] = (dot_nt(gk[...], wk[0]) + dot_nt(grad_v, wv[0])).astype(LOW)
    add_rows(s_ref, pl.program_id(0) == 0, [col_sum(grad_v)])


def frames_back(grad_k, grad_v, cross_b, block):
    rows, width = grad_k.shape
    tile = spec((block, width), lambda i: (i, 0))
    weight = lambda which: spec((1, width, width), lambda i: (which, 0, 0), once=True)
    return run(
        frames_back_body,
        "frames_back",
        (rows // block,),
        (grad_k, grad_v, cross_b, cross_b),
        [tile, tile, weight(0), weight(1)],
        [((rows, width), LOW, tile), ((8, width), WIDE, spec((8, width), lambda i: (0, 0)))],
        flops=4 * rows * width * width,
    )


def in_back_body(gq, gk, gv, wq, wk, wv, x_ref, gm_ref, vec_ref, gi_ref, s_ref):
    query, value = gq[...], gv[...]
    grad = dot_nt(query, wq[0]) + dot_nt(gk[...], wk[0]) + dot_nt(value, wv[0])
    through, for_gain = norm_backward(x_ref[...].astype(WIDE), grad, vec_ref[0:1, :])
    gi_ref[...] = (gm_ref[...] + through).astype(LOW)
    add_rows(
        s_ref,
        pl.program_id(0) == 0,
        [col_sum(for_gain), col_sum(grad), col_sum(query), col_sum(value)],
    )


def in_back(grad_q, grad_k, grad_v, self_a, self_b, x, grad_mid, vec, block):
    rows, width = x.shape
    tile = spec((block, width), lambda i: (i, 0))
    weight = lambda which: spec((1, width, width), lambda i: (which, 0, 0), once=True)
    return run(
        in_back_body,
        "in_back",
        (rows // block,),
        (grad_q, grad_k, grad_v, self_a, self_a, self_b, x, grad_mid, vec),
        [tile, tile, tile, weight(0), weight(1), weight(0), tile, tile, whole(vec.shape)],
        [((rows, width), LOW, tile), ((8, width), WIDE, spec((8, width), lambda i: (0, 0)))],
        flops=6 * rows * width * width,
    )


def axis_bits(count):
    bits = count.bit_length() - 1
    assert 1 << bits == count
    each = (bits - 1) // 3
    x_bits = list(range(1, 1 + each))
    y_bits = list(range(1 + each, 1 + 2 * each))
    z_bits = list(range(1 + 2 * each, bits))
    return x_bits, y_bits, z_bits


def gather_stages(count, parts):
    x_bits, y_bits, z_bits = (list(reversed(b)) for b in axis_bits(count))
    if parts == 1:
        return [[(b,) for b in bits] for bits in (z_bits[:1], z_bits[1:], y_bits, x_bits, [0])]
    return [
        [(z_bits[0],)],
        [(b,) for b in z_bits[1:]],
        list(zip(y_bits, x_bits)),
        list(zip(x_bits, y_bits)),
        [(0, 0)],
    ]


def scatter_stages(count, parts):
    return [list(reversed(stage)) for stage in reversed(gather_stages(count, parts))]


def swap(values, bit, count):
    return lax.ppermute(values, "fsdp", [(i, i ^ (1 << bit)) for i in range(count)])


def own_bit(bit):
    return (lax.axis_index("fsdp") >> bit) & 1


def halves(parts):
    if len(parts) == 2:
        return parts
    middle = parts[0].shape[0] // 2
    return [parts[0][:middle], parts[0][middle:]]


class Gather:
    def __init__(self, piece, count, parts=2):
        self.count = count
        self.bits = count.bit_length() - 1
        mats, rows, width = piece.shape
        self.shape = (rows, width)
        self.parts = [piece.reshape((mats,) + (1,) * self.bits + (rows, width))]
        self.stages = gather_stages(count, parts)
        self.flight = None

    def axis(self, bit):
        return self.bits - bit

    def land(self):
        if self.flight is not None:
            parts = []
            for held, (bit, other) in zip(self.parts, self.flight):
                axis = self.axis(bit)
                parts.append(
                    jnp.where(
                        own_bit(bit) == 0,
                        jnp.concatenate([held, other], axis),
                        jnp.concatenate([other, held], axis),
                    )
                )
            self.parts = parts
            self.flight = None

    def ready(self):
        self.land()
        if len(self.stages[0][0]) == 2:
            self.parts = halves(self.parts)
        return self.parts

    def launch(self, parts):
        self.parts = parts
        for place, step in enumerate(self.stages.pop(0)):
            if place:
                self.land()
            self.flight = [(bit, swap(part, bit, self.count)) for bit, part in zip(step, self.parts)]

    def result(self):
        self.land()
        rows, width = self.shape
        return [part.reshape(part.shape[0], self.count * rows, width) for part in self.parts]


class Scatter:
    def __init__(self, parts, count):
        self.count = count
        self.bits = count.bit_length() - 1
        self.pairs = []
        for part in parts:
            mats, rows, width = part.shape
            self.shape = (rows // count, width)
            self.pairs.append((part.reshape((mats,) + (2,) * self.bits + (rows // count, width)), None))
        self.stages = scatter_stages(count, len(parts))
        self.kind = parts[0].dtype

    def pick(self, pair, bit, side):
        axis = self.bits - bit
        values = [
            lax.dynamic_slice_in_dim(v, side, 1, axis) for v in pair if v is not None
        ]
        if len(values) == 1:
            return values[0]
        return (values[0].astype(jnp.float32) + values[1].astype(jnp.float32)).astype(self.kind)

    def prepare(self):
        step = self.stages[0][0]
        if len(step) == 1 and len(self.pairs) == 2:
            self.pairs = [
                (jnp.concatenate([self.total(p, self.kind) for p in self.pairs]), None)
            ]
        return [self.pick(pair, bit, 1 - own_bit(bit)) for bit, pair in zip(step, self.pairs)]

    def ready(self):
        return self.prepare()

    def total(self, pair, kind):
        if pair[1] is None:
            return pair[0]
        return (pair[0].astype(jnp.float32) + pair[1].astype(jnp.float32)).astype(kind)

    def launch(self, sends):
        steps = self.stages.pop(0)
        for place, step in enumerate(steps):
            if place:
                self.stages.insert(0, [step])
                sends = self.prepare()
                self.stages.pop(0)
            flight = [swap(v, bit, self.count) for bit, v in zip(step, sends)]
            self.pairs = [
                (self.pick(pair, bit, own_bit(bit)), other)
                for bit, pair, other in zip(step, self.pairs, flight)
            ]

    def result(self):
        total = jnp.concatenate([self.total(p, jnp.float32) for p in self.pairs])
        return total.astype(jnp.float32).reshape((total.shape[0],) + self.shape)


def tick(chains, values=()):
    ready = [chain.ready() for chain in chains]
    ready, values = lax.optimization_barrier((ready, values))
    for chain, parts in zip(chains, ready):
        chain.launch(parts)
    return values


def shards(
    count,
    hidden_in,
    encoder_states,
    lengths,
    out_grad,
    attn_in,
    attn_out,
    fc_in,
    fc_out,
    gains,
    biases,
    ffn_bias,
):
    batch, length, width = hidden_in.shape
    rows = batch * length
    block = length // 2
    frame_rows = encoder_states.shape[1]
    share = gains.shape[1]
    ff_share = ffn_bias.shape[0]
    mats = ff_share // share

    small = jnp.concatenate([gains.reshape(-1), biases.reshape(-1), ffn_bias])
    small_count = small.shape[0]
    small_rows = -(-(small_count + 5) // 128)
    small_size = small_rows * 128
    small = jnp.pad(small, (0, small_size - small_count)).reshape(1, small_rows, 128)
    fc_in_mats = fc_in.reshape(share, count, mats, share).transpose(2, 0, 1, 3).reshape(mats, share, width)
    fc_out_mats = fc_out.reshape(mats, share, width)
    g_small = Gather(small, count, 1)
    g_self = Gather(jnp.concatenate([attn_in[0:3], attn_out[0:1]]), count)
    g_cross = Gather(jnp.concatenate([attn_in[3:4], attn_out[1:2], attn_in[4:6]]), count)
    g_ffn = Gather(jnp.concatenate([fc_in_mats, fc_out_mats]), count)

    x = hidden_in.reshape(rows, width)
    frames = encoder_states.reshape(-1, width)
    valid = jnp.arange(length)[None, :, None] < lengths[:, None, None]
    grad = jnp.where(valid, out_grad, jnp.zeros_like(out_grad)).reshape(rows, width)

    tick([g_self, g_small])
    tick([g_self, g_small])
    tick([g_self, g_small, g_cross])
    tick([g_self, g_small, g_cross, g_ffn])
    tick([g_self, g_small, g_cross, g_ffn])
    small = g_small.result()[0].astype(jnp.float32).reshape(count, small_size)
    vec = small[:, : 13 * share].reshape(count, 13, share).transpose(1, 0, 2).reshape(13, width)
    vec = jnp.pad(vec, ((0, 3), (0, 0)))
    bias = small[:, 13 * share : small_count].reshape(count, mats, share)
    bias = bias.transpose(1, 0, 2).reshape(mats, 1, width)
    self_a, self_b = g_self.result()
    norm_one, query, key, value = qkv(x, vec, self_a, self_b, block)
    query, key, value = tick([g_cross, g_ffn], (query, key, value))
    attended = attend(query, key, value, batch, True)
    mid, norm_two, square_self = mid_stage(lengths, attended, x, vec, self_b, batch, block)
    norm_two = tick([g_cross, g_ffn], norm_two)
    cross_a, cross_b = g_cross.result()
    cross_q, cross_k, cross_v = cross_stage(norm_two, frames, vec, cross_a, cross_b, batch)
    cross_attended = attend(cross_q, cross_k, cross_v, batch, False)
    late, norm_three, square_cross = late_stage(lengths, cross_attended, mid, vec, cross_a, batch, block)
    norm_three = tick([g_ffn], norm_three)
    w_in, w_out = g_ffn.result()
    grad_norm, d_in, d_out, sums_ff, result, square_rest = ffn_stage(
        lengths, norm_three, grad, bias, w_in, w_out, None, late, vec, batch, block
    )
    s_ffn = Scatter([d_in, d_out], count)
    grad_norm = tick([s_ffn], grad_norm)
    grad_late, grad_cross, grad_cross_att, sums_late = late_back(
        grad_norm, late, grad, vec, cross_a, block
    )
    grad_cross_att = tick([s_ffn], grad_cross_att)
    grad_cq, grad_ck, grad_cv = attend_back(
        cross_q, cross_k, cross_v, grad_cross_att, batch, False
    )
    d_cross_a = weight_grads([(norm_two, grad_cq), (cross_attended, grad_cross)], width // 3)
    d_cross_b = weight_grads([(frames, grad_ck), (frames, grad_cv)], width // 3)
    s_cross = Scatter([d_cross_a, d_cross_b], count)
    grad_cq = tick([s_cross], grad_cq)
    grad_mid, grad_self, grad_att, sums_mid = mid_back(
        grad_cq, cross_a, mid, grad_late, vec, self_b, block
    )
    grad_att = tick([s_cross, s_ffn], grad_att)
    grad_q, grad_k, grad_v = attend_back(query, key, value, grad_att, batch, True)
    d_self_a = weight_grads([(norm_one, grad_q), (norm_one, grad_k)], width // 3)
    d_self_b = weight_grads([(norm_one, grad_v), (attended, grad_self)], width // 3)
    s_self = Scatter([d_self_a, d_self_b], count)
    grad_q, grad_k, grad_v = tick([s_self, s_cross, s_ffn], (grad_q, grad_k, grad_v))
    grad_in, sums_one = in_back(grad_q, grad_k, grad_v, self_a, self_b, x, grad_mid, vec, block)
    grad_ck, grad_cv = tick([s_self, s_cross, s_ffn], (grad_ck, grad_cv))
    grad_frames, sums_frames = frames_back(grad_ck, grad_cv, cross_b, frame_rows)

    sum_rows = jnp.stack(
        [sums_one[0], sums_mid[0], sums_late[0]]
        + [sums_one[2], sums_one[3], sums_mid[2], sums_mid[3], sums_frames[0], sums_late[2], square_rest[2]]
        + [sums_one[1], sums_mid[1], sums_late[1]]
    )
    squares = jnp.stack([square_rest[0], square_self[0], square_cross[0], square_rest[1]])
    stats = jnp.concatenate([jnp.sum(squares, -1), jnp.sum(lengths).astype(WIDE)[None]])
    sums_ff = sums_ff.reshape(mats, count, share)
    sums = jnp.concatenate(
        [
            sum_rows.reshape(13, count, share).transpose(1, 0, 2).reshape(count, 13 * share),
            sums_ff.transpose(1, 0, 2).reshape(count, ff_share),
            jnp.broadcast_to(stats[None], (count, 5)),
        ],
        1,
    )
    sums = jnp.pad(sums, ((0, 0), (0, small_size - sums.shape[1])))
    s_small = Scatter([sums.reshape(1, count * small_rows, 128)], count)
    tick([s_self, s_cross, s_small])
    tick([s_self, s_small])
    tick([s_self, s_small])
    tick([s_small])
    tick([s_small])
    d_ffn = s_ffn.result()
    d_in_all, d_out_all = d_ffn[:mats], d_ffn[mats:]
    d_cross = s_cross.result()
    d_self = s_self.result()
    small = s_small.result().reshape(-1)
    stats = small[small_count : small_count + 5]
    rms = jnp.sqrt(stats[:4] / (stats[4] * width))
    return (
        result.reshape(hidden_in.shape),
        grad_in.reshape(hidden_in.shape),
        grad_frames.reshape(encoder_states.shape),
        jnp.concatenate([d_self[:3], d_cross[:1], d_cross[2:]]),
        jnp.concatenate([d_self[3:], d_cross[1:2]]),
        d_in_all.reshape(mats, share, count, share).transpose(1, 2, 0, 3).reshape(share, -1),
        d_out_all.reshape(ff_share, width),
        small[: 3 * share].reshape(3, share),
        small[3 * share : 13 * share].reshape(10, share),
        small[13 * share : small_count],
        rms,
    )


def solution(mesh):
    placed = (
        P("fsdp", None, None),
        P("fsdp", None, None),
        P("fsdp"),
        P("fsdp", None, None),
        P(None, "fsdp", None),
        P(None, "fsdp", None),
        P("fsdp", None),
        P("fsdp", None),
        P(None, "fsdp"),
        P(None, "fsdp"),
        P("fsdp"),
    )
    return jax.shard_map(
        functools.partial(shards, mesh.shape["fsdp"]),
        mesh=mesh,
        in_specs=placed,
        out_specs=(
            P("fsdp", None, None),
            P("fsdp", None, None),
            P("fsdp", None, None),
            P(None, "fsdp", None),
            P(None, "fsdp", None),
            P("fsdp", None),
            P("fsdp", None),
            P(None, "fsdp"),
            P(None, "fsdp"),
            P("fsdp"),
            P(),
        ),
        check_vma=False,
    )
```

```python
import functools
import math

import jax
import jax.numpy as jnp
from jax import lax
from jax.experimental import pallas as pl
from jax.experimental.pallas import tpu as pltpu
from jax.sharding import PartitionSpec as P

NORM_EPS = 1e-05
LOW = jnp.bfloat16
WIDE = jnp.float32
HEADS = 12
PAIR = 128
HALF_PAIR = 64
SCALE = 0.125


def dot_nn(left, right):
    return lax.dot_general(left, right, (((1,), (0,)), ((), ())), preferred_element_type=WIDE)


def dot_nt(left, right):
    return lax.dot_general(left, right, (((1,), (1,)), ((), ())), preferred_element_type=WIDE)


def dot_tn(left, right):
    return lax.dot_general(left, right, (((0,), (0,)), ((), ())), preferred_element_type=WIDE)


def spec(block, index, once=False):
    if once:
        return pl.BlockSpec(block, index, pipeline_mode=pl.Buffered(1))
    return pl.BlockSpec(block, index)


def run(body, name, grid, operands, in_specs, outs, scratch=(), flops=0, exps=0, limit=20):
    moved = sum(o.size * o.dtype.itemsize for o in operands)
    moved += sum(math.prod(s) * jnp.dtype(d).itemsize for s, d, _ in outs)
    return pl.pallas_call(
        body,
        name=name,
        grid=grid,
        in_specs=in_specs,
        out_specs=[o[2] for o in outs],
        out_shape=[jax.ShapeDtypeStruct(o[0], o[1]) for o in outs],
        scratch_shapes=list(scratch),
        compiler_params=pltpu.CompilerParams(
            dimension_semantics=("arbitrary",) * len(grid), vmem_limit_bytes=limit << 20
        ),
        cost_estimate=pl.CostEstimate(flops=flops, transcendentals=exps, bytes_accessed=moved),
    )(*operands)


def normalised(values):
    center = values - jnp.mean(values, -1, keepdims=True)
    spread = jnp.mean(center * center, -1, keepdims=True)
    scale = lax.rsqrt(spread + NORM_EPS)
    return center * scale, scale


def norm_backward(values, grad, gain):
    unit, scale = normalised(values)
    inner = grad * gain
    mean_inner = jnp.mean(inner, -1, keepdims=True)
    mean_unit = jnp.mean(inner * unit, -1, keepdims=True)
    return scale * (inner - mean_inner - unit * mean_unit), grad * unit


def col_sum(values):
    return jnp.sum(values.astype(WIDE), 0, keepdims=True)


def add_rows(ref, first, rows):
    @pl.when(first)
    def _():
        ref[...] = jnp.zeros_like(ref)

    for place, row in enumerate(rows):
        ref[place : place + 1, :] += row


def masked_squares(values, length_ref, step, per_seq):
    rows = values.shape[0]
    start = (step % per_seq) * rows
    index = start + lax.broadcasted_iota(jnp.int32, (rows, 1), 0)
    inside = index < length_ref[step // per_seq]
    return col_sum(jnp.where(inside, values * values, 0.0))


def qkv_body(x_ref, vec_ref, wq, wk, wv, n_ref, q_ref, k_ref, v_ref):
    unit, _ = normalised(x_ref[...].astype(WIDE))
    norm = (unit * vec_ref[0:1, :] + vec_ref[10:11, :]).astype(LOW)
    n_ref[...] = norm
    query = (dot_nn(norm, wq[0]) + vec_ref[3:4, :]).astype(LOW)
    q_ref[...] = query * jnp.asarray(SCALE, LOW)
    k_ref[...] = dot_nn(norm, wk[0]).astype(LOW)
    v_ref[...] = (dot_nn(norm, wv[0]) + vec_ref[4:5, :]).astype(LOW)


def whole(shape):
    return spec(shape, lambda *_: (0,) * len(shape), once=True)


def qkv(x, vec, self_a, self_b, block):
    rows, width = x.shape
    row = lambda i: (i, 0)
    weight = lambda which: spec((1, width, width), lambda i: (which, 0, 0), once=True)
    return run(
        qkv_body,
        "qkv",
        (rows // block,),
        (x, vec, self_a, self_a, self_b),
        [spec((block, width), row), whole(vec.shape), weight(0), weight(1), weight(0)],
        [((rows, width), LOW, spec((block, width), row))] * 4,
        flops=6 * rows * width * width,
    )


def head_lanes(values, head):
    lane = lax.broadcasted_iota(jnp.int32, (1, PAIR), 1)
    inside = lane < HALF_PAIR if head == 0 else lane >= HALF_PAIR
    return jnp.where(inside, values, jnp.zeros_like(values))


def attend_cross_body(pairs, q_ref, k_ref, v_ref, o_ref):
    for pair in range(pairs):
        lanes = slice(pair * PAIR, (pair + 1) * PAIR)
        values, keys, queries = v_ref[:, lanes], k_ref[:, lanes], q_ref[:, lanes]
        total = None
        for head in (0, 1):
            scores = dot_nt(head_lanes(queries, head), keys)
            exps = jnp.exp(scores - jnp.max(scores, -1, keepdims=True))
            probs = exps * (1.0 / jnp.sum(exps, -1, keepdims=True))
            part = dot_nn(probs.astype(LOW), head_lanes(values, head))
            total = part if total is None else total + part
        o_ref[:, lanes] = total.astype(LOW)


def attend_body(pairs, step_rows, q_ref, k_ref, v_ref, o_ref):
    length = q_ref.shape[0]
    starts = list(range(0, length, step_rows))
    for pair in range(pairs):
        lanes = slice(pair * PAIR, (pair + 1) * PAIR)
        turned = v_ref[:, lanes].T
        keys = [head_lanes(k_ref[:, lanes], head) for head in (0, 1)]
        work = []
        for start in starts:
            stop = min(start + step_rows, length)
            queries = q_ref[start:stop, lanes]
            cuts = ([(0, start)] if start else []) + [(start, stop)]
            for head in (0, 1):
                parts = []
                for low, high in cuts:
                    scores = dot_nt(keys[head][low:high], queries)
                    if low == start:
                        key_at = lax.broadcasted_iota(jnp.int32, scores.shape, 0)
                        query_at = lax.broadcasted_iota(jnp.int32, scores.shape, 1)
                        scores = jnp.where(key_at <= query_at, scores, -1e30)
                    parts.append(scores)
                work.append((start, stop, head, cuts, parts))
        tops = []
        for start, stop, head, cuts, parts in work:
            top = jnp.max(parts[0], 0, keepdims=True)
            for scores in parts[1:]:
                top = jnp.maximum(top, jnp.max(scores, 0, keepdims=True))
            tops.append(top)
        exps = [[jnp.exp(s - top) for s in item[4]] for item, top in zip(work, tops)]
        totals = [sum(jnp.sum(e, 0, keepdims=True) for e in group) for group in exps]
        outs = []
        for (start, stop, head, cuts, _), group, total in zip(work, exps, totals):
            out = None
            for (low, high), e in zip(cuts, group):
                part = dot_nn(turned[head * HALF_PAIR : (head + 1) * HALF_PAIR, low:high], e.astype(LOW))
                out = part if out is None else out + part
            outs.append(out * (1.0 / total))
        for place, start in enumerate(starts):
            stop = min(start + step_rows, length)
            both = jnp.concatenate(outs[2 * place : 2 * place + 2], 0)
            o_ref[start:stop, lanes] = both.T.astype(LOW)


def attend(q, k, v, batch, causal, pairs=6, step_rows=128):
    rows, width = q.shape
    length, frames = rows // batch, k.shape[0] // batch
    lanes = pairs * PAIR
    at = lambda b, p: (b, p)
    return run(
        functools.partial(attend_body, pairs, step_rows) if causal else functools.partial(attend_cross_body, pairs),
        "attend_self" if causal else "attend_cross",
        (batch, width // lanes),
        (q, k, v),
        [spec((length, lanes), at), spec((frames, lanes), at), spec((frames, lanes), at)],
        [((rows, width), LOW, spec((length, lanes), at))],
        flops=4 * rows * frames * width,
        exps=rows * frames * HEADS,
    )[0]


def attend_back_body(causal, pairs, step_rows, q_ref, k_ref, v_ref, g_ref, gq_ref, gk_ref, gv_ref, dk, dv):
    length = q_ref.shape[0]
    frames = k_ref.shape[0]
    starts = list(range(0, length, step_rows))
    for pair in range(pairs):
        lanes = slice(pair * PAIR, (pair + 1) * PAIR)
        keys = [head_lanes(k_ref[:, lanes], head) for head in (0, 1)]
        values = [head_lanes(v_ref[:, lanes], head) for head in (0, 1)]
        work = []
        for start in starts:
            stop = min(start + step_rows, length)
            cuts = ([(0, start)] if start else []) + [(start, stop)] if causal else [(0, frames)]
            for head in (0, 1):
                queries, grads = q_ref[start:stop, lanes], g_ref[start:stop, lanes]
                parts = []
                for low, high in cuts:
                    scores = dot_nt(keys[head][low:high], queries)
                    if causal and low == start:
                        key_at = lax.broadcasted_iota(jnp.int32, scores.shape, 0)
                        query_at = lax.broadcasted_iota(jnp.int32, scores.shape, 1)
                        scores = jnp.where(key_at <= query_at, scores, -1e30)
                    parts.append(scores)
                grad_parts = [dot_nt(values[head][low:high], grads) for low, high in cuts]
                work.append((start, stop, head, cuts, parts, grad_parts))
        probs = []
        for item in work:
            parts = item[4]
            top = jnp.max(parts[0], 0, keepdims=True)
            for scores in parts[1:]:
                top = jnp.maximum(top, jnp.max(scores, 0, keepdims=True))
            exps = [jnp.exp(scores - top) for scores in parts]
            total = 1.0 / sum(jnp.sum(e, 0, keepdims=True) for e in exps)
            probs.append([e * total for e in exps])
        scores = []
        for item, group in zip(work, probs):
            weighted = [p * g for p, g in zip(group, item[5])]
            inner = sum(jnp.sum(w, 0, keepdims=True) for w in weighted)
            scores.append([(w - p * inner).astype(LOW) for w, p in zip(weighted, group)])
        grad_q = {}
        for (start, stop, head, cuts, _, _), group, low_scores in zip(work, probs, scores):
            queries = head_lanes(q_ref[start:stop, lanes], head)
            grads = head_lanes(g_ref[start:stop, lanes], head)
            for (low, high), p, s in zip(cuts, group, low_scores):
                part_v = dot_nn(p.astype(LOW), grads)
                part_k = dot_nn(s, queries)
                part_q = dot_tn(s, keys[head][low:high])
                grad_q[start] = part_q if start not in grad_q else grad_q[start] + part_q
                if head == 0 and (low == start or not causal and start == 0):
                    dv[low:high, :] = part_v
                    dk[low:high, :] = part_k
                else:
                    dv[low:high, :] += part_v
                    dk[low:high, :] += part_k
        for start, total in grad_q.items():
            gq_ref[start : start + total.shape[0], lanes] = (total * SCALE).astype(LOW)
        gk_ref[:, lanes] = dk[...].astype(LOW)
        gv_ref[:, lanes] = dv[...].astype(LOW)


def attend_back(q, k, v, grad, batch, causal, pairs=6):
    rows, width = q.shape
    length, frames = rows // batch, k.shape[0] // batch
    lanes = pairs * PAIR
    at = lambda b, p: (b, p)
    long, short = spec((length, lanes), at), spec((frames, lanes), at)
    return run(
        functools.partial(attend_back_body, causal, pairs, 128 if causal else length),
        "attend_self_back" if causal else "attend_cross_back",
        (batch, width // lanes),
        (q, k, v, grad),
        [long, short, short, long],
        [((rows, width), LOW, long), (k.shape, LOW, short), (k.shape, LOW, short)],
        [pltpu.VMEM((frames, PAIR), WIDE)] * 2,
        flops=10 * rows * frames * width,
        exps=rows * frames * HEADS,
    )


def mid_body(per_seq, len_ref, a_ref, x_ref, vec_ref, wo, mid_ref, n_ref, s_ref):
    step = pl.program_id(0)
    branch = dot_nn(a_ref[...], wo[0]) + vec_ref[5:6, :]
    mid = x_ref[...].astype(WIDE) + branch
    mid_ref[...] = mid
    unit, _ = normalised(mid)
    n_ref[...] = (unit * vec_ref[1:2, :] + vec_ref[11:12, :]).astype(LOW)
    add_rows(s_ref, step == 0, [masked_squares(branch, len_ref, step, per_seq)])


def smem():
    return pl.BlockSpec(memory_space=pltpu.SMEM)


def mid_stage(lengths, attended, x, vec, self_b, batch, block):
    rows, width = x.shape
    weight = spec((1, width, width), lambda i: (1, 0, 0), once=True)
    tile = spec((block, width), lambda i: (i, 0))
    return run(
        functools.partial(mid_body, rows // batch // block),
        "mid_stage",
        (rows // block,),
        (lengths, attended, x, vec, self_b),
        [smem(), tile, tile, whole(vec.shape), weight],
        [
            ((rows, width), WIDE, tile),
            ((rows, width), LOW, tile),
            ((8, width), WIDE, spec((8, width), lambda i: (0, 0))),
        ],
        flops=2 * rows * width * width,
    )


def cross_body(n_ref, f_ref, vec_ref, wq, wk, wv, q_ref, k_ref, v_ref):
    query = (dot_nn(n_ref[...], wq[0]) + vec_ref[6:7, :]).astype(LOW)
    q_ref[...] = query * jnp.asarray(SCALE, LOW)
    frames = f_ref[...]
    k_ref[...] = dot_nn(frames, wk[0]).astype(LOW)
    v_ref[...] = (dot_nn(frames, wv[0]) + vec_ref[7:8, :]).astype(LOW)


def cross_stage(norm, frames, vec, cross_a, cross_b, batch):
    width = norm.shape[1]
    rows, frame_rows = norm.shape[0], frames.shape[0]
    long = spec((rows // batch, width), lambda i: (i, 0))
    short = spec((frame_rows // batch, width), lambda i: (i, 0))
    weight = lambda which: spec((1, width, width), lambda i: (which, 0, 0), once=True)
    return run(
        cross_body,
        "cross_stage",
        (batch,),
        (norm, frames, vec, cross_a, cross_b, cross_b),
        [long, short, whole(vec.shape), weight(0), weight(0), weight(1)],
        [((rows, width), LOW, long), ((frame_rows, width), LOW, short), ((frame_rows, width), LOW, short)],
        flops=(2 * rows + 4 * frame_rows) * width * width,
    )


def late_body(per_seq, len_ref, a_ref, mid_ref, vec_ref, wo, late_ref, n_ref, s_ref):
    step = pl.program_id(0)
    branch = dot_nn(a_ref[...], wo[0]) + vec_ref[8:9, :]
    late = mid_ref[...] + branch
    late_ref[...] = late
    unit, _ = normalised(late)
    n_ref[...] = (unit * vec_ref[2:3, :] + vec_ref[12:13, :]).astype(LOW)
    add_rows(s_ref, step == 0, [masked_squares(branch, len_ref, step, per_seq)])


def late_stage(lengths, attended, mid, vec, cross_a, batch, block):
    rows, width = mid.shape
    tile = spec((block, width), lambda i: (i, 0))
    return run(
        functools.partial(late_body, rows // batch // block),
        "late_stage",
        (rows // block,),
        (lengths, attended, mid, vec, cross_a),
        [smem(), tile, tile, whole(vec.shape), spec((1, width, width), lambda i: (1, 0, 0), once=True)],
        [
            ((rows, width), WIDE, tile),
            ((rows, width), LOW, tile),
            ((8, width), WIDE, spec((8, width), lambda i: (0, 0))),
        ],
        flops=2 * rows * width * width,
    )


def ffn_body(first, last, batch, block, len_ref, n_ref, g_ref, b_ref, wi_ref, wo_ref, *refs):
    refs = list(refs)
    before = [] if first else [refs.pop(0), refs.pop(0)]
    late_ref, vec_ref = (refs.pop(0), refs.pop(0)) if last else (None, None)
    gn_ref, di_ref, do_ref, sf_ref, f_ref = refs[:5]
    rest = refs[5:]
    s_ref = rest.pop(0) if last else None
    hidden_ref, pre_ref = rest[:2]
    acc_ref = rest[2] if last else f_ref
    step = pl.program_id(0)
    rows = n_ref.shape[0]

    @pl.when(step == 0)
    def _():
        if first:
            acc_ref[...] = jnp.zeros_like(acc_ref)
            gn_ref[...] = jnp.zeros_like(gn_ref)
        else:
            acc_ref[...] = before[0][...]
            gn_ref[...] = before[1][...]

    def chunk(place, carry):
        at = pl.ds(pl.multiple_of(place * block, block), block)
        pre = dot_nn(n_ref[at, :], wi_ref[0]) + b_ref[0]
        below = 0.5 + 0.5 * lax.erf(pre * (0.5**0.5))
        density = jnp.exp(-0.5 * pre * pre) * (1.0 / math.sqrt(2.0 * math.pi))
        hidden = (pre * below).astype(LOW)
        hidden_ref[at, :] = hidden
        acc_ref[at, :] += dot_nn(hidden, wo_ref[0])
        grad = dot_nt(g_ref[at, :], wo_ref[0])
        grad = (grad * (below + pre * density)).astype(LOW)
        pre_ref[at, :] = grad
        gn_ref[at, :] += dot_nt(grad, wi_ref[0])
        return carry

    lax.fori_loop(0, rows // block, chunk, 0)
    sf_ref[0] = col_sum(pre_ref[...])
    di_ref[0] = dot_tn(n_ref[...], pre_ref[...]).astype(LOW)
    do_ref[0] = dot_tn(hidden_ref[...], g_ref[...]).astype(LOW)
    if last:
        @pl.when(step == pl.num_programs(0) - 1)
        def _():
            s_ref[...] = jnp.zeros_like(s_ref)

            def finish(place, carry):
                at = pl.ds(pl.multiple_of(place * block, block), block)
                branch = acc_ref[at, :] + vec_ref[9:10, :]
                result = late_ref[at, :] + branch
                f_ref[at, :] = result.astype(LOW)
                per_seq = rows // batch // block
                s_ref[0:1, :] += masked_squares(result, len_ref, place, per_seq)
                s_ref[1:2, :] += masked_squares(branch, len_ref, place, per_seq)
                s_ref[2:3, :] += col_sum(g_ref[at, :])
                return carry

            lax.fori_loop(0, rows // block, finish, 0)


def ffn_stage(lengths, norm, grad, bias, w_in, w_out, before, late, vec, batch, block):
    rows, width = norm.shape
    mats = w_in.shape[0]
    first, last = before is None, late is not None
    mat = spec((1, width, width), lambda j: (j, 0, 0))
    line = spec((1, 1, width), lambda j: (j, 0, 0))
    operands = [lengths, norm, grad, bias, w_in, w_out]
    specs = [smem(), whole(norm.shape), whole(grad.shape), line, mat, mat]
    if not first:
        operands += list(before)
        specs += [whole((rows, width))] * 2
    if last:
        operands += [late, vec]
        specs += [whole((rows, width)), whole(vec.shape)]
    fixed = whole((rows, width))
    outs = [
        ((rows, width), WIDE, fixed),
        ((mats, width, width), LOW, mat),
        ((mats, width, width), LOW, mat),
        ((mats, 1, width), WIDE, line),
        ((rows, width), LOW if last else WIDE, fixed),
    ]
    scratch = [pltpu.VMEM((rows, width), LOW)] * 2
    if last:
        outs.append(((8, width), WIDE, whole((8, width))))
        scratch.append(pltpu.VMEM((rows, width), WIDE))
    return run(
        functools.partial(ffn_body, first, last, batch, block),
        "ffn_stage",
        (mats,),
        tuple(operands),
        specs,
        outs,
        scratch,
        flops=12 * rows * width * width * mats,
        exps=2 * rows * width * mats,
        limit=44,
    )


def late_back_body(gn_ref, late_ref, og_ref, vec_ref, wo, gl_ref, gc_ref, ga_ref, s_ref):
    grad = gn_ref[...]
    through, for_gain = norm_backward(late_ref[...], grad, vec_ref[2:3, :])
    total = og_ref[...].astype(WIDE) + through
    gl_ref[...] = total
    low = total.astype(LOW)
    gc_ref[...] = low
    ga_ref[...] = dot_nt(low, wo[0]).astype(LOW)
    add_rows(s_ref, pl.program_id(0) == 0, [col_sum(for_gain), col_sum(grad), col_sum(low)])


def late_back(grad_norm, late, grad, vec, cross_a, block):
    rows, width = late.shape
    tile = spec((block, width), lambda i: (i, 0))
    return run(
        late_back_body,
        "late_back",
        (rows // block,),
        (grad_norm, late, grad, vec, cross_a),
        [
            tile,
            tile,
            tile,
            whole(vec.shape),
            spec((1, width, width), lambda i: (1, 0, 0), once=True),
        ],
        [
            ((rows, width), WIDE, tile),
            ((rows, width), LOW, tile),
            ((rows, width), LOW, tile),
            ((8, width), WIDE, spec((8, width), lambda i: (0, 0))),
        ],
        flops=2 * rows * width * width,
    )


def weights_body(count, *refs):
    out = refs[-1]
    for place in range(count):
        out[place] = dot_tn(refs[2 * place][...], refs[2 * place + 1][...]).astype(LOW)


def weight_grads(pairs, block):
    width = pairs[0][0].shape[1]
    operands, specs = [], []
    for left, right in pairs:
        operands += [left, right]
        specs += [spec((left.shape[0], block), lambda j: (0, j)), whole(right.shape)]
    return run(
        functools.partial(weights_body, len(pairs)),
        "weight_grads",
        (width // block,),
        tuple(operands),
        specs,
        [((len(pairs), width, width), LOW, spec((len(pairs), block, width), lambda j: (0, j, 0)))],
        flops=sum(2 * left.shape[0] * width * width for left, _ in pairs),
    )[0]


def mid_back_body(gq, wq, mid_ref, gl_ref, vec_ref, wo, gm_ref, gs_ref, ga_ref, s_ref):
    query = gq[...]
    grad = dot_nt(query, wq[0])
    through, for_gain = norm_backward(mid_ref[...], grad, vec_ref[1:2, :])
    total = gl_ref[...] + through
    gm_ref[...] = total
    low = total.astype(LOW)
    gs_ref[...] = low
    ga_ref[...] = dot_nt(low, wo[0]).astype(LOW)
    add_rows(
        s_ref,
        pl.program_id(0) == 0,
        [col_sum(for_gain), col_sum(grad), col_sum(low), col_sum(query)],
    )


def mid_back(grad_q, cross_a, mid, grad_late, vec, self_b, block):
    rows, width = mid.shape
    tile = spec((block, width), lambda i: (i, 0))
    weight = lambda which: spec((1, width, width), lambda i: (which, 0, 0), once=True)
    return run(
        mid_back_body,
        "mid_back",
        (rows // block,),
        (grad_q, cross_a, mid, grad_late, vec, self_b),
        [tile, weight(0), tile, tile, whole(vec.shape), weight(1)],
        [
            ((rows, width), WIDE, tile),
            ((rows, width), LOW, tile),
            ((rows, width), LOW, tile),
            ((8, width), WIDE, spec((8, width), lambda i: (0, 0))),
        ],
        flops=4 * rows * width * width,
    )


def frames_back_body(gk, gv, wk, wv, ge_ref, s_ref):
    grad_v = gv[...]
    ge_ref[...] = (dot_nt(gk[...], wk[0]) + dot_nt(grad_v, wv[0])).astype(LOW)
    add_rows(s_ref, pl.program_id(0) == 0, [col_sum(grad_v)])


def frames_back(grad_k, grad_v, cross_b, block):
    rows, width = grad_k.shape
    tile = spec((block, width), lambda i: (i, 0))
    weight = lambda which: spec((1, width, width), lambda i: (which, 0, 0), once=True)
    return run(
        frames_back_body,
        "frames_back",
        (rows // block,),
        (grad_k, grad_v, cross_b, cross_b),
        [tile, tile, weight(0), weight(1)],
        [((rows, width), LOW, tile), ((8, width), WIDE, spec((8, width), lambda i: (0, 0)))],
        flops=4 * rows * width * width,
    )


def in_back_body(gq, gk, gv, wq, wk, wv, x_ref, gm_ref, vec_ref, gi_ref, s_ref):
    query, value = gq[...], gv[...]
    grad = dot_nt(query, wq[0]) + dot_nt(gk[...], wk[0]) + dot_nt(value, wv[0])
    through, for_gain = norm_backward(x_ref[...].astype(WIDE), grad, vec_ref[0:1, :])
    gi_ref[...] = (gm_ref[...] + through).astype(LOW)
    add_rows(
        s_ref,
        pl.program_id(0) == 0,
        [col_sum(for_gain), col_sum(grad), col_sum(query), col_sum(value)],
    )


def in_back(grad_q, grad_k, grad_v, self_a, self_b, x, grad_mid, vec, block):
    rows, width = x.shape
    tile = spec((block, width), lambda i: (i, 0))
    weight = lambda which: spec((1, width, width), lambda i: (which, 0, 0), once=True)
    return run(
        in_back_body,
        "in_back",
        (rows // block,),
        (grad_q, grad_k, grad_v, self_a, self_a, self_b, x, grad_mid, vec),
        [tile, tile, tile, weight(0), weight(1), weight(0), tile, tile, whole(vec.shape)],
        [((rows, width), LOW, tile), ((8, width), WIDE, spec((8, width), lambda i: (0, 0)))],
        flops=6 * rows * width * width,
    )


def axis_bits(count):
    bits = count.bit_length() - 1
    assert 1 << bits == count
    each = (bits - 1) // 3
    x_bits = list(range(1, 1 + each))
    y_bits = list(range(1 + each, 1 + 2 * each))
    z_bits = list(range(1 + 2 * each, bits))
    return x_bits, y_bits, z_bits


def gather_stages(count, parts):
    x_bits, y_bits, z_bits = (list(reversed(b)) for b in axis_bits(count))
    if parts == 1:
        return [[(b,) for b in bits] for bits in (z_bits[:1], z_bits[1:], y_bits, x_bits, [0])]
    return [
        [(z_bits[0],)],
        [(b,) for b in z_bits[1:]],
        list(zip(y_bits, x_bits)),
        list(zip(x_bits, y_bits)),
        [(0, 0)],
    ]


def scatter_stages(count, parts):
    return [list(reversed(stage)) for stage in reversed(gather_stages(count, parts))]


def swap(values, bit, count):
    return lax.ppermute(values, "fsdp", [(i, i ^ (1 << bit)) for i in range(count)])


def own_bit(bit):
    return (lax.axis_index("fsdp") >> bit) & 1


def weave_body(parts, core_ref, *refs):
    for part in range(parts):
        out = refs[2 * parts + part]
        out[0, :, core_ref[0]] = refs[part][:, 0]
        out[0, :, 1 - core_ref[0]] = refs[parts + part][:, 0]


def weave(held, other, core):
    groups, mats, rows, width = held[0].shape
    parts = len(held)
    half = spec((groups, 1, rows, width), lambda i: (0, i, 0, 0))
    both = spec((1, groups, 2, rows, width), lambda i: (i, 0, 0, 0, 0))
    return run(
        functools.partial(weave_body, parts),
        "weave",
        (mats,),
        (core, *held, *other),
        [smem()] + [half] * (2 * parts),
        [((mats, groups, 2, rows, width), held[0].dtype, both)] * parts,
    )


class Gather:
    def __init__(self, piece, count, parts=2):
        self.count = count
        self.bits = count.bit_length() - 1
        mats, rows, width = piece.shape
        self.shape = (rows, width)
        self.parts = [piece.reshape((1,) * self.bits + (mats, rows, width))]
        self.stages = gather_stages(count, parts)
        self.flight = None

    def land(self):
        if self.flight is not None:
            parts = []
            for held, (bit, other) in zip(self.parts, self.flight):
                axis = self.bits - 1 - bit
                parts.append(
                    jnp.where(
                        own_bit(bit) == 0,
                        jnp.concatenate([held, other], axis),
                        jnp.concatenate([other, held], axis),
                    )
                )
            self.parts = parts
            self.flight = None

    def ready(self):
        self.land()
        if len(self.stages[0][0]) == 2 and len(self.parts) == 1:
            self.parts = jnp.split(self.parts[0], 2, self.bits)
        return self.parts

    def launch(self, parts):
        self.parts = parts
        for place, step in enumerate(self.stages.pop(0)):
            if place:
                self.land()
            self.flight = [(bit, swap(part, bit, self.count)) for bit, part in zip(step, self.parts)]

    def result(self):
        rows, width = self.shape
        merged = lambda v: v.reshape((self.count // 2,) + v.shape[self.bits :])
        held = [merged(v) for v in self.parts]
        other = [merged(v) for _, v in self.flight]
        if len(held) == 1:
            self.land()
            return [self.parts[0].reshape(self.count * rows, width)]
        done = weave(held, other, own_bit(0).astype(jnp.int32).reshape(1))
        return [v.reshape(v.shape[0], self.count * rows, width) for v in done]


class Scatter:
    def __init__(self, parts, count):
        self.count = count
        self.bits = count.bit_length() - 1
        self.pairs = []
        for part in parts:
            mats, rows, width = part.shape
            self.shape = (rows // count, width)
            self.pairs.append((part.reshape((mats,) + (2,) * self.bits + (rows // count, width)), None))
        self.stages = scatter_stages(count, len(parts))
        self.kind = parts[0].dtype

    def pick(self, pair, bit, side):
        axis = self.bits - bit
        values = [
            lax.dynamic_slice_in_dim(v, side, 1, axis) for v in pair if v is not None
        ]
        if len(values) == 1:
            return values[0]
        return (values[0].astype(jnp.float32) + values[1].astype(jnp.float32)).astype(self.kind)

    def prepare(self):
        step = self.stages[0][0]
        if len(step) == 1 and len(self.pairs) == 2:
            self.pairs = [
                (jnp.concatenate([self.total(p, self.kind) for p in self.pairs]), None)
            ]
        return [self.pick(pair, bit, 1 - own_bit(bit)) for bit, pair in zip(step, self.pairs)]

    def ready(self):
        return self.prepare()

    def total(self, pair, kind):
        if pair[1] is None:
            return pair[0]
        return (pair[0].astype(jnp.float32) + pair[1].astype(jnp.float32)).astype(kind)

    def launch(self, sends):
        steps = self.stages.pop(0)
        for place, step in enumerate(steps):
            if place:
                self.stages.insert(0, [step])
                sends = self.prepare()
                self.stages.pop(0)
            flight = [swap(v, bit, self.count) for bit, v in zip(step, sends)]
            self.pairs = [
                (self.pick(pair, bit, own_bit(bit)), other)
                for bit, pair, other in zip(step, self.pairs, flight)
            ]

    def result(self):
        total = jnp.concatenate([self.total(p, jnp.float32) for p in self.pairs])
        return total.astype(jnp.float32).reshape((total.shape[0],) + self.shape)


def tick(chains, values=()):
    ready = [chain.ready() for chain in chains]
    ready, values = lax.optimization_barrier((ready, values))
    for chain, parts in zip(chains, ready):
        chain.launch(parts)
    return values


def shards(
    count,
    hidden_in,
    encoder_states,
    lengths,
    out_grad,
    attn_in,
    attn_out,
    fc_in,
    fc_out,
    gains,
    biases,
    ffn_bias,
):
    batch, length, width = hidden_in.shape
    rows = batch * length
    block = length // 2
    frame_rows = encoder_states.shape[1]
    share = gains.shape[1]
    ff_share = ffn_bias.shape[0]
    mats = ff_share // share

    small = jnp.concatenate([gains.reshape(-1), biases.reshape(-1), ffn_bias])
    small_count = small.shape[0]
    small_rows = -(-(small_count + 5) // 128)
    small_size = small_rows * 128
    small = jnp.pad(small, (0, small_size - small_count)).reshape(1, small_rows, 128)
    fc_in_mats = fc_in.reshape(share, count, mats, share).transpose(2, 0, 1, 3).reshape(mats, share, width)
    fc_out_mats = fc_out.reshape(mats, share, width)
    g_small = Gather(small, count, 1)
    g_self = Gather(jnp.concatenate([attn_in[0:3], attn_out[0:1]]), count)
    g_cross = Gather(jnp.concatenate([attn_in[3:4], attn_out[1:2], attn_in[4:6]]), count)
    g_ffn = Gather(jnp.concatenate([fc_in_mats, fc_out_mats]), count)

    x = hidden_in.reshape(rows, width)
    frames = encoder_states.reshape(-1, width)
    valid = jnp.arange(length)[None, :, None] < lengths[:, None, None]
    grad = jnp.where(valid, out_grad, jnp.zeros_like(out_grad)).reshape(rows, width)

    tick([g_self, g_small])
    tick([g_self, g_small])
    tick([g_self, g_small, g_cross])
    tick([g_self, g_small, g_cross, g_ffn])
    tick([g_self, g_small, g_cross, g_ffn])
    small = g_small.result()[0].astype(jnp.float32).reshape(count, small_size)
    vec = small[:, : 13 * share].reshape(count, 13, share).transpose(1, 0, 2).reshape(13, width)
    vec = jnp.pad(vec, ((0, 3), (0, 0)))
    bias = small[:, 13 * share : small_count].reshape(count, mats, share)
    bias = bias.transpose(1, 0, 2).reshape(mats, 1, width)
    self_a, self_b = g_self.result()
    norm_one, query, key, value = qkv(x, vec, self_a, self_b, block)
    query, key, value = tick([g_cross, g_ffn], (query, key, value))
    attended = attend(query, key, value, batch, True)
    mid, norm_two, square_self = mid_stage(lengths, attended, x, vec, self_b, batch, block)
    norm_two = tick([g_cross, g_ffn], norm_two)
    cross_a, cross_b = g_cross.result()
    cross_q, cross_k, cross_v = cross_stage(norm_two, frames, vec, cross_a, cross_b, batch)
    cross_attended = attend(cross_q, cross_k, cross_v, batch, False)
    late, norm_three, square_cross = late_stage(lengths, cross_attended, mid, vec, cross_a, batch, block)
    norm_three = tick([g_ffn], norm_three)
    w_in, w_out = g_ffn.result()
    grad_norm, d_in, d_out, sums_ff, result, square_rest = ffn_stage(
        lengths, norm_three, grad, bias, w_in, w_out, None, late, vec, batch, block
    )
    s_ffn = Scatter([d_in, d_out], count)
    grad_norm = tick([s_ffn], grad_norm)
    grad_late, grad_cross, grad_cross_att, sums_late = late_back(
        grad_norm, late, grad, vec, cross_a, block
    )
    grad_cross_att = tick([s_ffn], grad_cross_att)
    grad_cq, grad_ck, grad_cv = attend_back(
        cross_q, cross_k, cross_v, grad_cross_att, batch, False
    )
    d_cross_a = weight_grads([(norm_two, grad_cq), (cross_attended, grad_cross)], width // 3)
    d_cross_b = weight_grads([(frames, grad_ck), (frames, grad_cv)], width // 3)
    s_cross = Scatter([d_cross_a, d_cross_b], count)
    grad_cq, grad_ck, grad_cv = tick([s_cross], (grad_cq, grad_ck, grad_cv))
    grad_mid, grad_self, grad_att, sums_mid = mid_back(
        grad_cq, cross_a, mid, grad_late, vec, self_b, block
    )
    grad_frames, sums_frames = frames_back(grad_ck, grad_cv, cross_b, frame_rows)
    grad_att, grad_frames = tick([s_cross, s_ffn], (grad_att, grad_frames))
    grad_q, grad_k, grad_v = attend_back(query, key, value, grad_att, batch, True)
    d_self_a = weight_grads([(norm_one, grad_q), (norm_one, grad_k)], width // 3)
    d_self_b = weight_grads([(norm_one, grad_v), (attended, grad_self)], width // 3)
    s_self = Scatter([d_self_a, d_self_b], count)
    grad_q, grad_k, grad_v = tick([s_self, s_cross, s_ffn], (grad_q, grad_k, grad_v))
    grad_in, sums_one = in_back(grad_q, grad_k, grad_v, self_a, self_b, x, grad_mid, vec, block)

    sums_one = tick([s_self, s_cross, s_ffn], sums_one)
    sum_rows = jnp.stack(
        [sums_one[0], sums_mid[0], sums_late[0]]
        + [sums_one[2], sums_one[3], sums_mid[2], sums_mid[3], sums_frames[0], sums_late[2], square_rest[2]]
        + [sums_one[1], sums_mid[1], sums_late[1]]
    )
    squares = jnp.stack([square_rest[0], square_self[0], square_cross[0], square_rest[1]])
    stats = jnp.concatenate([jnp.sum(squares, -1), jnp.sum(lengths).astype(WIDE)[None]])
    sums_ff = sums_ff.reshape(mats, count, share)
    sums = jnp.concatenate(
        [
            sum_rows.reshape(13, count, share).transpose(1, 0, 2).reshape(count, 13 * share),
            sums_ff.transpose(1, 0, 2).reshape(count, ff_share),
            jnp.broadcast_to(stats[None], (count, 5)),
        ],
        1,
    )
    sums = jnp.pad(sums, ((0, 0), (0, small_size - sums.shape[1])))
    s_small = Scatter([sums.reshape(1, count * small_rows, 128)], count)
    tick([s_small])
    tick([s_small])
    tick([s_self, s_cross, s_small])
    tick([s_self, s_small])
    tick([s_self, s_small])
    d_ffn = s_ffn.result()
    d_in_all, d_out_all = d_ffn[:mats], d_ffn[mats:]
    d_cross = s_cross.result()
    d_self = s_self.result()
    small = s_small.result().reshape(-1)
    stats = small[small_count : small_count + 5]
    rms = jnp.sqrt(stats[:4] / (stats[4] * width))
    return (
        result.reshape(hidden_in.shape),
        grad_in.reshape(hidden_in.shape),
        grad_frames.reshape(encoder_states.shape),
        jnp.concatenate([d_self[:3], d_cross[:1], d_cross[2:]]),
        jnp.concatenate([d_self[3:], d_cross[1:2]]),
        d_in_all.reshape(mats, share, count, share).transpose(1, 2, 0, 3).reshape(share, -1),
        d_out_all.reshape(ff_share, width),
        small[: 3 * share].reshape(3, share),
        small[3 * share : 13 * share].reshape(10, share),
        small[13 * share : small_count],
        rms,
    )


def solution(mesh):
    placed = (
        P("fsdp", None, None),
        P("fsdp", None, None),
        P("fsdp"),
        P("fsdp", None, None),
        P(None, "fsdp", None),
        P(None, "fsdp", None),
        P("fsdp", None),
        P("fsdp", None),
        P(None, "fsdp"),
        P(None, "fsdp"),
        P("fsdp"),
    )
    return jax.shard_map(
        functools.partial(shards, mesh.shape["fsdp"]),
        mesh=mesh,
        in_specs=placed,
        out_specs=(
            P("fsdp", None, None),
            P("fsdp", None, None),
            P("fsdp", None, None),
            P(None, "fsdp", None),
            P(None, "fsdp", None),
            P("fsdp", None),
            P("fsdp", None),
            P(None, "fsdp"),
            P(None, "fsdp"),
            P("fsdp"),
            P(),
        ),
        check_vma=False,
    )
```

```python
import functools
import math

import jax
import jax.numpy as jnp
from jax import lax
from jax.experimental import pallas as pl
from jax.experimental.pallas import tpu as pltpu
from jax.sharding import PartitionSpec as P

NORM_EPS = 1e-05
LOW = jnp.bfloat16
WIDE = jnp.float32
HEADS = 12
PAIR = 128
HALF_PAIR = 64
SCALE = 0.125


def dot_nn(left, right):
    return lax.dot_general(left, right, (((1,), (0,)), ((), ())), preferred_element_type=WIDE)


def dot_nt(left, right):
    return lax.dot_general(left, right, (((1,), (1,)), ((), ())), preferred_element_type=WIDE)


def dot_tn(left, right):
    return lax.dot_general(left, right, (((0,), (0,)), ((), ())), preferred_element_type=WIDE)


def spec(block, index, once=False):
    if once:
        return pl.BlockSpec(block, index, pipeline_mode=pl.Buffered(1))
    return pl.BlockSpec(block, index)


def run(body, name, grid, operands, in_specs, outs, scratch=(), flops=0, exps=0, limit=14):
    moved = sum(o.size * o.dtype.itemsize for o in operands)
    moved += sum(math.prod(s) * jnp.dtype(d).itemsize for s, d, _ in outs)
    return pl.pallas_call(
        body,
        name=name,
        grid=grid,
        in_specs=in_specs,
        out_specs=[o[2] for o in outs],
        out_shape=[jax.ShapeDtypeStruct(o[0], o[1]) for o in outs],
        scratch_shapes=list(scratch),
        compiler_params=pltpu.CompilerParams(
            dimension_semantics=("arbitrary",) * len(grid), vmem_limit_bytes=limit << 20
        ),
        cost_estimate=pl.CostEstimate(flops=flops, transcendentals=exps, bytes_accessed=moved),
    )(*operands)


def normalised(values):
    center = values - jnp.mean(values, -1, keepdims=True)
    spread = jnp.mean(center * center, -1, keepdims=True)
    scale = lax.rsqrt(spread + NORM_EPS)
    return center * scale, scale


def norm_backward(values, grad, gain):
    unit, scale = normalised(values)
    inner = grad * gain
    mean_inner = jnp.mean(inner, -1, keepdims=True)
    mean_unit = jnp.mean(inner * unit, -1, keepdims=True)
    return scale * (inner - mean_inner - unit * mean_unit), grad * unit


def col_sum(values):
    return jnp.sum(values.astype(WIDE), 0, keepdims=True)


def add_rows(ref, first, rows):
    @pl.when(first)
    def _():
        ref[...] = jnp.zeros_like(ref)

    for place, row in enumerate(rows):
        ref[place : place + 1, :] += row


def masked_squares(values, length_ref, step, per_seq):
    rows = values.shape[0]
    start = (step % per_seq) * rows
    index = start + lax.broadcasted_iota(jnp.int32, (rows, 1), 0)
    inside = index < length_ref[step // per_seq]
    return col_sum(jnp.where(inside, values * values, 0.0))


def qkv_body(x_ref, vec_ref, wq, wk, wv, n_ref, q_ref, k_ref, v_ref):
    unit, _ = normalised(x_ref[...].astype(WIDE))
    norm = (unit * vec_ref[0:1, :] + vec_ref[10:11, :]).astype(LOW)
    n_ref[...] = norm
    query = (dot_nn(norm, wq[0]) + vec_ref[3:4, :]).astype(LOW)
    q_ref[...] = query * jnp.asarray(SCALE, LOW)
    k_ref[...] = dot_nn(norm, wk[0]).astype(LOW)
    v_ref[...] = (dot_nn(norm, wv[0]) + vec_ref[4:5, :]).astype(LOW)


def whole(shape):
    return spec(shape, lambda *_: (0,) * len(shape), once=True)


def qkv(x, vec, self_a, self_b, block):
    rows, width = x.shape
    row = lambda i: (i, 0)
    weight = lambda which: spec((1, width, width), lambda i: (which, 0, 0), once=True)
    return run(
        qkv_body,
        "qkv",
        (rows // block,),
        (x, vec, self_a, self_a, self_b),
        [spec((block, width), row), whole(vec.shape), weight(0), weight(1), weight(0)],
        [((rows, width), LOW, spec((block, width), row))] * 4,
        flops=6 * rows * width * width,
    )


def head_lanes(values, head):
    lane = lax.broadcasted_iota(jnp.int32, (1, PAIR), 1)
    inside = lane < HALF_PAIR if head == 0 else lane >= HALF_PAIR
    return jnp.where(inside, values, jnp.zeros_like(values))


def attend_cross_body(pairs, q_ref, k_ref, v_ref, o_ref):
    for pair in range(pairs):
        lanes = slice(pair * PAIR, (pair + 1) * PAIR)
        values, keys, queries = v_ref[:, lanes], k_ref[:, lanes], q_ref[:, lanes]
        total = None
        for head in (0, 1):
            scores = dot_nt(head_lanes(queries, head), keys)
            exps = jnp.exp(scores - jnp.max(scores, -1, keepdims=True))
            probs = exps * (1.0 / jnp.sum(exps, -1, keepdims=True))
            part = dot_nn(probs.astype(LOW), head_lanes(values, head))
            total = part if total is None else total + part
        o_ref[:, lanes] = total.astype(LOW)


def attend_body(pairs, step_rows, q_ref, k_ref, v_ref, o_ref):
    length = q_ref.shape[0]
    starts = list(range(0, length, step_rows))
    for pair in range(pairs):
        lanes = slice(pair * PAIR, (pair + 1) * PAIR)
        turned = v_ref[:, lanes].T
        keys = [head_lanes(k_ref[:, lanes], head) for head in (0, 1)]
        work = []
        for start in starts:
            stop = min(start + step_rows, length)
            queries = q_ref[start:stop, lanes]
            cuts = ([(0, start)] if start else []) + [(start, stop)]
            for head in (0, 1):
                parts = []
                for low, high in cuts:
                    scores = dot_nt(keys[head][low:high], queries)
                    if low == start:
                        key_at = lax.broadcasted_iota(jnp.int32, scores.shape, 0)
                        query_at = lax.broadcasted_iota(jnp.int32, scores.shape, 1)
                        scores = jnp.where(key_at <= query_at, scores, -1e30)
                    parts.append(scores)
                work.append((start, stop, head, cuts, parts))
        tops = []
        for start, stop, head, cuts, parts in work:
            top = jnp.max(parts[0], 0, keepdims=True)
            for scores in parts[1:]:
                top = jnp.maximum(top, jnp.max(scores, 0, keepdims=True))
            tops.append(top)
        exps = [[jnp.exp(s - top) for s in item[4]] for item, top in zip(work, tops)]
        totals = [sum(jnp.sum(e, 0, keepdims=True) for e in group) for group in exps]
        outs = []
        for (start, stop, head, cuts, _), group, total in zip(work, exps, totals):
            out = None
            for (low, high), e in zip(cuts, group):
                part = dot_nn(turned[head * HALF_PAIR : (head + 1) * HALF_PAIR, low:high], e.astype(LOW))
                out = part if out is None else out + part
            outs.append(out * (1.0 / total))
        for place, start in enumerate(starts):
            stop = min(start + step_rows, length)
            both = jnp.concatenate(outs[2 * place : 2 * place + 2], 0)
            o_ref[start:stop, lanes] = both.T.astype(LOW)


def attend(q, k, v, batch, causal, pairs=6, step_rows=128):
    rows, width = q.shape
    length, frames = rows // batch, k.shape[0] // batch
    lanes = pairs * PAIR
    at = lambda b, p: (b, p)
    return run(
        functools.partial(attend_body, pairs, step_rows) if causal else functools.partial(attend_cross_body, pairs),
        "attend_self" if causal else "attend_cross",
        (batch, width // lanes),
        (q, k, v),
        [spec((length, lanes), at), spec((frames, lanes), at), spec((frames, lanes), at)],
        [((rows, width), LOW, spec((length, lanes), at))],
        flops=4 * rows * frames * width,
        exps=rows * frames * HEADS,
    )[0]


def attend_back_body(causal, pairs, step_rows, q_ref, k_ref, v_ref, g_ref, gq_ref, gk_ref, gv_ref, dk, dv):
    length = q_ref.shape[0]
    frames = k_ref.shape[0]
    starts = list(range(0, length, step_rows))
    for pair in range(pairs):
        lanes = slice(pair * PAIR, (pair + 1) * PAIR)
        keys = [head_lanes(k_ref[:, lanes], head) for head in (0, 1)]
        values = [head_lanes(v_ref[:, lanes], head) for head in (0, 1)]
        work = []
        for start in starts:
            stop = min(start + step_rows, length)
            cuts = ([(0, start)] if start else []) + [(start, stop)] if causal else [(0, frames)]
            for head in (0, 1):
                queries, grads = q_ref[start:stop, lanes], g_ref[start:stop, lanes]
                parts = []
                for low, high in cuts:
                    scores = dot_nt(keys[head][low:high], queries)
                    if causal and low == start:
                        key_at = lax.broadcasted_iota(jnp.int32, scores.shape, 0)
                        query_at = lax.broadcasted_iota(jnp.int32, scores.shape, 1)
                        scores = jnp.where(key_at <= query_at, scores, -1e30)
                    parts.append(scores)
                grad_parts = [dot_nt(values[head][low:high], grads) for low, high in cuts]
                work.append((start, stop, head, cuts, parts, grad_parts))
        probs = []
        for item in work:
            parts = item[4]
            top = jnp.max(parts[0], 0, keepdims=True)
            for scores in parts[1:]:
                top = jnp.maximum(top, jnp.max(scores, 0, keepdims=True))
            exps = [jnp.exp(scores - top) for scores in parts]
            total = 1.0 / sum(jnp.sum(e, 0, keepdims=True) for e in exps)
            probs.append([e * total for e in exps])
        scores = []
        for item, group in zip(work, probs):
            weighted = [p * g for p, g in zip(group, item[5])]
            inner = sum(jnp.sum(w, 0, keepdims=True) for w in weighted)
            scores.append([(w - p * inner).astype(LOW) for w, p in zip(weighted, group)])
        grad_q = {}
        for (start, stop, head, cuts, _, _), group, low_scores in zip(work, probs, scores):
            queries = head_lanes(q_ref[start:stop, lanes], head)
            grads = head_lanes(g_ref[start:stop, lanes], head)
            for (low, high), p, s in zip(cuts, group, low_scores):
                part_v = dot_nn(p.astype(LOW), grads)
                part_k = dot_nn(s, queries)
                part_q = dot_tn(s, keys[head][low:high])
                grad_q[start] = part_q if start not in grad_q else grad_q[start] + part_q
                if head == 0 and (low == start or not causal and start == 0):
                    dv[low:high, :] = part_v
                    dk[low:high, :] = part_k
                else:
                    dv[low:high, :] += part_v
                    dk[low:high, :] += part_k
        for start, total in grad_q.items():
            gq_ref[start : start + total.shape[0], lanes] = (total * SCALE).astype(LOW)
        gk_ref[:, lanes] = dk[...].astype(LOW)
        gv_ref[:, lanes] = dv[...].astype(LOW)


def attend_back(q, k, v, grad, batch, causal, pairs=6):
    rows, width = q.shape
    length, frames = rows // batch, k.shape[0] // batch
    lanes = pairs * PAIR
    at = lambda b, p: (b, p)
    long, short = spec((length, lanes), at), spec((frames, lanes), at)
    return run(
        functools.partial(attend_back_body, causal, pairs, 128 if causal else length),
        "attend_self_back" if causal else "attend_cross_back",
        (batch, width // lanes),
        (q, k, v, grad),
        [long, short, short, long],
        [((rows, width), LOW, long), (k.shape, LOW, short), (k.shape, LOW, short)],
        [pltpu.VMEM((frames, PAIR), WIDE)] * 2,
        flops=10 * rows * frames * width,
        exps=rows * frames * HEADS,
    )


def mid_body(per_seq, len_ref, a_ref, x_ref, vec_ref, wo, mid_ref, n_ref, s_ref):
    step = pl.program_id(0)
    branch = dot_nn(a_ref[...], wo[0]) + vec_ref[5:6, :]
    mid = x_ref[...].astype(WIDE) + branch
    mid_ref[...] = mid
    unit, _ = normalised(mid)
    n_ref[...] = (unit * vec_ref[1:2, :] + vec_ref[11:12, :]).astype(LOW)
    add_rows(s_ref, step == 0, [masked_squares(branch, len_ref, step, per_seq)])


def smem():
    return pl.BlockSpec(memory_space=pltpu.SMEM)


def mid_stage(lengths, attended, x, vec, self_b, batch, block):
    rows, width = x.shape
    weight = spec((1, width, width), lambda i: (1, 0, 0), once=True)
    tile = spec((block, width), lambda i: (i, 0))
    return run(
        functools.partial(mid_body, rows // batch // block),
        "mid_stage",
        (rows // block,),
        (lengths, attended, x, vec, self_b),
        [smem(), tile, tile, whole(vec.shape), weight],
        [
            ((rows, width), WIDE, tile),
            ((rows, width), LOW, tile),
            ((8, width), WIDE, spec((8, width), lambda i: (0, 0))),
        ],
        flops=2 * rows * width * width,
    )


def cross_body(n_ref, f_ref, vec_ref, wq, wk, wv, q_ref, k_ref, v_ref):
    query = (dot_nn(n_ref[...], wq[0]) + vec_ref[6:7, :]).astype(LOW)
    q_ref[...] = query * jnp.asarray(SCALE, LOW)
    frames = f_ref[...]
    k_ref[...] = dot_nn(frames, wk[0]).astype(LOW)
    v_ref[...] = (dot_nn(frames, wv[0]) + vec_ref[7:8, :]).astype(LOW)


def cross_stage(norm, frames, vec, cross_a, cross_b, batch):
    width = norm.shape[1]
    rows, frame_rows = norm.shape[0], frames.shape[0]
    long = spec((rows // batch, width), lambda i: (i, 0))
    short = spec((frame_rows // batch, width), lambda i: (i, 0))
    weight = lambda which: spec((1, width, width), lambda i: (which, 0, 0), once=True)
    return run(
        cross_body,
        "cross_stage",
        (batch,),
        (norm, frames, vec, cross_a, cross_b, cross_b),
        [long, short, whole(vec.shape), weight(0), weight(0), weight(1)],
        [((rows, width), LOW, long), ((frame_rows, width), LOW, short), ((frame_rows, width), LOW, short)],
        flops=(2 * rows + 4 * frame_rows) * width * width,
    )


def late_body(per_seq, len_ref, a_ref, mid_ref, vec_ref, wo, late_ref, n_ref, s_ref):
    step = pl.program_id(0)
    branch = dot_nn(a_ref[...], wo[0]) + vec_ref[8:9, :]
    late = mid_ref[...] + branch
    late_ref[...] = late
    unit, _ = normalised(late)
    n_ref[...] = (unit * vec_ref[2:3, :] + vec_ref[12:13, :]).astype(LOW)
    add_rows(s_ref, step == 0, [masked_squares(branch, len_ref, step, per_seq)])


def late_stage(lengths, attended, mid, vec, cross_a, batch, block):
    rows, width = mid.shape
    tile = spec((block, width), lambda i: (i, 0))
    return run(
        functools.partial(late_body, rows // batch // block),
        "late_stage",
        (rows // block,),
        (lengths, attended, mid, vec, cross_a),
        [smem(), tile, tile, whole(vec.shape), spec((1, width, width), lambda i: (1, 0, 0), once=True)],
        [
            ((rows, width), WIDE, tile),
            ((rows, width), LOW, tile),
            ((8, width), WIDE, spec((8, width), lambda i: (0, 0))),
        ],
        flops=2 * rows * width * width,
    )


def ffn_body(first, last, batch, block, split, len_ref, core_ref, n_ref, g_ref, b_ref, wi_ref, wo_ref, *refs):
    refs = list(refs)
    before = [] if first else [refs.pop(0), refs.pop(0)]
    late_ref, vec_ref = (refs.pop(0), refs.pop(0)) if last else (None, None)
    gn_ref = refs.pop(0)
    di_refs = [refs.pop(0) for _ in range(split)]
    do_refs = [refs.pop(0) for _ in range(split)]
    sf_ref, f_ref = refs[:2]
    rest = refs[2:]
    s_ref = rest.pop(0) if last else None
    hidden_ref, pre_ref = rest[:2]
    acc_ref = rest[2] if last else f_ref
    step = pl.program_id(0)
    rows = n_ref.shape[0]

    @pl.when(step == 0)
    def _():
        if first:
            acc_ref[...] = jnp.zeros_like(acc_ref)
            gn_ref[...] = jnp.zeros_like(gn_ref)
        else:
            acc_ref[...] = before[0][...]
            gn_ref[...] = before[1][...]

    def chunk(place, carry):
        at = pl.ds(pl.multiple_of(place * block, block), block)
        pre = dot_nn(n_ref[at, :], wi_ref[0]) + b_ref[0]
        below = 0.5 + 0.5 * lax.erf(pre * (0.5**0.5))
        density = jnp.exp(-0.5 * pre * pre) * (1.0 / math.sqrt(2.0 * math.pi))
        hidden = (pre * below).astype(LOW)
        hidden_ref[at, :] = hidden
        acc_ref[at, :] += dot_nn(hidden, wo_ref[0])
        grad = dot_nt(g_ref[at, :], wo_ref[0])
        grad = (grad * (below + pre * density)).astype(LOW)
        pre_ref[at, :] = grad
        gn_ref[at, :] += dot_nt(grad, wi_ref[0])
        return carry

    lax.fori_loop(0, rows // block, chunk, 0)
    sf_ref[0] = col_sum(pre_ref[...])
    store_grad(dot_tn(n_ref[...], pre_ref[...]), di_refs, 0, core_ref)
    store_grad(dot_tn(hidden_ref[...], g_ref[...]), do_refs, 0, core_ref)
    if last:
        @pl.when(step == pl.num_programs(0) - 1)
        def _():
            s_ref[...] = jnp.zeros_like(s_ref)

            def finish(place, carry):
                at = pl.ds(pl.multiple_of(place * block, block), block)
                branch = acc_ref[at, :] + vec_ref[9:10, :]
                result = late_ref[at, :] + branch
                f_ref[at, :] = result.astype(LOW)
                per_seq = rows // batch // block
                s_ref[0:1, :] += masked_squares(result, len_ref, place, per_seq)
                s_ref[1:2, :] += masked_squares(branch, len_ref, place, per_seq)
                s_ref[2:3, :] += col_sum(g_ref[at, :])
                return carry

            lax.fori_loop(0, rows // block, finish, 0)


def ffn_stage(lengths, core, count, norm, grad, bias, w_in, w_out, before, late, vec, batch, block):
    rows, width = norm.shape
    mats = w_in.shape[0]
    first, last = before is None, late is not None
    mat = spec((1, width, width), lambda j: (j, 0, 0))
    line = spec((1, 1, width), lambda j: (j, 0, 0))
    operands = [lengths, core, norm, grad, bias, w_in, w_out]
    specs = [smem(), smem(), whole(norm.shape), whole(grad.shape), line, mat, mat]
    if not first:
        operands += list(before)
        specs += [whole((rows, width))] * 2
    if last:
        operands += [late, vec]
        specs += [whole((rows, width)), whole(vec.shape)]
    fixed = whole((rows, width))
    grads = grad_outs(mats, width, count, (1, width), lambda j: (j, 0))
    outs = [
        ((rows, width), WIDE, fixed),
        *grads,
        *grads,
        ((mats, 1, width), WIDE, line),
        ((rows, width), LOW if last else WIDE, fixed),
    ]
    scratch = [pltpu.VMEM((rows, width), LOW)] * 2
    if last:
        outs.append(((8, width), WIDE, whole((8, width))))
        scratch.append(pltpu.VMEM((rows, width), WIDE))
    done = run(
        functools.partial(ffn_body, first, last, batch, block, len(grads)),
        "ffn_stage",
        (mats,),
        tuple(operands),
        specs,
        outs,
        scratch,
        flops=12 * rows * width * width * mats,
        exps=2 * rows * width * mats,
        limit=30,
    )
    split = len(grads)
    return done[0], done[1 : 1 + split], done[1 + split : 1 + 2 * split], *done[1 + 2 * split :]


def late_back_body(gn_ref, late_ref, og_ref, vec_ref, wo, gl_ref, gc_ref, ga_ref, s_ref):
    grad = gn_ref[...]
    through, for_gain = norm_backward(late_ref[...], grad, vec_ref[2:3, :])
    total = og_ref[...].astype(WIDE) + through
    gl_ref[...] = total
    low = total.astype(LOW)
    gc_ref[...] = low
    ga_ref[...] = dot_nt(low, wo[0]).astype(LOW)
    add_rows(s_ref, pl.program_id(0) == 0, [col_sum(for_gain), col_sum(grad), col_sum(low)])


def late_back(grad_norm, late, grad, vec, cross_a, block):
    rows, width = late.shape
    tile = spec((block, width), lambda i: (i, 0))
    return run(
        late_back_body,
        "late_back",
        (rows // block,),
        (grad_norm, late, grad, vec, cross_a),
        [
            tile,
            tile,
            tile,
            whole(vec.shape),
            spec((1, width, width), lambda i: (1, 0, 0), once=True),
        ],
        [
            ((rows, width), WIDE, tile),
            ((rows, width), LOW, tile),
            ((rows, width), LOW, tile),
            ((8, width), WIDE, spec((8, width), lambda i: (0, 0))),
        ],
        flops=2 * rows * width * width,
    )


def store_grad(grad, outs, place, core_ref):
    if len(outs) == 1:
        outs[0][place] = grad.astype(LOW)
        return
    groups, _, rows, width = outs[0].shape
    pairs = grad.reshape(groups, 2, rows, width)
    for core in (0, 1):

        @pl.when(core_ref[0] == core)
        def _(core=core):
            outs[0][:, place] = pairs[:, 1 - core].astype(LOW)
            outs[1][:, place] = pairs[:, core].astype(LOW)


def grad_outs(mats, width, count, block, index):
    rows = width // count
    if rows % 8 or block[1] % (2 * rows):
        whole_out = spec(block + (width,), lambda i: index(i) + (0,))
        return [((mats, width, width), LOW, whole_out)]
    groups = block[1] // (2 * rows)
    half = spec((groups, block[0], rows, width), lambda i: index(i)[::-1] + (0, 0))
    return [((count // 2, mats, rows, width), LOW, half)] * 2


def weights_body(count, core_ref, *refs):
    outs = refs[2 * count :]
    for place in range(count):
        grad = dot_tn(refs[2 * place][...], refs[2 * place + 1][...])
        store_grad(grad, outs, place, core_ref)


def weight_grads(pairs, core, count):
    width = pairs[0][0].shape[1]
    block = width // 2
    operands, specs = [core], [smem()]
    for left, right in pairs:
        operands += [left, right]
        specs += [spec((left.shape[0], block), lambda j: (0, j)), whole(right.shape)]
    return run(
        functools.partial(weights_body, len(pairs)),
        "weight_grads",
        (width // block,),
        tuple(operands),
        specs,
        grad_outs(len(pairs), width, count, (len(pairs), block), lambda j: (0, j)),
        flops=sum(2 * left.shape[0] * width * width for left, _ in pairs),
    )


def mid_back_body(gq, wq, mid_ref, gl_ref, vec_ref, wo, gm_ref, gs_ref, ga_ref, s_ref):
    query = gq[...]
    grad = dot_nt(query, wq[0])
    through, for_gain = norm_backward(mid_ref[...], grad, vec_ref[1:2, :])
    total = gl_ref[...] + through
    gm_ref[...] = total
    low = total.astype(LOW)
    gs_ref[...] = low
    ga_ref[...] = dot_nt(low, wo[0]).astype(LOW)
    add_rows(
        s_ref,
        pl.program_id(0) == 0,
        [col_sum(for_gain), col_sum(grad), col_sum(low), col_sum(query)],
    )


def mid_back(grad_q, cross_a, mid, grad_late, vec, self_b, block):
    rows, width = mid.shape
    tile = spec((block, width), lambda i: (i, 0))
    weight = lambda which: spec((1, width, width), lambda i: (which, 0, 0), once=True)
    return run(
        mid_back_body,
        "mid_back",
        (rows // block,),
        (grad_q, cross_a, mid, grad_late, vec, self_b),
        [tile, weight(0), tile, tile, whole(vec.shape), weight(1)],
        [
            ((rows, width), WIDE, tile),
            ((rows, width), LOW, tile),
            ((rows, width), LOW, tile),
            ((8, width), WIDE, spec((8, width), lambda i: (0, 0))),
        ],
        flops=4 * rows * width * width,
    )


def frames_back_body(gk, gv, wk, wv, ge_ref, s_ref):
    grad_v = gv[...]
    ge_ref[...] = (dot_nt(gk[...], wk[0]) + dot_nt(grad_v, wv[0])).astype(LOW)
    add_rows(s_ref, pl.program_id(0) == 0, [col_sum(grad_v)])


def frames_back(grad_k, grad_v, cross_b, block):
    rows, width = grad_k.shape
    tile = spec((block, width), lambda i: (i, 0))
    weight = lambda which: spec((1, width, width), lambda i: (which, 0, 0), once=True)
    return run(
        frames_back_body,
        "frames_back",
        (rows // block,),
        (grad_k, grad_v, cross_b, cross_b),
        [tile, tile, weight(0), weight(1)],
        [((rows, width), LOW, tile), ((8, width), WIDE, spec((8, width), lambda i: (0, 0)))],
        flops=4 * rows * width * width,
    )


def in_back_body(gq, gk, gv, wq, wk, wv, x_ref, gm_ref, vec_ref, gi_ref, s_ref):
    query, value = gq[...], gv[...]
    grad = dot_nt(query, wq[0]) + dot_nt(gk[...], wk[0]) + dot_nt(value, wv[0])
    through, for_gain = norm_backward(x_ref[...].astype(WIDE), grad, vec_ref[0:1, :])
    gi_ref[...] = (gm_ref[...] + through).astype(LOW)
    add_rows(
        s_ref,
        pl.program_id(0) == 0,
        [col_sum(for_gain), col_sum(grad), col_sum(query), col_sum(value)],
    )


def in_back(grad_q, grad_k, grad_v, self_a, self_b, x, grad_mid, vec, block):
    rows, width = x.shape
    tile = spec((block, width), lambda i: (i, 0))
    weight = lambda which: spec((1, width, width), lambda i: (which, 0, 0), once=True)
    return run(
        in_back_body,
        "in_back",
        (rows // block,),
        (grad_q, grad_k, grad_v, self_a, self_a, self_b, x, grad_mid, vec),
        [tile, tile, tile, weight(0), weight(1), weight(0), tile, tile, whole(vec.shape)],
        [((rows, width), LOW, tile), ((8, width), WIDE, spec((8, width), lambda i: (0, 0)))],
        flops=6 * rows * width * width,
    )


def axis_bits(count):
    bits = count.bit_length() - 1
    assert 1 << bits == count
    each = (bits - 1) // 3
    x_bits = list(range(1, 1 + each))
    y_bits = list(range(1 + each, 1 + 2 * each))
    z_bits = list(range(1 + 2 * each, bits))
    return x_bits, y_bits, z_bits


def gather_stages(count, parts):
    x_bits, y_bits, z_bits = (list(reversed(b)) for b in axis_bits(count))
    if parts == 1:
        return [[(b,) for b in bits] for bits in (z_bits[:1], z_bits[1:], y_bits, x_bits, [0])]
    return [
        [(z_bits[0],)],
        [(b,) for b in z_bits[1:]],
        list(zip(y_bits, x_bits)),
        list(zip(x_bits, y_bits)),
        [(0, 0)],
    ]


def scatter_stages(count, parts):
    return [list(reversed(stage)) for stage in reversed(gather_stages(count, parts))]


def swap(values, bit, count):
    return lax.ppermute(values, "fsdp", [(i, i ^ (1 << bit)) for i in range(count)])


def own_bit(bit):
    return (lax.axis_index("fsdp") >> bit) & 1


def weave_body(parts, core_ref, *refs):
    for part in range(parts):
        out = refs[2 * parts + part]
        out[0, :, core_ref[0]] = refs[part][:, 0]
        out[0, :, 1 - core_ref[0]] = refs[parts + part][:, 0]


def weave(held, other, core):
    groups, mats, rows, width = held[0].shape
    parts = len(held)
    half = spec((groups, 1, rows, width), lambda i: (0, i, 0, 0))
    both = spec((1, groups, 2, rows, width), lambda i: (i, 0, 0, 0, 0))
    return run(
        functools.partial(weave_body, parts),
        "weave",
        (mats,),
        (core, *held, *other),
        [smem()] + [half] * (2 * parts),
        [((mats, groups, 2, rows, width), held[0].dtype, both)] * parts,
    )


class Gather:
    def __init__(self, piece, count, parts=2):
        self.count = count
        self.bits = count.bit_length() - 1
        mats, rows, width = piece.shape
        self.shape = (rows, width)
        self.parts = [piece.reshape((1,) * self.bits + (mats, rows, width))]
        self.stages = gather_stages(count, parts)
        self.flight = None

    def land(self):
        if self.flight is not None:
            parts = []
            for held, (bit, other) in zip(self.parts, self.flight):
                axis = self.bits - 1 - bit
                parts.append(
                    jnp.where(
                        own_bit(bit) == 0,
                        jnp.concatenate([held, other], axis),
                        jnp.concatenate([other, held], axis),
                    )
                )
            self.parts = parts
            self.flight = None

    def ready(self):
        self.land()
        if len(self.stages[0][0]) == 2 and len(self.parts) == 1:
            self.parts = jnp.split(self.parts[0], 2, self.bits)
        return self.parts

    def launch(self, parts):
        self.parts = parts
        for place, step in enumerate(self.stages.pop(0)):
            if place:
                self.land()
            self.flight = [(bit, swap(part, bit, self.count)) for bit, part in zip(step, self.parts)]

    def result(self):
        rows, width = self.shape
        merged = lambda v: v.reshape((self.count // 2,) + v.shape[self.bits :])
        held = [merged(v) for v in self.parts]
        other = [merged(v) for _, v in self.flight]
        if len(held) == 1:
            self.land()
            return [self.parts[0].reshape(self.count * rows, width)]
        done = weave(held, other, own_bit(0).astype(jnp.int32).reshape(1))
        return [v.reshape(v.shape[0], self.count * rows, width) for v in done]


class Scatter:
    def __init__(self, parts, count):
        self.count = count
        self.bits = count.bit_length() - 1
        self.kind = parts[0][0].dtype
        self.stages = scatter_stages(count, len(parts))
        self.sends, self.pairs = [], []
        for part in parts:
            if len(part) == 1:
                mats, rows, width = part[0].shape
                groups = part[0].reshape(mats, count // 2, 2, rows // count, width)
                part = [
                    jnp.swapaxes(lax.dynamic_index_in_dim(groups, side, 2, False), 0, 1)
                    for side in (1 - own_bit(0), own_bit(0))
                ]
            self.shape = part[0].shape[2:]
            shaped = [v.reshape((2,) * (self.bits - 1) + (1,) + v.shape[1:]) for v in part]
            self.sends.append(shaped[0])
            self.pairs.append((shaped[1], None))

    def pick(self, pair, bit, side):
        axis = self.bits - 1 - bit
        values = [lax.dynamic_slice_in_dim(v, side, 1, axis) for v in pair]
        return self.total(values, self.kind)

    def total(self, pair, kind):
        return (pair[0].astype(WIDE) + pair[1].astype(WIDE)).astype(kind)

    def ready(self):
        if self.sends is not None:
            return self.sends
        step = self.stages[0][0]
        if len(step) == 1 and len(self.pairs) == 2:
            self.pairs = [
                tuple(jnp.concatenate([p[i] for p in self.pairs], self.bits) for i in (0, 1))
            ]
        return [self.pick(pair, bit, 1 - own_bit(bit)) for bit, pair in zip(step, self.pairs)]

    def launch(self, sends):
        for place, step in enumerate(self.stages.pop(0)):
            if place:
                sends = [self.pick(p, b, 1 - own_bit(b)) for b, p in zip(step, self.pairs)]
            flight = [swap(v, bit, self.count) for bit, v in zip(step, sends)]
            if self.sends is None:
                kept = [self.pick(p, bit, own_bit(bit)) for bit, p in zip(step, self.pairs)]
            else:
                kept, self.sends = [p[0] for p in self.pairs], None
            self.pairs = list(zip(kept, flight))

    def result(self):
        total = jnp.concatenate([self.total(p, WIDE) for p in self.pairs], self.bits)
        return total.reshape((-1,) + self.shape)


def tick(chains, values=()):
    ready = [chain.ready() for chain in chains]
    ready, values = lax.optimization_barrier((ready, values))
    for chain, parts in zip(chains, ready):
        chain.launch(parts)
    return values


def shards(
    count,
    hidden_in,
    encoder_states,
    lengths,
    out_grad,
    attn_in,
    attn_out,
    fc_in,
    fc_out,
    gains,
    biases,
    ffn_bias,
):
    batch, length, width = hidden_in.shape
    rows = batch * length
    block = length // 2
    frame_rows = encoder_states.shape[1]
    share = gains.shape[1]
    ff_share = ffn_bias.shape[0]
    mats = ff_share // share

    small = jnp.concatenate([gains.reshape(-1), biases.reshape(-1), ffn_bias])
    small_count = small.shape[0]
    small_rows = -(-(small_count + 5) // 128)
    small_size = small_rows * 128
    small = jnp.pad(small, (0, small_size - small_count)).reshape(1, small_rows, 128)
    fc_in_mats = fc_in.reshape(share, count, mats, share).transpose(2, 0, 1, 3).reshape(mats, share, width)
    fc_out_mats = fc_out.reshape(mats, share, width)
    g_small = Gather(small, count, 1)
    g_self = Gather(jnp.concatenate([attn_in[0:3], attn_out[0:1]]), count)
    g_cross = Gather(jnp.concatenate([attn_in[3:4], attn_out[1:2], attn_in[4:6]]), count)
    g_ffn = Gather(jnp.concatenate([fc_in_mats, fc_out_mats]), count)

    core = own_bit(0).astype(jnp.int32).reshape(1)
    x = hidden_in.reshape(rows, width)
    frames = encoder_states.reshape(-1, width)
    valid = jnp.arange(length)[None, :, None] < lengths[:, None, None]
    grad = jnp.where(valid, out_grad, jnp.zeros_like(out_grad)).reshape(rows, width)

    tick([g_self, g_small])
    tick([g_self, g_small])
    tick([g_self, g_small, g_cross])
    tick([g_self, g_small, g_cross, g_ffn])
    tick([g_self, g_small, g_cross, g_ffn])
    small = g_small.result()[0].astype(jnp.float32).reshape(count, small_size)
    vec = small[:, : 13 * share].reshape(count, 13, share).transpose(1, 0, 2).reshape(13, width)
    vec = jnp.pad(vec, ((0, 3), (0, 0)))
    bias = small[:, 13 * share : small_count].reshape(count, mats, share)
    bias = bias.transpose(1, 0, 2).reshape(mats, 1, width)
    self_a, self_b = g_self.result()
    x = tick([g_cross], x)
    norm_one, query, key, value = qkv(x, vec, self_a, self_b, block)
    query, key, value = tick([g_ffn], (query, key, value))
    attended = attend(query, key, value, batch, True)
    mid, norm_two, square_self = mid_stage(lengths, attended, x, vec, self_b, batch, block)
    norm_two = tick([g_cross], norm_two)
    norm_two = tick([g_ffn], norm_two)
    cross_a, cross_b = g_cross.result()
    cross_q, cross_k, cross_v = cross_stage(norm_two, frames, vec, cross_a, cross_b, batch)
    cross_attended = attend(cross_q, cross_k, cross_v, batch, False)
    late, norm_three, square_cross = late_stage(lengths, cross_attended, mid, vec, cross_a, batch, block)
    norm_three = tick([g_ffn], norm_three)
    w_in, w_out = g_ffn.result()
    grad_norm, d_in, d_out, sums_ff, result, square_rest = ffn_stage(
        lengths, core, count, norm_three, grad, bias, w_in, w_out, None, late, vec, batch, block
    )
    s_ffn = Scatter([d_in, d_out], count)
    grad_norm = tick([s_ffn], grad_norm)
    grad_late, grad_cross, grad_cross_att, sums_late = late_back(
        grad_norm, late, grad, vec, cross_a, block
    )
    grad_cross_att = tick([s_ffn], grad_cross_att)
    grad_cq, grad_ck, grad_cv = attend_back(
        cross_q, cross_k, cross_v, grad_cross_att, batch, False
    )
    d_cross_a = weight_grads([(norm_two, grad_cq), (cross_attended, grad_cross)], core, count)
    d_cross_b = weight_grads([(frames, grad_ck), (frames, grad_cv)], core, count)
    s_cross = Scatter([d_cross_a, d_cross_b], count)
    grad_cq, grad_ck, grad_cv = tick([s_cross], (grad_cq, grad_ck, grad_cv))
    grad_mid, grad_self, grad_att, sums_mid = mid_back(
        grad_cq, cross_a, mid, grad_late, vec, self_b, block
    )
    grad_frames, sums_frames = frames_back(grad_ck, grad_cv, cross_b, frame_rows)
    grad_att, grad_frames = tick([s_cross, s_ffn], (grad_att, grad_frames))
    grad_q, grad_k, grad_v = attend_back(query, key, value, grad_att, batch, True)
    d_self_a = weight_grads([(norm_one, grad_q), (norm_one, grad_k)], core, count)
    d_self_b = weight_grads([(norm_one, grad_v), (attended, grad_self)], core, count)
    s_self = Scatter([d_self_a, d_self_b], count)
    grad_q, grad_k, grad_v = tick([s_self, s_cross, s_ffn], (grad_q, grad_k, grad_v))
    grad_in, sums_one = in_back(grad_q, grad_k, grad_v, self_a, self_b, x, grad_mid, vec, block)

    sums_one = tick([s_self, s_cross, s_ffn], sums_one)
    sum_rows = jnp.stack(
        [sums_one[0], sums_mid[0], sums_late[0]]
        + [sums_one[2], sums_one[3], sums_mid[2], sums_mid[3], sums_frames[0], sums_late[2], square_rest[2]]
        + [sums_one[1], sums_mid[1], sums_late[1]]
    )
    squares = jnp.stack([square_rest[0], square_self[0], square_cross[0], square_rest[1]])
    stats = jnp.concatenate([jnp.sum(squares, -1), jnp.sum(lengths).astype(WIDE)[None]])
    sums_ff = sums_ff.reshape(mats, count, share)
    sums = jnp.concatenate(
        [
            sum_rows.reshape(13, count, share).transpose(1, 0, 2).reshape(count, 13 * share),
            sums_ff.transpose(1, 0, 2).reshape(count, ff_share),
            jnp.broadcast_to(stats[None], (count, 5)),
        ],
        1,
    )
    sums = jnp.pad(sums, ((0, 0), (0, small_size - sums.shape[1])))
    s_small = Scatter([[sums.reshape(1, count * small_rows, 128)]], count)
    tick([s_small])
    tick([s_small])
    tick([s_self, s_cross, s_small])
    tick([s_self, s_small])
    tick([s_self, s_small])
    d_ffn = s_ffn.result()
    d_in_all, d_out_all = d_ffn[:mats], d_ffn[mats:]
    d_cross = s_cross.result()
    d_self = s_self.result()
    small = s_small.result().reshape(-1)
    stats = small[small_count : small_count + 5]
    rms = jnp.sqrt(stats[:4] / (stats[4] * width))
    return (
        result.reshape(hidden_in.shape),
        grad_in.reshape(hidden_in.shape),
        grad_frames.reshape(encoder_states.shape),
        jnp.concatenate([d_self[:3], d_cross[:1], d_cross[2:]]),
        jnp.concatenate([d_self[3:], d_cross[1:2]]),
        d_in_all.reshape(mats, share, count, share).transpose(1, 2, 0, 3).reshape(share, -1),
        d_out_all.reshape(ff_share, width),
        small[: 3 * share].reshape(3, share),
        small[3 * share : 13 * share].reshape(10, share),
        small[13 * share : small_count],
        rms,
    )


def solution(mesh):
    placed = (
        P("fsdp", None, None),
        P("fsdp", None, None),
        P("fsdp"),
        P("fsdp", None, None),
        P(None, "fsdp", None),
        P(None, "fsdp", None),
        P("fsdp", None),
        P("fsdp", None),
        P(None, "fsdp"),
        P(None, "fsdp"),
        P("fsdp"),
    )
    return jax.shard_map(
        functools.partial(shards, mesh.shape["fsdp"]),
        mesh=mesh,
        in_specs=placed,
        out_specs=(
            P("fsdp", None, None),
            P("fsdp", None, None),
            P("fsdp", None, None),
            P(None, "fsdp", None),
            P(None, "fsdp", None),
            P("fsdp", None),
            P("fsdp", None),
            P(None, "fsdp"),
            P(None, "fsdp"),
            P("fsdp"),
            P(),
        ),
        check_vma=False,
    )
```

```python
import functools
import math

import jax
import jax.numpy as jnp
from jax import lax
from jax.experimental import pallas as pl
from jax.experimental.pallas import tpu as pltpu
from jax.sharding import PartitionSpec as P

NORM_EPS = 1e-05
LOW = jnp.bfloat16
WIDE = jnp.float32
HEADS = 12
PAIR = 128
HALF_PAIR = 64
SCALE = 0.125


def dot_nn(left, right):
    return lax.dot_general(left, right, (((1,), (0,)), ((), ())), preferred_element_type=WIDE)


def dot_nt(left, right):
    return lax.dot_general(left, right, (((1,), (1,)), ((), ())), preferred_element_type=WIDE)


def dot_tn(left, right):
    return lax.dot_general(left, right, (((0,), (0,)), ((), ())), preferred_element_type=WIDE)


def spec(block, index, once=False):
    if once:
        return pl.BlockSpec(block, index, pipeline_mode=pl.Buffered(1))
    return pl.BlockSpec(block, index)


def run(body, name, grid, operands, in_specs, outs, scratch=(), flops=0, exps=0, limit=14):
    moved = sum(o.size * o.dtype.itemsize for o in operands)
    moved += sum(math.prod(s) * jnp.dtype(d).itemsize for s, d, _ in outs)
    return pl.pallas_call(
        body,
        name=name,
        grid=grid,
        in_specs=in_specs,
        out_specs=[o[2] for o in outs],
        out_shape=[jax.ShapeDtypeStruct(o[0], o[1]) for o in outs],
        scratch_shapes=list(scratch),
        compiler_params=pltpu.CompilerParams(
            dimension_semantics=("arbitrary",) * len(grid), vmem_limit_bytes=limit << 20
        ),
        cost_estimate=pl.CostEstimate(flops=flops, transcendentals=exps, bytes_accessed=moved),
    )(*operands)


def normalised(values):
    center = values - jnp.mean(values, -1, keepdims=True)
    spread = jnp.mean(center * center, -1, keepdims=True)
    scale = lax.rsqrt(spread + NORM_EPS)
    return center * scale, scale


def norm_backward(values, grad, gain):
    unit, scale = normalised(values)
    inner = grad * gain
    mean_inner = jnp.mean(inner, -1, keepdims=True)
    mean_unit = jnp.mean(inner * unit, -1, keepdims=True)
    return scale * (inner - mean_inner - unit * mean_unit), grad * unit


def col_sum(values):
    return jnp.sum(values.astype(WIDE), 0, keepdims=True)


def add_rows(ref, first, rows):
    @pl.when(first)
    def _():
        ref[...] = jnp.zeros_like(ref)

    for place, row in enumerate(rows):
        ref[place : place + 1, :] += row


def masked_squares(values, length_ref, step, per_seq):
    rows = values.shape[0]
    start = (step % per_seq) * rows
    index = start + lax.broadcasted_iota(jnp.int32, (rows, 1), 0)
    inside = index < length_ref[step // per_seq]
    return col_sum(jnp.where(inside, values * values, 0.0))


def qkv_body(x_ref, vec_ref, wq, wk, wv, n_ref, q_ref, k_ref, v_ref):
    unit, _ = normalised(x_ref[...].astype(WIDE))
    norm = (unit * vec_ref[0:1, :] + vec_ref[10:11, :]).astype(LOW)
    n_ref[...] = norm
    query = (dot_nn(norm, wq[0]) + vec_ref[3:4, :]).astype(LOW)
    q_ref[...] = query * jnp.asarray(SCALE, LOW)
    k_ref[...] = dot_nn(norm, wk[0]).astype(LOW)
    v_ref[...] = (dot_nn(norm, wv[0]) + vec_ref[4:5, :]).astype(LOW)


def whole(shape):
    return spec(shape, lambda *_: (0,) * len(shape), once=True)


def qkv(x, vec, self_a, self_b, block):
    rows, width = x.shape
    row = lambda i: (i, 0)
    weight = lambda which: spec((1, width, width), lambda i: (which, 0, 0), once=True)
    return run(
        qkv_body,
        "qkv",
        (rows // block,),
        (x, vec, self_a, self_a, self_b),
        [spec((block, width), row), whole(vec.shape), weight(0), weight(1), weight(0)],
        [((rows, width), LOW, spec((block, width), row))] * 4,
        flops=6 * rows * width * width,
    )


def head_lanes(values, head):
    lane = lax.broadcasted_iota(jnp.int32, (1, PAIR), 1)
    inside = lane < HALF_PAIR if head == 0 else lane >= HALF_PAIR
    return jnp.where(inside, values, jnp.zeros_like(values))


def attend_cross_body(pairs, q_ref, k_ref, v_ref, o_ref):
    for pair in range(pairs):
        lanes = slice(pair * PAIR, (pair + 1) * PAIR)
        values, keys, queries = v_ref[:, lanes], k_ref[:, lanes], q_ref[:, lanes]
        total = None
        for head in (0, 1):
            scores = dot_nt(head_lanes(queries, head), keys)
            exps = jnp.exp(scores - jnp.max(scores, -1, keepdims=True))
            probs = exps * (1.0 / jnp.sum(exps, -1, keepdims=True))
            part = dot_nn(probs.astype(LOW), head_lanes(values, head))
            total = part if total is None else total + part
        o_ref[:, lanes] = total.astype(LOW)


def attend_body(pairs, step_rows, q_ref, k_ref, v_ref, o_ref):
    length = q_ref.shape[0]
    starts = list(range(0, length, step_rows))
    for pair in range(pairs):
        lanes = slice(pair * PAIR, (pair + 1) * PAIR)
        turned = v_ref[:, lanes].T
        keys = [head_lanes(k_ref[:, lanes], head) for head in (0, 1)]
        work = []
        for start in starts:
            stop = min(start + step_rows, length)
            queries = q_ref[start:stop, lanes]
            cuts = ([(0, start)] if start else []) + [(start, stop)]
            for head in (0, 1):
                parts = []
                for low, high in cuts:
                    scores = dot_nt(keys[head][low:high], queries)
                    if low == start:
                        key_at = lax.broadcasted_iota(jnp.int32, scores.shape, 0)
                        query_at = lax.broadcasted_iota(jnp.int32, scores.shape, 1)
                        scores = jnp.where(key_at <= query_at, scores, -1e30)
                    parts.append(scores)
                work.append((start, stop, head, cuts, parts))
        tops = []
        for start, stop, head, cuts, parts in work:
            top = jnp.max(parts[0], 0, keepdims=True)
            for scores in parts[1:]:
                top = jnp.maximum(top, jnp.max(scores, 0, keepdims=True))
            tops.append(top)
        exps = [[jnp.exp(s - top) for s in item[4]] for item, top in zip(work, tops)]
        totals = [sum(jnp.sum(e, 0, keepdims=True) for e in group) for group in exps]
        outs = []
        for (start, stop, head, cuts, _), group, total in zip(work, exps, totals):
            out = None
            for (low, high), e in zip(cuts, group):
                part = dot_nn(turned[head * HALF_PAIR : (head + 1) * HALF_PAIR, low:high], e.astype(LOW))
                out = part if out is None else out + part
            outs.append(out * (1.0 / total))
        for place, start in enumerate(starts):
            stop = min(start + step_rows, length)
            both = jnp.concatenate(outs[2 * place : 2 * place + 2], 0)
            o_ref[start:stop, lanes] = both.T.astype(LOW)


def attend(q, k, v, batch, causal, pairs=6, step_rows=128):
    rows, width = q.shape
    length, frames = rows // batch, k.shape[0] // batch
    lanes = pairs * PAIR
    at = lambda b, p: (b, p)
    return run(
        functools.partial(attend_body, pairs, step_rows) if causal else functools.partial(attend_cross_body, pairs),
        "attend_self" if causal else "attend_cross",
        (batch, width // lanes),
        (q, k, v),
        [spec((length, lanes), at), spec((frames, lanes), at), spec((frames, lanes), at)],
        [((rows, width), LOW, spec((length, lanes), at))],
        flops=4 * rows * frames * width,
        exps=rows * frames * HEADS,
    )[0]


def attend_back_body(causal, pairs, step_rows, q_ref, k_ref, v_ref, g_ref, gq_ref, gk_ref, gv_ref, dk, dv):
    length = q_ref.shape[0]
    frames = k_ref.shape[0]
    starts = list(range(0, length, step_rows))
    for pair in range(pairs):
        lanes = slice(pair * PAIR, (pair + 1) * PAIR)
        keys = [head_lanes(k_ref[:, lanes], head) for head in (0, 1)]
        values = [head_lanes(v_ref[:, lanes], head) for head in (0, 1)]
        work = []
        for start in starts:
            stop = min(start + step_rows, length)
            cuts = ([(0, start)] if start else []) + [(start, stop)] if causal else [(0, frames)]
            for head in (0, 1):
                queries, grads = q_ref[start:stop, lanes], g_ref[start:stop, lanes]
                parts = []
                for low, high in cuts:
                    scores = dot_nt(keys[head][low:high], queries)
                    if causal and low == start:
                        key_at = lax.broadcasted_iota(jnp.int32, scores.shape, 0)
                        query_at = lax.broadcasted_iota(jnp.int32, scores.shape, 1)
                        scores = jnp.where(key_at <= query_at, scores, -1e30)
                    parts.append(scores)
                grad_parts = [dot_nt(values[head][low:high], grads) for low, high in cuts]
                work.append((start, stop, head, cuts, parts, grad_parts))
        probs = []
        for item in work:
            parts = item[4]
            top = jnp.max(parts[0], 0, keepdims=True)
            for scores in parts[1:]:
                top = jnp.maximum(top, jnp.max(scores, 0, keepdims=True))
            exps = [jnp.exp(scores - top) for scores in parts]
            total = 1.0 / sum(jnp.sum(e, 0, keepdims=True) for e in exps)
            probs.append([e * total for e in exps])
        scores = []
        for item, group in zip(work, probs):
            weighted = [p * g for p, g in zip(group, item[5])]
            inner = sum(jnp.sum(w, 0, keepdims=True) for w in weighted)
            scores.append([(w - p * inner).astype(LOW) for w, p in zip(weighted, group)])
        grad_q = {}
        for (start, stop, head, cuts, _, _), group, low_scores in zip(work, probs, scores):
            queries = head_lanes(q_ref[start:stop, lanes], head)
            grads = head_lanes(g_ref[start:stop, lanes], head)
            for (low, high), p, s in zip(cuts, group, low_scores):
                part_v = dot_nn(p.astype(LOW), grads)
                part_k = dot_nn(s, queries)
                part_q = dot_tn(s, keys[head][low:high])
                grad_q[start] = part_q if start not in grad_q else grad_q[start] + part_q
                if head == 0 and (low == start or not causal and start == 0):
                    dv[low:high, :] = part_v
                    dk[low:high, :] = part_k
                else:
                    dv[low:high, :] += part_v
                    dk[low:high, :] += part_k
        for start, total in grad_q.items():
            gq_ref[start : start + total.shape[0], lanes] = (total * SCALE).astype(LOW)
        gk_ref[:, lanes] = dk[...].astype(LOW)
        gv_ref[:, lanes] = dv[...].astype(LOW)


def attend_back(q, k, v, grad, batch, causal, pairs=6):
    rows, width = q.shape
    length, frames = rows // batch, k.shape[0] // batch
    lanes = pairs * PAIR
    at = lambda b, p: (b, p)
    long, short = spec((length, lanes), at), spec((frames, lanes), at)
    return run(
        functools.partial(attend_back_body, causal, pairs, 128 if causal else length),
        "attend_self_back" if causal else "attend_cross_back",
        (batch, width // lanes),
        (q, k, v, grad),
        [long, short, short, long],
        [((rows, width), LOW, long), (k.shape, LOW, short), (k.shape, LOW, short)],
        [pltpu.VMEM((frames, PAIR), WIDE)] * 2,
        flops=10 * rows * frames * width,
        exps=rows * frames * HEADS,
    )


def mid_body(per_seq, len_ref, a_ref, x_ref, vec_ref, wo, mid_ref, n_ref, s_ref):
    step = pl.program_id(0)
    branch = dot_nn(a_ref[...], wo[0]) + vec_ref[5:6, :]
    mid = x_ref[...].astype(WIDE) + branch
    mid_ref[...] = mid
    unit, _ = normalised(mid)
    n_ref[...] = (unit * vec_ref[1:2, :] + vec_ref[11:12, :]).astype(LOW)
    add_rows(s_ref, step == 0, [masked_squares(branch, len_ref, step, per_seq)])


def smem():
    return pl.BlockSpec(memory_space=pltpu.SMEM)


def mid_stage(lengths, attended, x, vec, self_b, batch, block):
    rows, width = x.shape
    weight = spec((1, width, width), lambda i: (1, 0, 0), once=True)
    tile = spec((block, width), lambda i: (i, 0))
    return run(
        functools.partial(mid_body, rows // batch // block),
        "mid_stage",
        (rows // block,),
        (lengths, attended, x, vec, self_b),
        [smem(), tile, tile, whole(vec.shape), weight],
        [
            ((rows, width), WIDE, tile),
            ((rows, width), LOW, tile),
            ((8, width), WIDE, spec((8, width), lambda i: (0, 0))),
        ],
        flops=2 * rows * width * width,
    )


def cross_body(n_ref, f_ref, vec_ref, wq, wk, wv, q_ref, k_ref, v_ref):
    query = (dot_nn(n_ref[...], wq[0]) + vec_ref[6:7, :]).astype(LOW)
    q_ref[...] = query * jnp.asarray(SCALE, LOW)
    frames = f_ref[...]
    k_ref[...] = dot_nn(frames, wk[0]).astype(LOW)
    v_ref[...] = (dot_nn(frames, wv[0]) + vec_ref[7:8, :]).astype(LOW)


def cross_stage(norm, frames, vec, cross_a, cross_b, batch):
    width = norm.shape[1]
    rows, frame_rows = norm.shape[0], frames.shape[0]
    long = spec((rows // batch, width), lambda i: (i, 0))
    short = spec((frame_rows // batch, width), lambda i: (i, 0))
    weight = lambda which: spec((1, width, width), lambda i: (which, 0, 0), once=True)
    return run(
        cross_body,
        "cross_stage",
        (batch,),
        (norm, frames, vec, cross_a, cross_b, cross_b),
        [long, short, whole(vec.shape), weight(0), weight(0), weight(1)],
        [((rows, width), LOW, long), ((frame_rows, width), LOW, short), ((frame_rows, width), LOW, short)],
        flops=(2 * rows + 4 * frame_rows) * width * width,
    )


def late_body(per_seq, len_ref, a_ref, mid_ref, vec_ref, wo, late_ref, n_ref, s_ref):
    step = pl.program_id(0)
    branch = dot_nn(a_ref[...], wo[0]) + vec_ref[8:9, :]
    late = mid_ref[...] + branch
    late_ref[...] = late
    unit, _ = normalised(late)
    n_ref[...] = (unit * vec_ref[2:3, :] + vec_ref[12:13, :]).astype(LOW)
    add_rows(s_ref, step == 0, [masked_squares(branch, len_ref, step, per_seq)])


def late_stage(lengths, attended, mid, vec, cross_a, batch, block):
    rows, width = mid.shape
    tile = spec((block, width), lambda i: (i, 0))
    return run(
        functools.partial(late_body, rows // batch // block),
        "late_stage",
        (rows // block,),
        (lengths, attended, mid, vec, cross_a),
        [smem(), tile, tile, whole(vec.shape), spec((1, width, width), lambda i: (1, 0, 0), once=True)],
        [
            ((rows, width), WIDE, tile),
            ((rows, width), LOW, tile),
            ((8, width), WIDE, spec((8, width), lambda i: (0, 0))),
        ],
        flops=2 * rows * width * width,
    )


def ffn_body(first, last, batch, block, split, len_ref, core_ref, n_ref, g_ref, b_ref, wi_ref, wo_ref, *refs):
    refs = list(refs)
    before = [] if first else [refs.pop(0), refs.pop(0)]
    late_ref, vec_ref = (refs.pop(0), refs.pop(0)) if last else (None, None)
    gn_ref = refs.pop(0)
    di_refs = [refs.pop(0) for _ in range(split)]
    do_refs = [refs.pop(0) for _ in range(split)]
    sf_ref, f_ref = refs[:2]
    rest = refs[2:]
    s_ref = rest.pop(0) if last else None
    hidden_ref, pre_ref = rest[:2]
    acc_ref = rest[2] if last else f_ref
    step = pl.program_id(0)
    rows = n_ref.shape[0]

    @pl.when(step == 0)
    def _():
        if first:
            acc_ref[...] = jnp.zeros_like(acc_ref)
            gn_ref[...] = jnp.zeros_like(gn_ref)
        else:
            acc_ref[...] = before[0][...]
            gn_ref[...] = before[1][...]

    def chunk(place, carry):
        at = pl.ds(pl.multiple_of(place * block, block), block)
        pre = dot_nn(n_ref[at, :], wi_ref[0]) + b_ref[0]
        below = 0.5 + 0.5 * lax.erf(pre * (0.5**0.5))
        density = jnp.exp(-0.5 * pre * pre) * (1.0 / math.sqrt(2.0 * math.pi))
        hidden = (pre * below).astype(LOW)
        hidden_ref[at, :] = hidden
        acc_ref[at, :] += dot_nn(hidden, wo_ref[0])
        grad = dot_nt(g_ref[at, :], wo_ref[0])
        grad = (grad * (below + pre * density)).astype(LOW)
        pre_ref[at, :] = grad
        gn_ref[at, :] += dot_nt(grad, wi_ref[0])
        return carry

    lax.fori_loop(0, rows // block, chunk, 0)
    sf_ref[0] = col_sum(pre_ref[...])
    store_grad(dot_tn(n_ref[...], pre_ref[...]), di_refs, 0, core_ref)
    store_grad(dot_tn(hidden_ref[...], g_ref[...]), do_refs, 0, core_ref)
    if last:
        @pl.when(step == pl.num_programs(0) - 1)
        def _():
            s_ref[...] = jnp.zeros_like(s_ref)

            def finish(place, carry):
                at = pl.ds(pl.multiple_of(place * block, block), block)
                branch = acc_ref[at, :] + vec_ref[9:10, :]
                result = late_ref[at, :] + branch
                f_ref[at, :] = result.astype(LOW)
                per_seq = rows // batch // block
                s_ref[0:1, :] += masked_squares(result, len_ref, place, per_seq)
                s_ref[1:2, :] += masked_squares(branch, len_ref, place, per_seq)
                s_ref[2:3, :] += col_sum(g_ref[at, :])
                return carry

            lax.fori_loop(0, rows // block, finish, 0)


def ffn_stage(lengths, core, count, norm, grad, bias, w_in, w_out, before, late, vec, batch, block):
    rows, width = norm.shape
    mats = w_in.shape[0]
    first, last = before is None, late is not None
    mat = spec((1, width, width), lambda j: (j, 0, 0))
    line = spec((1, 1, width), lambda j: (j, 0, 0))
    operands = [lengths, core, norm, grad, bias, w_in, w_out]
    specs = [smem(), smem(), whole(norm.shape), whole(grad.shape), line, mat, mat]
    if not first:
        operands += list(before)
        specs += [whole((rows, width))] * 2
    if last:
        operands += [late, vec]
        specs += [whole((rows, width)), whole(vec.shape)]
    fixed = whole((rows, width))
    grads = grad_outs(mats, width, count, (1, width), lambda j: (j, 0))
    outs = [
        ((rows, width), WIDE, fixed),
        *grads,
        *grads,
        ((mats, 1, width), WIDE, line),
        ((rows, width), LOW if last else WIDE, fixed),
    ]
    scratch = [pltpu.VMEM((rows, width), LOW)] * 2
    if last:
        outs.append(((8, width), WIDE, whole((8, width))))
        scratch.append(pltpu.VMEM((rows, width), WIDE))
    done = run(
        functools.partial(ffn_body, first, last, batch, block, len(grads)),
        "ffn_stage",
        (mats,),
        tuple(operands),
        specs,
        outs,
        scratch,
        flops=12 * rows * width * width * mats,
        exps=2 * rows * width * mats,
        limit=30,
    )
    split = len(grads)
    return done[0], done[1 : 1 + split], done[1 + split : 1 + 2 * split], *done[1 + 2 * split :]


def late_back_body(gn_ref, late_ref, og_ref, vec_ref, wo, gl_ref, gc_ref, ga_ref, s_ref):
    grad = gn_ref[...]
    through, for_gain = norm_backward(late_ref[...], grad, vec_ref[2:3, :])
    total = og_ref[...].astype(WIDE) + through
    gl_ref[...] = total
    low = total.astype(LOW)
    gc_ref[...] = low
    ga_ref[...] = dot_nt(low, wo[0]).astype(LOW)
    add_rows(s_ref, pl.program_id(0) == 0, [col_sum(for_gain), col_sum(grad), col_sum(low)])


def late_back(grad_norm, late, grad, vec, cross_a, block):
    rows, width = late.shape
    tile = spec((block, width), lambda i: (i, 0))
    return run(
        late_back_body,
        "late_back",
        (rows // block,),
        (grad_norm, late, grad, vec, cross_a),
        [
            tile,
            tile,
            tile,
            whole(vec.shape),
            spec((1, width, width), lambda i: (1, 0, 0), once=True),
        ],
        [
            ((rows, width), WIDE, tile),
            ((rows, width), LOW, tile),
            ((rows, width), LOW, tile),
            ((8, width), WIDE, spec((8, width), lambda i: (0, 0))),
        ],
        flops=2 * rows * width * width,
    )


def store_grad(grad, outs, place, core_ref):
    if len(outs) == 1:
        outs[0][place] = grad.astype(LOW)
        return
    groups, _, rows, width = outs[0].shape
    pairs = grad.reshape(groups, 2, rows, width)
    for core in (0, 1):

        @pl.when(core_ref[0] == core)
        def _(core=core):
            outs[0][:, place] = pairs[:, 1 - core].astype(LOW)
            outs[1][:, place] = pairs[:, core].astype(LOW)


def grad_outs(mats, width, count, block, index):
    rows = width // count
    if rows % 8 or block[1] % (2 * rows):
        whole_out = spec(block + (width,), lambda i: index(i) + (0,))
        return [((mats, width, width), LOW, whole_out)]
    groups = block[1] // (2 * rows)
    half = spec((groups, block[0], rows, width), lambda i: index(i)[::-1] + (0, 0))
    return [((count // 2, mats, rows, width), LOW, half)] * 2


def weights_body(count, core_ref, *refs):
    outs = refs[2 * count :]
    for place in range(count):
        grad = dot_tn(refs[2 * place][...], refs[2 * place + 1][...])
        store_grad(grad, outs, place, core_ref)


def weight_grads(pairs, core, count):
    width = pairs[0][0].shape[1]
    block = width // 2
    operands, specs = [core], [smem()]
    for left, right in pairs:
        operands += [left, right]
        specs += [spec((left.shape[0], block), lambda j: (0, j)), whole(right.shape)]
    return run(
        functools.partial(weights_body, len(pairs)),
        "weight_grads",
        (width // block,),
        tuple(operands),
        specs,
        grad_outs(len(pairs), width, count, (len(pairs), block), lambda j: (0, j)),
        flops=sum(2 * left.shape[0] * width * width for left, _ in pairs),
    )


def mid_back_body(gq, wq, mid_ref, gl_ref, vec_ref, wo, gm_ref, gs_ref, ga_ref, s_ref):
    query = gq[...]
    grad = dot_nt(query, wq[0])
    through, for_gain = norm_backward(mid_ref[...], grad, vec_ref[1:2, :])
    total = gl_ref[...] + through
    gm_ref[...] = total
    low = total.astype(LOW)
    gs_ref[...] = low
    ga_ref[...] = dot_nt(low, wo[0]).astype(LOW)
    add_rows(
        s_ref,
        pl.program_id(0) == 0,
        [col_sum(for_gain), col_sum(grad), col_sum(low), col_sum(query)],
    )


def mid_back(grad_q, cross_a, mid, grad_late, vec, self_b, block):
    rows, width = mid.shape
    tile = spec((block, width), lambda i: (i, 0))
    weight = lambda which: spec((1, width, width), lambda i: (which, 0, 0), once=True)
    return run(
        mid_back_body,
        "mid_back",
        (rows // block,),
        (grad_q, cross_a, mid, grad_late, vec, self_b),
        [tile, weight(0), tile, tile, whole(vec.shape), weight(1)],
        [
            ((rows, width), WIDE, tile),
            ((rows, width), LOW, tile),
            ((rows, width), LOW, tile),
            ((8, width), WIDE, spec((8, width), lambda i: (0, 0))),
        ],
        flops=4 * rows * width * width,
    )


def frames_back_body(gk, gv, wk, wv, ge_ref, s_ref):
    grad_v = gv[...]
    ge_ref[...] = (dot_nt(gk[...], wk[0]) + dot_nt(grad_v, wv[0])).astype(LOW)
    add_rows(s_ref, pl.program_id(0) == 0, [col_sum(grad_v)])


def frames_back(grad_k, grad_v, cross_b, block):
    rows, width = grad_k.shape
    tile = spec((block, width), lambda i: (i, 0))
    weight = lambda which: spec((1, width, width), lambda i: (which, 0, 0), once=True)
    return run(
        frames_back_body,
        "frames_back",
        (rows // block,),
        (grad_k, grad_v, cross_b, cross_b),
        [tile, tile, weight(0), weight(1)],
        [((rows, width), LOW, tile), ((8, width), WIDE, spec((8, width), lambda i: (0, 0)))],
        flops=4 * rows * width * width,
    )


def in_back_body(gq, gk, gv, wq, wk, wv, x_ref, gm_ref, vec_ref, gi_ref, s_ref):
    query, value = gq[...], gv[...]
    grad = dot_nt(query, wq[0]) + dot_nt(gk[...], wk[0]) + dot_nt(value, wv[0])
    through, for_gain = norm_backward(x_ref[...].astype(WIDE), grad, vec_ref[0:1, :])
    gi_ref[...] = (gm_ref[...] + through).astype(LOW)
    add_rows(
        s_ref,
        pl.program_id(0) == 0,
        [col_sum(for_gain), col_sum(grad), col_sum(query), col_sum(value)],
    )


def in_back(grad_q, grad_k, grad_v, self_a, self_b, x, grad_mid, vec, block):
    rows, width = x.shape
    tile = spec((block, width), lambda i: (i, 0))
    weight = lambda which: spec((1, width, width), lambda i: (which, 0, 0), once=True)
    return run(
        in_back_body,
        "in_back",
        (rows // block,),
        (grad_q, grad_k, grad_v, self_a, self_a, self_b, x, grad_mid, vec),
        [tile, tile, tile, weight(0), weight(1), weight(0), tile, tile, whole(vec.shape)],
        [((rows, width), LOW, tile), ((8, width), WIDE, spec((8, width), lambda i: (0, 0)))],
        flops=6 * rows * width * width,
    )


def axis_bits(count):
    bits = count.bit_length() - 1
    assert 1 << bits == count
    each = (bits - 1) // 3
    x_bits = list(range(1, 1 + each))
    y_bits = list(range(1 + each, 1 + 2 * each))
    z_bits = list(range(1 + 2 * each, bits))
    return x_bits, y_bits, z_bits


def gather_stages(count, parts):
    x_bits, y_bits, z_bits = (list(reversed(b)) for b in axis_bits(count))
    if parts == 1:
        return [[(b,) for b in bits] for bits in (x_bits, y_bits, z_bits[:1], z_bits[1:], [0])]
    return [
        [(z_bits[0],)],
        [(b,) for b in z_bits[1:]],
        list(zip(y_bits, x_bits)),
        list(zip(x_bits, y_bits)),
        [(0, 0)],
    ]


def scatter_stages(count, parts):
    return [list(reversed(stage)) for stage in reversed(gather_stages(count, parts))]


def swap(values, bit, count):
    return lax.ppermute(values, "fsdp", [(i, i ^ (1 << bit)) for i in range(count)])


def own_bit(bit):
    return (lax.axis_index("fsdp") >> bit) & 1


def weave_body(parts, core_ref, *refs):
    for part in range(parts):
        out = refs[2 * parts + part]
        out[0, :, core_ref[0]] = refs[part][:, 0]
        out[0, :, 1 - core_ref[0]] = refs[parts + part][:, 0]


def weave(held, other, core):
    groups, mats, rows, width = held[0].shape
    parts = len(held)
    half = spec((groups, 1, rows, width), lambda i: (0, i, 0, 0))
    both = spec((1, groups, 2, rows, width), lambda i: (i, 0, 0, 0, 0))
    return run(
        functools.partial(weave_body, parts),
        "weave",
        (mats,),
        (core, *held, *other),
        [smem()] + [half] * (2 * parts),
        [((mats, groups, 2, rows, width), held[0].dtype, both)] * parts,
    )


class Gather:
    def __init__(self, piece, count, parts=2):
        self.count = count
        self.bits = count.bit_length() - 1
        mats, rows, width = piece.shape
        self.shape = (rows, width)
        self.parts = [piece.reshape((1,) * self.bits + (mats, rows, width))]
        self.stages = gather_stages(count, parts)
        self.flight = None

    def land(self):
        if self.flight is not None:
            parts = []
            for held, (bit, other) in zip(self.parts, self.flight):
                axis = self.bits - 1 - bit
                parts.append(
                    jnp.where(
                        own_bit(bit) == 0,
                        jnp.concatenate([held, other], axis),
                        jnp.concatenate([other, held], axis),
                    )
                )
            self.parts = parts
            self.flight = None

    def ready(self):
        self.land()
        if len(self.stages[0][0]) == 2 and len(self.parts) == 1:
            self.parts = jnp.split(self.parts[0], 2, self.bits)
        return self.parts

    def launch(self, parts):
        self.parts = parts
        for place, step in enumerate(self.stages.pop(0)):
            if place:
                self.land()
            self.flight = [(bit, swap(part, bit, self.count)) for bit, part in zip(step, self.parts)]

    def result(self):
        rows, width = self.shape
        merged = lambda v: v.reshape((self.count // 2,) + v.shape[self.bits :])
        held = [merged(v) for v in self.parts]
        other = [merged(v) for _, v in self.flight]
        if len(held) == 1:
            self.land()
            return [self.parts[0].reshape(self.count * rows, width)]
        done = weave(held, other, own_bit(0).astype(jnp.int32).reshape(1))
        return [v.reshape(v.shape[0], self.count * rows, width) for v in done]


class Scatter:
    def __init__(self, parts, count):
        self.count = count
        self.bits = count.bit_length() - 1
        self.kind = parts[0][0].dtype
        self.stages = scatter_stages(count, len(parts))
        self.sends, self.pairs = [], []
        for part in parts:
            if len(part) == 1:
                mats, rows, width = part[0].shape
                groups = part[0].reshape(mats, count // 2, 2, rows // count, width)
                part = [
                    jnp.swapaxes(lax.dynamic_index_in_dim(groups, side, 2, False), 0, 1)
                    for side in (1 - own_bit(0), own_bit(0))
                ]
            self.shape = part[0].shape[2:]
            shaped = [v.reshape((2,) * (self.bits - 1) + (1,) + v.shape[1:]) for v in part]
            self.sends.append(shaped[0])
            self.pairs.append((shaped[1], None))

    def pick(self, pair, bit, side):
        axis = self.bits - 1 - bit
        values = [lax.dynamic_slice_in_dim(v, side, 1, axis) for v in pair]
        return self.total(values, self.kind)

    def total(self, pair, kind):
        return (pair[0].astype(WIDE) + pair[1].astype(WIDE)).astype(kind)

    def ready(self):
        if self.sends is not None:
            return self.sends
        step = self.stages[0][0]
        if len(step) == 1 and len(self.pairs) == 2:
            self.pairs = [
                tuple(jnp.concatenate([p[i] for p in self.pairs], self.bits) for i in (0, 1))
            ]
        return [self.pick(pair, bit, 1 - own_bit(bit)) for bit, pair in zip(step, self.pairs)]

    def launch(self, sends):
        for place, step in enumerate(self.stages.pop(0)):
            if place:
                sends = [self.pick(p, b, 1 - own_bit(b)) for b, p in zip(step, self.pairs)]
            flight = [swap(v, bit, self.count) for bit, v in zip(step, sends)]
            if self.sends is None:
                kept = [self.pick(p, bit, own_bit(bit)) for bit, p in zip(step, self.pairs)]
            else:
                kept, self.sends = [p[0] for p in self.pairs], None
            self.pairs = list(zip(kept, flight))

    def result(self):
        total = jnp.concatenate([self.total(p, WIDE) for p in self.pairs], self.bits)
        return total.reshape((-1,) + self.shape)


def tick(chains, values=()):
    ready = [chain.ready() for chain in chains]
    ready, values = lax.optimization_barrier((ready, values))
    for chain, parts in zip(chains, ready):
        chain.launch(parts)
    return values


def shards(
    count,
    hidden_in,
    encoder_states,
    lengths,
    out_grad,
    attn_in,
    attn_out,
    fc_in,
    fc_out,
    gains,
    biases,
    ffn_bias,
):
    batch, length, width = hidden_in.shape
    rows = batch * length
    block = length // 2
    frame_rows = encoder_states.shape[1]
    share = gains.shape[1]
    ff_share = ffn_bias.shape[0]
    mats = ff_share // share

    small = jnp.concatenate([gains.reshape(-1), biases.reshape(-1), ffn_bias])
    small_count = small.shape[0]
    small_rows = -(-(small_count + 5) // 128)
    small_size = small_rows * 128
    small = jnp.pad(small, (0, small_size - small_count)).reshape(1, small_rows, 128)
    fc_in_mats = fc_in.reshape(share, count, mats, share).transpose(2, 0, 1, 3).reshape(mats, share, width)
    fc_out_mats = fc_out.reshape(mats, share, width)
    g_small = Gather(small, count, 1)
    g_self = Gather(jnp.concatenate([attn_in[0:3], attn_out[0:1]]), count)
    g_cross = Gather(jnp.concatenate([attn_in[3:4], attn_out[1:2], attn_in[4:6]]), count)
    g_ffn = Gather(jnp.concatenate([fc_in_mats, fc_out_mats]), count)

    core = own_bit(0).astype(jnp.int32).reshape(1)
    x = hidden_in.reshape(rows, width)
    frames = encoder_states.reshape(-1, width)
    valid = jnp.arange(length)[None, :, None] < lengths[:, None, None]
    grad = jnp.where(valid, out_grad, jnp.zeros_like(out_grad)).reshape(rows, width)

    tick([g_self, g_small])
    tick([g_self, g_small])
    tick([g_self, g_small, g_cross])
    tick([g_self, g_small, g_cross, g_ffn])
    tick([g_self, g_small, g_cross, g_ffn])
    small = g_small.result()[0].astype(jnp.float32).reshape(count, small_size)
    vec = small[:, : 13 * share].reshape(count, 13, share).transpose(1, 0, 2).reshape(13, width)
    vec = jnp.pad(vec, ((0, 3), (0, 0)))
    bias = small[:, 13 * share : small_count].reshape(count, mats, share)
    bias = bias.transpose(1, 0, 2).reshape(mats, 1, width)
    self_a, self_b = g_self.result()
    x = tick([g_cross], x)
    norm_one, query, key, value = qkv(x, vec, self_a, self_b, block)
    query, key, value = tick([g_ffn], (query, key, value))
    attended = attend(query, key, value, batch, True)
    mid, norm_two, square_self = mid_stage(lengths, attended, x, vec, self_b, batch, block)
    norm_two = tick([g_cross], norm_two)
    norm_two = tick([g_ffn], norm_two)
    cross_a, cross_b = g_cross.result()
    cross_q, cross_k, cross_v = cross_stage(norm_two, frames, vec, cross_a, cross_b, batch)
    cross_attended = attend(cross_q, cross_k, cross_v, batch, False)
    late, norm_three, square_cross = late_stage(lengths, cross_attended, mid, vec, cross_a, batch, block)
    norm_three = tick([g_ffn], norm_three)
    w_in, w_out = g_ffn.result()
    grad_norm, d_in, d_out, sums_ff, result, square_rest = ffn_stage(
        lengths, core, count, norm_three, grad, bias, w_in, w_out, None, late, vec, batch, block
    )
    s_ffn = Scatter([d_in, d_out], count)
    grad_norm = tick([s_ffn], grad_norm)
    grad_late, grad_cross, grad_cross_att, sums_late = late_back(
        grad_norm, late, grad, vec, cross_a, block
    )
    grad_cross_att = tick([s_ffn], grad_cross_att)
    grad_cq, grad_ck, grad_cv = attend_back(
        cross_q, cross_k, cross_v, grad_cross_att, batch, False
    )
    d_cross_a = weight_grads([(norm_two, grad_cq), (cross_attended, grad_cross)], core, count)
    d_cross_b = weight_grads([(frames, grad_ck), (frames, grad_cv)], core, count)
    s_cross = Scatter([d_cross_a, d_cross_b], count)
    grad_cq, grad_ck, grad_cv = tick([s_cross], (grad_cq, grad_ck, grad_cv))
    grad_mid, grad_self, grad_att, sums_mid = mid_back(
        grad_cq, cross_a, mid, grad_late, vec, self_b, block
    )
    grad_frames, sums_frames = frames_back(grad_ck, grad_cv, cross_b, frame_rows)
    grad_att, grad_frames = tick([s_cross, s_ffn], (grad_att, grad_frames))
    grad_q, grad_k, grad_v = attend_back(query, key, value, grad_att, batch, True)
    d_self_a = weight_grads([(norm_one, grad_q), (norm_one, grad_k)], core, count)
    d_self_b = weight_grads([(norm_one, grad_v), (attended, grad_self)], core, count)
    s_self = Scatter([d_self_a, d_self_b], count)
    grad_q, grad_k, grad_v = tick([s_self], (grad_q, grad_k, grad_v))
    grad_q, grad_k, grad_v = tick([s_cross, s_ffn], (grad_q, grad_k, grad_v))
    grad_q, grad_k, grad_v = tick([s_self], (grad_q, grad_k, grad_v))
    grad_in, sums_one = in_back(grad_q, grad_k, grad_v, self_a, self_b, x, grad_mid, vec, block)

    sums_one = tick([s_self, s_cross, s_ffn], sums_one)
    sum_rows = jnp.stack(
        [sums_one[0], sums_mid[0], sums_late[0]]
        + [sums_one[2], sums_one[3], sums_mid[2], sums_mid[3], sums_frames[0], sums_late[2], square_rest[2]]
        + [sums_one[1], sums_mid[1], sums_late[1]]
    )
    squares = jnp.stack([square_rest[0], square_self[0], square_cross[0], square_rest[1]])
    stats = jnp.concatenate([jnp.sum(squares, -1), jnp.sum(lengths).astype(WIDE)[None]])
    sums_ff = sums_ff.reshape(mats, count, share)
    sums = jnp.concatenate(
        [
            sum_rows.reshape(13, count, share).transpose(1, 0, 2).reshape(count, 13 * share),
            sums_ff.transpose(1, 0, 2).reshape(count, ff_share),
            jnp.broadcast_to(stats[None], (count, 5)),
        ],
        1,
    )
    sums = jnp.pad(sums, ((0, 0), (0, small_size - sums.shape[1])))
    s_small = Scatter([[sums.reshape(1, count * small_rows, 128)]], count)
    tick([s_small])
    tick([s_small])
    tick([s_small])
    tick([s_self, s_cross, s_small])
    tick([s_self, s_small])
    d_ffn = s_ffn.result()
    d_in_all, d_out_all = d_ffn[:mats], d_ffn[mats:]
    d_cross = s_cross.result()
    d_self = s_self.result()
    small = s_small.result().reshape(-1)
    stats = small[small_count : small_count + 5]
    rms = jnp.sqrt(stats[:4] / (stats[4] * width))
    return (
        result.reshape(hidden_in.shape),
        grad_in.reshape(hidden_in.shape),
        grad_frames.reshape(encoder_states.shape),
        jnp.concatenate([d_self[:3], d_cross[:1], d_cross[2:]]),
        jnp.concatenate([d_self[3:], d_cross[1:2]]),
        d_in_all.reshape(mats, share, count, share).transpose(1, 2, 0, 3).reshape(share, -1),
        d_out_all.reshape(ff_share, width),
        small[: 3 * share].reshape(3, share),
        small[3 * share : 13 * share].reshape(10, share),
        small[13 * share : small_count],
        rms,
    )


def solution(mesh):
    placed = (
        P("fsdp", None, None),
        P("fsdp", None, None),
        P("fsdp"),
        P("fsdp", None, None),
        P(None, "fsdp", None),
        P(None, "fsdp", None),
        P("fsdp", None),
        P("fsdp", None),
        P(None, "fsdp"),
        P(None, "fsdp"),
        P("fsdp"),
    )
    return jax.shard_map(
        functools.partial(shards, mesh.shape["fsdp"]),
        mesh=mesh,
        in_specs=placed,
        out_specs=(
            P("fsdp", None, None),
            P("fsdp", None, None),
            P("fsdp", None, None),
            P(None, "fsdp", None),
            P(None, "fsdp", None),
            P("fsdp", None),
            P("fsdp", None),
            P(None, "fsdp"),
            P(None, "fsdp"),
            P("fsdp"),
            P(),
        ),
        check_vma=False,
    )
```

```python
import functools
import math

import jax
import jax.numpy as jnp
from jax import lax
from jax.experimental import pallas as pl
from jax.experimental.pallas import tpu as pltpu
from jax.sharding import PartitionSpec as P

NORM_EPS = 1e-05
LOW = jnp.bfloat16
WIDE = jnp.float32
HEADS = 12
PAIR = 128
HALF_PAIR = 64
SCALE = 0.125


def dot_nn(left, right):
    return lax.dot_general(left, right, (((1,), (0,)), ((), ())), preferred_element_type=WIDE)


def dot_nt(left, right):
    return lax.dot_general(left, right, (((1,), (1,)), ((), ())), preferred_element_type=WIDE)


def dot_tn(left, right):
    return lax.dot_general(left, right, (((0,), (0,)), ((), ())), preferred_element_type=WIDE)


def spec(block, index, once=False):
    if once:
        return pl.BlockSpec(block, index, pipeline_mode=pl.Buffered(1))
    return pl.BlockSpec(block, index)


def run(body, name, grid, operands, in_specs, outs, scratch=(), flops=0, exps=0, limit=14, far=()):
    moved = sum(o.size * o.dtype.itemsize for o in operands)
    moved += sum(math.prod(s) * jnp.dtype(d).itemsize for s, d, _ in outs)
    return pl.pallas_call(
        body,
        name=name,
        grid=grid,
        in_specs=in_specs,
        out_specs=[o[2] for o in outs],
        out_shape=[
            pltpu.HBM(o[0], o[1]) if i in far else jax.ShapeDtypeStruct(o[0], o[1])
            for i, o in enumerate(outs)
        ],
        scratch_shapes=list(scratch),
        compiler_params=pltpu.CompilerParams(
            dimension_semantics=("arbitrary",) * len(grid), vmem_limit_bytes=limit << 20
        ),
        cost_estimate=pl.CostEstimate(flops=flops, transcendentals=exps, bytes_accessed=moved),
    )(*operands)


def in_hbm(values):
    return pltpu.with_memory_space_constraint(values, pltpu.HBM)


def normalised(values):
    center = values - jnp.mean(values, -1, keepdims=True)
    spread = jnp.mean(center * center, -1, keepdims=True)
    scale = lax.rsqrt(spread + NORM_EPS)
    return center * scale, scale


def norm_backward(values, grad, gain):
    unit, scale = normalised(values)
    inner = grad * gain
    mean_inner = jnp.mean(inner, -1, keepdims=True)
    mean_unit = jnp.mean(inner * unit, -1, keepdims=True)
    return scale * (inner - mean_inner - unit * mean_unit), grad * unit


def col_sum(values):
    return jnp.sum(values.astype(WIDE), 0, keepdims=True)


def add_rows(ref, first, rows):
    @pl.when(first)
    def _():
        ref[...] = jnp.zeros_like(ref)

    for place, row in enumerate(rows):
        ref[place : place + 1, :] += row


def masked_squares(values, length_ref, step, per_seq):
    rows = values.shape[0]
    start = (step % per_seq) * rows
    index = start + lax.broadcasted_iota(jnp.int32, (rows, 1), 0)
    inside = index < length_ref[step // per_seq]
    return col_sum(jnp.where(inside, values * values, 0.0))


def qkv_body(x_ref, vec_ref, wq, wk, wv, n_ref, q_ref, k_ref, v_ref):
    unit, _ = normalised(x_ref[...].astype(WIDE))
    norm = (unit * vec_ref[0:1, :] + vec_ref[10:11, :]).astype(LOW)
    n_ref[...] = norm
    query = (dot_nn(norm, wq[0]) + vec_ref[3:4, :]).astype(LOW)
    q_ref[...] = query * jnp.asarray(SCALE, LOW)
    k_ref[...] = dot_nn(norm, wk[0]).astype(LOW)
    v_ref[...] = (dot_nn(norm, wv[0]) + vec_ref[4:5, :]).astype(LOW)


def whole(shape):
    return spec(shape, lambda *_: (0,) * len(shape), once=True)


def qkv(x, vec, self_a, self_b, block):
    rows, width = x.shape
    row = lambda i: (i, 0)
    weight = lambda which: spec((1, width, width), lambda i: (which, 0, 0), once=True)
    return run(
        qkv_body,
        "qkv",
        (rows // block,),
        (x, vec, self_a, self_a, self_b),
        [spec((block, width), row), whole(vec.shape), weight(0), weight(1), weight(0)],
        [((rows, width), LOW, spec((block, width), row))] * 4,
        flops=6 * rows * width * width,
    )


def head_lanes(values, head):
    lane = lax.broadcasted_iota(jnp.int32, (1, PAIR), 1)
    inside = lane < HALF_PAIR if head == 0 else lane >= HALF_PAIR
    return jnp.where(inside, values, jnp.zeros_like(values))


def attend_cross_body(pairs, q_ref, k_ref, v_ref, o_ref):
    for pair in range(pairs):
        lanes = slice(pair * PAIR, (pair + 1) * PAIR)
        values, keys, queries = v_ref[:, lanes], k_ref[:, lanes], q_ref[:, lanes]
        total = None
        for head in (0, 1):
            scores = dot_nt(head_lanes(queries, head), keys)
            exps = jnp.exp(scores - jnp.max(scores, -1, keepdims=True))
            probs = exps * (1.0 / jnp.sum(exps, -1, keepdims=True))
            part = dot_nn(probs.astype(LOW), head_lanes(values, head))
            total = part if total is None else total + part
        o_ref[:, lanes] = total.astype(LOW)


def attend_body(pairs, step_rows, q_ref, k_ref, v_ref, o_ref):
    length = q_ref.shape[0]
    starts = list(range(0, length, step_rows))
    for pair in range(pairs):
        lanes = slice(pair * PAIR, (pair + 1) * PAIR)
        turned = v_ref[:, lanes].T
        keys = [head_lanes(k_ref[:, lanes], head) for head in (0, 1)]
        work = []
        for start in starts:
            stop = min(start + step_rows, length)
            queries = q_ref[start:stop, lanes]
            cuts = ([(0, start)] if start else []) + [(start, stop)]
            for head in (0, 1):
                parts = []
                for low, high in cuts:
                    scores = dot_nt(keys[head][low:high], queries)
                    if low == start:
                        key_at = lax.broadcasted_iota(jnp.int32, scores.shape, 0)
                        query_at = lax.broadcasted_iota(jnp.int32, scores.shape, 1)
                        scores = jnp.where(key_at <= query_at, scores, -1e30)
                    parts.append(scores)
                work.append((start, stop, head, cuts, parts))
        tops = []
        for start, stop, head, cuts, parts in work:
            top = jnp.max(parts[0], 0, keepdims=True)
            for scores in parts[1:]:
                top = jnp.maximum(top, jnp.max(scores, 0, keepdims=True))
            tops.append(top)
        exps = [[jnp.exp(s - top) for s in item[4]] for item, top in zip(work, tops)]
        totals = [sum(jnp.sum(e, 0, keepdims=True) for e in group) for group in exps]
        outs = []
        for (start, stop, head, cuts, _), group, total in zip(work, exps, totals):
            out = None
            for (low, high), e in zip(cuts, group):
                part = dot_nn(turned[head * HALF_PAIR : (head + 1) * HALF_PAIR, low:high], e.astype(LOW))
                out = part if out is None else out + part
            outs.append(out * (1.0 / total))
        for place, start in enumerate(starts):
            stop = min(start + step_rows, length)
            both = jnp.concatenate(outs[2 * place : 2 * place + 2], 0)
            o_ref[start:stop, lanes] = both.T.astype(LOW)


def attend(q, k, v, batch, causal, pairs=6, step_rows=128):
    rows, width = q.shape
    length, frames = rows // batch, k.shape[0] // batch
    lanes = pairs * PAIR
    at = lambda b, p: (b, p)
    return run(
        functools.partial(attend_body, pairs, step_rows) if causal else functools.partial(attend_cross_body, pairs),
        "attend_self" if causal else "attend_cross",
        (batch, width // lanes),
        (q, k, v),
        [spec((length, lanes), at), spec((frames, lanes), at), spec((frames, lanes), at)],
        [((rows, width), LOW, spec((length, lanes), at))],
        flops=4 * rows * frames * width,
        exps=rows * frames * HEADS,
    )[0]


def attend_back_body(causal, pairs, step_rows, q_ref, k_ref, v_ref, g_ref, gq_ref, gk_ref, gv_ref, dk, dv):
    length = q_ref.shape[0]
    frames = k_ref.shape[0]
    starts = list(range(0, length, step_rows))
    for pair in range(pairs):
        lanes = slice(pair * PAIR, (pair + 1) * PAIR)
        keys = [head_lanes(k_ref[:, lanes], head) for head in (0, 1)]
        values = [head_lanes(v_ref[:, lanes], head) for head in (0, 1)]
        work = []
        for start in starts:
            stop = min(start + step_rows, length)
            cuts = ([(0, start)] if start else []) + [(start, stop)] if causal else [(0, frames)]
            for head in (0, 1):
                queries, grads = q_ref[start:stop, lanes], g_ref[start:stop, lanes]
                parts = []
                for low, high in cuts:
                    scores = dot_nt(keys[head][low:high], queries)
                    if causal and low == start:
                        key_at = lax.broadcasted_iota(jnp.int32, scores.shape, 0)
                        query_at = lax.broadcasted_iota(jnp.int32, scores.shape, 1)
                        scores = jnp.where(key_at <= query_at, scores, -1e30)
                    parts.append(scores)
                grad_parts = [dot_nt(values[head][low:high], grads) for low, high in cuts]
                work.append((start, stop, head, cuts, parts, grad_parts))
        probs = []
        for item in work:
            parts = item[4]
            top = jnp.max(parts[0], 0, keepdims=True)
            for scores in parts[1:]:
                top = jnp.maximum(top, jnp.max(scores, 0, keepdims=True))
            exps = [jnp.exp(scores - top) for scores in parts]
            total = 1.0 / sum(jnp.sum(e, 0, keepdims=True) for e in exps)
            probs.append([e * total for e in exps])
        scores = []
        for item, group in zip(work, probs):
            weighted = [p * g for p, g in zip(group, item[5])]
            inner = sum(jnp.sum(w, 0, keepdims=True) for w in weighted)
            scores.append([(w - p * inner).astype(LOW) for w, p in zip(weighted, group)])
        grad_q = {}
        for (start, stop, head, cuts, _, _), group, low_scores in zip(work, probs, scores):
            queries = head_lanes(q_ref[start:stop, lanes], head)
            grads = head_lanes(g_ref[start:stop, lanes], head)
            for (low, high), p, s in zip(cuts, group, low_scores):
                part_v = dot_nn(p.astype(LOW), grads)
                part_k = dot_nn(s, queries)
                part_q = dot_tn(s, keys[head][low:high])
                grad_q[start] = part_q if start not in grad_q else grad_q[start] + part_q
                if head == 0 and (low == start or not causal and start == 0):
                    dv[low:high, :] = part_v
                    dk[low:high, :] = part_k
                else:
                    dv[low:high, :] += part_v
                    dk[low:high, :] += part_k
        for start, total in grad_q.items():
            gq_ref[start : start + total.shape[0], lanes] = (total * SCALE).astype(LOW)
        gk_ref[:, lanes] = dk[...].astype(LOW)
        gv_ref[:, lanes] = dv[...].astype(LOW)


def attend_back(q, k, v, grad, batch, causal, pairs=6):
    rows, width = q.shape
    length, frames = rows // batch, k.shape[0] // batch
    lanes = pairs * PAIR
    at = lambda b, p: (b, p)
    long, short = spec((length, lanes), at), spec((frames, lanes), at)
    return run(
        functools.partial(attend_back_body, causal, pairs, 128 if causal else length),
        "attend_self_back" if causal else "attend_cross_back",
        (batch, width // lanes),
        (q, k, v, grad),
        [long, short, short, long],
        [((rows, width), LOW, long), (k.shape, LOW, short), (k.shape, LOW, short)],
        [pltpu.VMEM((frames, PAIR), WIDE)] * 2,
        flops=10 * rows * frames * width,
        exps=rows * frames * HEADS,
    )


def mid_body(per_seq, len_ref, a_ref, x_ref, vec_ref, wo, mid_ref, n_ref, s_ref):
    step = pl.program_id(0)
    branch = dot_nn(a_ref[...], wo[0]) + vec_ref[5:6, :]
    mid = x_ref[...].astype(WIDE) + branch
    mid_ref[...] = mid
    unit, _ = normalised(mid)
    n_ref[...] = (unit * vec_ref[1:2, :] + vec_ref[11:12, :]).astype(LOW)
    add_rows(s_ref, step == 0, [masked_squares(branch, len_ref, step, per_seq)])


def smem():
    return pl.BlockSpec(memory_space=pltpu.SMEM)


def mid_stage(lengths, attended, x, vec, self_b, batch, block):
    rows, width = x.shape
    weight = spec((1, width, width), lambda i: (1, 0, 0), once=True)
    tile = spec((block, width), lambda i: (i, 0))
    return run(
        functools.partial(mid_body, rows // batch // block),
        "mid_stage",
        (rows // block,),
        (lengths, attended, x, vec, self_b),
        [smem(), tile, tile, whole(vec.shape), weight],
        [
            ((rows, width), WIDE, tile),
            ((rows, width), LOW, tile),
            ((8, width), WIDE, spec((8, width), lambda i: (0, 0))),
        ],
        flops=2 * rows * width * width,
    )


def cross_body(n_ref, f_ref, vec_ref, wq, wk, wv, q_ref, k_ref, v_ref):
    query = (dot_nn(n_ref[...], wq[0]) + vec_ref[6:7, :]).astype(LOW)
    q_ref[...] = query * jnp.asarray(SCALE, LOW)
    frames = f_ref[...]
    k_ref[...] = dot_nn(frames, wk[0]).astype(LOW)
    v_ref[...] = (dot_nn(frames, wv[0]) + vec_ref[7:8, :]).astype(LOW)


def cross_stage(norm, frames, vec, cross_a, cross_b, batch):
    width = norm.shape[1]
    rows, frame_rows = norm.shape[0], frames.shape[0]
    long = spec((rows // batch, width), lambda i: (i, 0))
    short = spec((frame_rows // batch, width), lambda i: (i, 0))
    weight = lambda which: spec((1, width, width), lambda i: (which, 0, 0), once=True)
    return run(
        cross_body,
        "cross_stage",
        (batch,),
        (norm, frames, vec, cross_a, cross_b, cross_b),
        [long, short, whole(vec.shape), weight(0), weight(0), weight(1)],
        [((rows, width), LOW, long), ((frame_rows, width), LOW, short), ((frame_rows, width), LOW, short)],
        flops=(2 * rows + 4 * frame_rows) * width * width,
    )


def late_body(per_seq, len_ref, a_ref, mid_ref, vec_ref, wo, late_ref, n_ref, s_ref):
    step = pl.program_id(0)
    branch = dot_nn(a_ref[...], wo[0]) + vec_ref[8:9, :]
    late = mid_ref[...] + branch
    late_ref[...] = late
    unit, _ = normalised(late)
    n_ref[...] = (unit * vec_ref[2:3, :] + vec_ref[12:13, :]).astype(LOW)
    add_rows(s_ref, step == 0, [masked_squares(branch, len_ref, step, per_seq)])


def late_stage(lengths, attended, mid, vec, cross_a, batch, block):
    rows, width = mid.shape
    tile = spec((block, width), lambda i: (i, 0))
    return run(
        functools.partial(late_body, rows // batch // block),
        "late_stage",
        (rows // block,),
        (lengths, attended, mid, vec, cross_a),
        [smem(), tile, tile, whole(vec.shape), spec((1, width, width), lambda i: (1, 0, 0), once=True)],
        [
            ((rows, width), WIDE, tile),
            ((rows, width), LOW, tile),
            ((8, width), WIDE, spec((8, width), lambda i: (0, 0))),
        ],
        flops=2 * rows * width * width,
        far=(0,),
    )


def ffn_body(first, last, batch, block, split, len_ref, core_ref, n_ref, g_ref, b_ref, wi_ref, wo_ref, *refs):
    refs = list(refs)
    before = [] if first else [refs.pop(0), refs.pop(0)]
    late_ref, vec_ref = (refs.pop(0), refs.pop(0)) if last else (None, None)
    gn_ref = refs.pop(0)
    di_refs = [refs.pop(0) for _ in range(split)]
    do_refs = [refs.pop(0) for _ in range(split)]
    sf_ref, f_ref = refs[:2]
    rest = refs[2:]
    s_ref = rest.pop(0) if last else None
    hidden_ref, pre_ref = rest[:2]
    acc_ref = rest[2] if last else f_ref
    step = pl.program_id(0)
    rows = n_ref.shape[0]

    @pl.when(step == 0)
    def _():
        if first:
            acc_ref[...] = jnp.zeros_like(acc_ref)
            gn_ref[...] = jnp.zeros_like(gn_ref)
        else:
            acc_ref[...] = before[0][...]
            gn_ref[...] = before[1][...]

    def chunk(place, carry):
        at = pl.ds(pl.multiple_of(place * block, block), block)
        pre = dot_nn(n_ref[at, :], wi_ref[0]) + b_ref[0]
        below = 0.5 + 0.5 * lax.erf(pre * (0.5**0.5))
        density = jnp.exp(-0.5 * pre * pre) * (1.0 / math.sqrt(2.0 * math.pi))
        hidden = (pre * below).astype(LOW)
        hidden_ref[at, :] = hidden
        acc_ref[at, :] += dot_nn(hidden, wo_ref[0])
        grad = dot_nt(g_ref[at, :], wo_ref[0])
        grad = (grad * (below + pre * density)).astype(LOW)
        pre_ref[at, :] = grad
        gn_ref[at, :] += dot_nt(grad, wi_ref[0])
        return carry

    lax.fori_loop(0, rows // block, chunk, 0)
    sf_ref[0] = col_sum(pre_ref[...])
    store_grad(dot_tn(n_ref[...], pre_ref[...]), di_refs, 0, core_ref)
    store_grad(dot_tn(hidden_ref[...], g_ref[...]), do_refs, 0, core_ref)
    if last:
        @pl.when(step == pl.num_programs(0) - 1)
        def _():
            s_ref[...] = jnp.zeros_like(s_ref)

            def finish(place, carry):
                at = pl.ds(pl.multiple_of(place * block, block), block)
                branch = acc_ref[at, :] + vec_ref[9:10, :]
                result = late_ref[at, :] + branch
                f_ref[at, :] = result.astype(LOW)
                per_seq = rows // batch // block
                s_ref[0:1, :] += masked_squares(result, len_ref, place, per_seq)
                s_ref[1:2, :] += masked_squares(branch, len_ref, place, per_seq)
                s_ref[2:3, :] += col_sum(g_ref[at, :])
                return carry

            lax.fori_loop(0, rows // block, finish, 0)


def ffn_stage(lengths, core, count, norm, grad, bias, w_in, w_out, before, late, vec, batch, block):
    rows, width = norm.shape
    mats = w_in.shape[0]
    first, last = before is None, late is not None
    mat = spec((1, width, width), lambda j: (j, 0, 0))
    line = spec((1, 1, width), lambda j: (j, 0, 0))
    operands = [lengths, core, norm, grad, bias, w_in, w_out]
    specs = [smem(), smem(), whole(norm.shape), whole(grad.shape), line, mat, mat]
    if not first:
        operands += list(before)
        specs += [whole((rows, width))] * 2
    if last:
        operands += [late, vec]
        specs += [whole((rows, width)), whole(vec.shape)]
    fixed = whole((rows, width))
    grads = grad_outs(mats, width, count, (1, width), lambda j: (j, 0))
    outs = [
        ((rows, width), WIDE, fixed),
        *grads,
        *grads,
        ((mats, 1, width), WIDE, line),
        ((rows, width), LOW if last else WIDE, fixed),
    ]
    scratch = [pltpu.VMEM((rows, width), LOW)] * 2
    if last:
        outs.append(((8, width), WIDE, whole((8, width))))
        scratch.append(pltpu.VMEM((rows, width), WIDE))
    done = run(
        functools.partial(ffn_body, first, last, batch, block, len(grads)),
        "ffn_stage",
        (mats,),
        tuple(operands),
        specs,
        outs,
        scratch,
        flops=12 * rows * width * width * mats,
        exps=2 * rows * width * mats,
        limit=30,
        far=(0, 2, 4),
    )
    split = len(grads)
    return done[0], done[1 : 1 + split], done[1 + split : 1 + 2 * split], *done[1 + 2 * split :]


def late_back_body(gn_ref, late_ref, og_ref, vec_ref, wo, gl_ref, gc_ref, ga_ref, s_ref):
    grad = gn_ref[...]
    through, for_gain = norm_backward(late_ref[...], grad, vec_ref[2:3, :])
    total = og_ref[...].astype(WIDE) + through
    gl_ref[...] = total
    low = total.astype(LOW)
    gc_ref[...] = low
    ga_ref[...] = dot_nt(low, wo[0]).astype(LOW)
    add_rows(s_ref, pl.program_id(0) == 0, [col_sum(for_gain), col_sum(grad), col_sum(low)])


def late_back(grad_norm, late, grad, vec, cross_a, block):
    rows, width = late.shape
    tile = spec((block, width), lambda i: (i, 0))
    return run(
        late_back_body,
        "late_back",
        (rows // block,),
        (in_hbm(grad_norm), in_hbm(late), grad, vec, cross_a),
        [
            tile,
            tile,
            tile,
            whole(vec.shape),
            spec((1, width, width), lambda i: (1, 0, 0), once=True),
        ],
        [
            ((rows, width), WIDE, tile),
            ((rows, width), LOW, tile),
            ((rows, width), LOW, tile),
            ((8, width), WIDE, spec((8, width), lambda i: (0, 0))),
        ],
        flops=2 * rows * width * width,
    )


def store_grad(grad, outs, place, core_ref):
    if len(outs) == 1:
        outs[0][place] = grad.astype(LOW)
        return
    groups, _, rows, width = outs[0].shape
    pairs = grad.reshape(groups, 2, rows, width)
    for core in (0, 1):

        @pl.when(core_ref[0] == core)
        def _(core=core):
            outs[0][:, place] = pairs[:, 1 - core].astype(LOW)
            outs[1][:, place] = pairs[:, core].astype(LOW)


def grad_outs(mats, width, count, block, index):
    rows = width // count
    if rows % 8 or block[1] % (2 * rows):
        whole_out = spec(block + (width,), lambda i: index(i) + (0,))
        return [((mats, width, width), LOW, whole_out)]
    groups = block[1] // (2 * rows)
    half = spec((groups, block[0], rows, width), lambda i: index(i)[::-1] + (0, 0))
    return [((count // 2, mats, rows, width), LOW, half)] * 2


def weights_body(count, core_ref, *refs):
    outs = refs[2 * count :]
    for place in range(count):
        grad = dot_tn(refs[2 * place][...], refs[2 * place + 1][...])
        store_grad(grad, outs, place, core_ref)


def weight_grads(pairs, core, count):
    width = pairs[0][0].shape[1]
    block = width // 2
    operands, specs = [core], [smem()]
    for left, right in pairs:
        operands += [left, right]
        specs += [spec((left.shape[0], block), lambda j: (0, j)), whole(right.shape)]
    return run(
        functools.partial(weights_body, len(pairs)),
        "weight_grads",
        (width // block,),
        tuple(operands),
        specs,
        grad_outs(len(pairs), width, count, (len(pairs), block), lambda j: (0, j)),
        flops=sum(2 * left.shape[0] * width * width for left, _ in pairs),
    )


def mid_back_body(gq, wq, mid_ref, gl_ref, vec_ref, wo, gm_ref, gs_ref, ga_ref, s_ref):
    query = gq[...]
    grad = dot_nt(query, wq[0])
    through, for_gain = norm_backward(mid_ref[...], grad, vec_ref[1:2, :])
    total = gl_ref[...] + through
    gm_ref[...] = total
    low = total.astype(LOW)
    gs_ref[...] = low
    ga_ref[...] = dot_nt(low, wo[0]).astype(LOW)
    add_rows(
        s_ref,
        pl.program_id(0) == 0,
        [col_sum(for_gain), col_sum(grad), col_sum(low), col_sum(query)],
    )


def mid_back(grad_q, cross_a, mid, grad_late, vec, self_b, block):
    rows, width = mid.shape
    tile = spec((block, width), lambda i: (i, 0))
    weight = lambda which: spec((1, width, width), lambda i: (which, 0, 0), once=True)
    return run(
        mid_back_body,
        "mid_back",
        (rows // block,),
        (grad_q, cross_a, mid, grad_late, vec, self_b),
        [tile, weight(0), tile, tile, whole(vec.shape), weight(1)],
        [
            ((rows, width), WIDE, tile),
            ((rows, width), LOW, tile),
            ((rows, width), LOW, tile),
            ((8, width), WIDE, spec((8, width), lambda i: (0, 0))),
        ],
        flops=4 * rows * width * width,
    )


def frames_back_body(gk, gv, wk, wv, ge_ref, s_ref):
    grad_v = gv[...]
    ge_ref[...] = (dot_nt(gk[...], wk[0]) + dot_nt(grad_v, wv[0])).astype(LOW)
    add_rows(s_ref, pl.program_id(0) == 0, [col_sum(grad_v)])


def frames_back(grad_k, grad_v, cross_b, block):
    rows, width = grad_k.shape
    tile = spec((block, width), lambda i: (i, 0))
    weight = lambda which: spec((1, width, width), lambda i: (which, 0, 0), once=True)
    return run(
        frames_back_body,
        "frames_back",
        (rows // block,),
        (grad_k, grad_v, cross_b, cross_b),
        [tile, tile, weight(0), weight(1)],
        [((rows, width), LOW, tile), ((8, width), WIDE, spec((8, width), lambda i: (0, 0)))],
        flops=4 * rows * width * width,
    )


def in_back_body(gq, gk, gv, wq, wk, wv, x_ref, gm_ref, vec_ref, gi_ref, s_ref):
    query, value = gq[...], gv[...]
    grad = dot_nt(query, wq[0]) + dot_nt(gk[...], wk[0]) + dot_nt(value, wv[0])
    through, for_gain = norm_backward(x_ref[...].astype(WIDE), grad, vec_ref[0:1, :])
    gi_ref[...] = (gm_ref[...] + through).astype(LOW)
    add_rows(
        s_ref,
        pl.program_id(0) == 0,
        [col_sum(for_gain), col_sum(grad), col_sum(query), col_sum(value)],
    )


def in_back(grad_q, grad_k, grad_v, self_a, self_b, x, grad_mid, vec, block):
    rows, width = x.shape
    tile = spec((block, width), lambda i: (i, 0))
    weight = lambda which: spec((1, width, width), lambda i: (which, 0, 0), once=True)
    return run(
        in_back_body,
        "in_back",
        (rows // block,),
        (grad_q, grad_k, grad_v, self_a, self_a, self_b, x, grad_mid, vec),
        [tile, tile, tile, weight(0), weight(1), weight(0), tile, tile, whole(vec.shape)],
        [((rows, width), LOW, tile), ((8, width), WIDE, spec((8, width), lambda i: (0, 0)))],
        flops=6 * rows * width * width,
    )


def axis_bits(count):
    bits = count.bit_length() - 1
    assert 1 << bits == count
    each = (bits - 1) // 3
    x_bits = list(range(1, 1 + each))
    y_bits = list(range(1 + each, 1 + 2 * each))
    z_bits = list(range(1 + 2 * each, bits))
    return x_bits, y_bits, z_bits


def gather_stages(count, parts):
    x_bits, y_bits, z_bits = (list(reversed(b)) for b in axis_bits(count))
    if parts == 1:
        return [[(b,) for b in bits] for bits in (x_bits, y_bits, z_bits[:1], z_bits[1:], [0])]
    return [
        [(z_bits[0],)],
        [(b,) for b in z_bits[1:]],
        list(zip(y_bits, x_bits)),
        list(zip(x_bits, y_bits)),
        [(0, 0)],
    ]


def scatter_stages(count, parts):
    return [list(reversed(stage)) for stage in reversed(gather_stages(count, parts))]


def swap(values, bit, count):
    return lax.ppermute(values, "fsdp", [(i, i ^ (1 << bit)) for i in range(count)])


def own_bit(bit):
    return (lax.axis_index("fsdp") >> bit) & 1


def weave_body(parts, core_ref, *refs):
    for part in range(parts):
        out = refs[2 * parts + part]
        out[0, :, core_ref[0]] = refs[part][:, 0]
        out[0, :, 1 - core_ref[0]] = refs[parts + part][:, 0]


def weave(held, other, core):
    groups, mats, rows, width = held[0].shape
    parts = len(held)
    half = spec((groups, 1, rows, width), lambda i: (0, i, 0, 0))
    both = spec((1, groups, 2, rows, width), lambda i: (i, 0, 0, 0, 0))
    return run(
        functools.partial(weave_body, parts),
        "weave",
        (mats,),
        (core, *held, *other),
        [smem()] + [half] * (2 * parts),
        [((mats, groups, 2, rows, width), held[0].dtype, both)] * parts,
    )


class Gather:
    def __init__(self, piece, count, parts=2):
        self.count = count
        self.bits = count.bit_length() - 1
        mats, rows, width = piece.shape
        self.shape = (rows, width)
        self.parts = [piece.reshape((1,) * self.bits + (mats, rows, width))]
        self.stages = gather_stages(count, parts)
        self.flight = None

    def land(self):
        if self.flight is not None:
            parts = []
            for held, (bit, other) in zip(self.parts, self.flight):
                axis = self.bits - 1 - bit
                parts.append(
                    jnp.where(
                        own_bit(bit) == 0,
                        jnp.concatenate([held, other], axis),
                        jnp.concatenate([other, held], axis),
                    )
                )
            self.parts = parts
            self.flight = None

    def ready(self):
        self.land()
        if len(self.stages[0][0]) == 2 and len(self.parts) == 1:
            self.parts = jnp.split(self.parts[0], 2, self.bits)
        return self.parts

    def launch(self, parts):
        self.parts = parts
        for place, step in enumerate(self.stages.pop(0)):
            if place:
                self.land()
            self.flight = [(bit, swap(part, bit, self.count)) for bit, part in zip(step, self.parts)]

    def result(self):
        rows, width = self.shape
        merged = lambda v: v.reshape((self.count // 2,) + v.shape[self.bits :])
        held = [merged(v) for v in self.parts]
        other = [merged(v) for _, v in self.flight]
        if len(held) == 1:
            self.land()
            return [self.parts[0].reshape(self.count * rows, width)]
        done = weave(held, other, own_bit(0).astype(jnp.int32).reshape(1))
        return [v.reshape(v.shape[0], self.count * rows, width) for v in done]


class Scatter:
    def __init__(self, parts, count):
        self.count = count
        self.bits = count.bit_length() - 1
        self.kind = parts[0][0].dtype
        self.stages = scatter_stages(count, len(parts))
        self.sends, self.pairs = [], []
        for part in parts:
            if len(part) == 1:
                mats, rows, width = part[0].shape
                groups = part[0].reshape(mats, count // 2, 2, rows // count, width)
                part = [
                    jnp.swapaxes(lax.dynamic_index_in_dim(groups, side, 2, False), 0, 1)
                    for side in (1 - own_bit(0), own_bit(0))
                ]
            self.shape = part[0].shape[2:]
            shaped = [v.reshape((2,) * (self.bits - 1) + (1,) + v.shape[1:]) for v in part]
            self.sends.append(shaped[0])
            self.pairs.append((shaped[1], None))

    def pick(self, pair, bit, side):
        axis = self.bits - 1 - bit
        values = [lax.dynamic_slice_in_dim(v, side, 1, axis) for v in pair]
        return self.total(values, self.kind)

    def total(self, pair, kind):
        return (pair[0].astype(WIDE) + pair[1].astype(WIDE)).astype(kind)

    def ready(self):
        if self.sends is not None:
            return self.sends
        step = self.stages[0][0]
        if len(step) == 1 and len(self.pairs) == 2:
            self.pairs = [
                tuple(jnp.concatenate([p[i] for p in self.pairs], self.bits) for i in (0, 1))
            ]
        return [self.pick(pair, bit, 1 - own_bit(bit)) for bit, pair in zip(step, self.pairs)]

    def launch(self, sends):
        for place, step in enumerate(self.stages.pop(0)):
            if place:
                sends = [self.pick(p, b, 1 - own_bit(b)) for b, p in zip(step, self.pairs)]
            flight = [swap(v, bit, self.count) for bit, v in zip(step, sends)]
            if self.sends is None:
                kept = [self.pick(p, bit, own_bit(bit)) for bit, p in zip(step, self.pairs)]
            else:
                kept, self.sends = [p[0] for p in self.pairs], None
            self.pairs = list(zip(kept, flight))

    def result(self):
        total = jnp.concatenate([self.total(p, WIDE) for p in self.pairs], self.bits)
        return total.reshape((-1,) + self.shape)


def tick(chains, values=()):
    ready = [chain.ready() for chain in chains]
    ready, values = lax.optimization_barrier((ready, values))
    for chain, parts in zip(chains, ready):
        chain.launch(parts)
    return values


def shards(
    count,
    hidden_in,
    encoder_states,
    lengths,
    out_grad,
    attn_in,
    attn_out,
    fc_in,
    fc_out,
    gains,
    biases,
    ffn_bias,
):
    batch, length, width = hidden_in.shape
    rows = batch * length
    block = length // 2
    frame_rows = encoder_states.shape[1]
    share = gains.shape[1]
    ff_share = ffn_bias.shape[0]
    mats = ff_share // share

    small = jnp.concatenate([gains.reshape(-1), biases.reshape(-1), ffn_bias])
    small_count = small.shape[0]
    small_rows = -(-(small_count + 5) // 128)
    small_size = small_rows * 128
    small = jnp.pad(small, (0, small_size - small_count)).reshape(1, small_rows, 128)
    fc_in_mats = fc_in.reshape(share, count, mats, share).transpose(2, 0, 1, 3).reshape(mats, share, width)
    fc_out_mats = fc_out.reshape(mats, share, width)
    g_small = Gather(small, count, 1)
    g_self = Gather(jnp.concatenate([attn_in[0:3], attn_out[0:1]]), count)
    g_cross = Gather(jnp.concatenate([attn_in[3:4], attn_out[1:2], attn_in[4:6]]), count)
    g_ffn = Gather(jnp.concatenate([fc_in_mats, fc_out_mats]), count)

    core = own_bit(0).astype(jnp.int32).reshape(1)
    x = hidden_in.reshape(rows, width)
    frames = encoder_states.reshape(-1, width)
    valid = jnp.arange(length)[None, :, None] < lengths[:, None, None]
    grad = jnp.where(valid, out_grad, jnp.zeros_like(out_grad)).reshape(rows, width)

    tick([g_self, g_small])
    tick([g_self, g_small])
    tick([g_self, g_small, g_cross])
    tick([g_self, g_small, g_cross, g_ffn])
    tick([g_self, g_small, g_cross, g_ffn])
    small = g_small.result()[0].astype(jnp.float32).reshape(count, small_size)
    vec = small[:, : 13 * share].reshape(count, 13, share).transpose(1, 0, 2).reshape(13, width)
    vec = jnp.pad(vec, ((0, 3), (0, 0)))
    bias = small[:, 13 * share : small_count].reshape(count, mats, share)
    bias = bias.transpose(1, 0, 2).reshape(mats, 1, width)
    self_a, self_b = g_self.result()
    x = tick([g_cross], x)
    norm_one, query, key, value = qkv(x, vec, self_a, self_b, block)
    query, key, value = tick([g_ffn], (query, key, value))
    attended = attend(query, key, value, batch, True)
    mid, norm_two, square_self = mid_stage(lengths, attended, x, vec, self_b, batch, block)
    norm_two = tick([g_cross], norm_two)
    norm_two = tick([g_ffn], norm_two)
    cross_a, cross_b = g_cross.result()
    cross_q, cross_k, cross_v = cross_stage(norm_two, frames, vec, cross_a, cross_b, batch)
    cross_attended = attend(cross_q, cross_k, cross_v, batch, False)
    late, norm_three, square_cross = late_stage(lengths, cross_attended, mid, vec, cross_a, batch, block)
    norm_three = tick([g_ffn], norm_three)
    w_in, w_out = g_ffn.result()
    grad_norm, d_in, d_out, sums_ff, result, square_rest = ffn_stage(
        lengths, core, count, norm_three, grad, bias, w_in, w_out, None, late, vec, batch, block
    )
    s_ffn = Scatter([d_in, d_out], count)
    grad_norm = tick([s_ffn], grad_norm)
    grad_late, grad_cross, grad_cross_att, sums_late = late_back(
        grad_norm, late, grad, vec, cross_a, block
    )
    grad_cross_att = tick([s_ffn], grad_cross_att)
    grad_cq, grad_ck, grad_cv = attend_back(
        cross_q, cross_k, cross_v, grad_cross_att, batch, False
    )
    d_cross_a = weight_grads([(norm_two, grad_cq), (cross_attended, grad_cross)], core, count)
    d_cross_b = weight_grads([(frames, grad_ck), (frames, grad_cv)], core, count)
    s_cross = Scatter([d_cross_a, d_cross_b], count)
    grad_cq, grad_ck, grad_cv = tick([s_cross], (grad_cq, grad_ck, grad_cv))
    grad_mid, grad_self, grad_att, sums_mid = mid_back(
        grad_cq, cross_a, mid, grad_late, vec, self_b, block
    )
    grad_frames, sums_frames = frames_back(grad_ck, grad_cv, cross_b, frame_rows)
    grad_att, grad_frames = tick([s_cross, s_ffn], (grad_att, grad_frames))
    grad_q, grad_k, grad_v = attend_back(query, key, value, grad_att, batch, True)
    d_self_a = weight_grads([(norm_one, grad_q), (norm_one, grad_k)], core, count)
    d_self_b = weight_grads([(norm_one, grad_v), (attended, grad_self)], core, count)
    s_self = Scatter([d_self_a, d_self_b], count)
    grad_q, grad_k, grad_v = tick([s_self], (grad_q, grad_k, grad_v))
    grad_q, grad_k, grad_v = tick([s_cross, s_ffn], (grad_q, grad_k, grad_v))
    grad_q, grad_k, grad_v = tick([s_self], (grad_q, grad_k, grad_v))
    grad_in, sums_one = in_back(grad_q, grad_k, grad_v, self_a, self_b, x, grad_mid, vec, block)

    sums_one = tick([s_self, s_cross, s_ffn], sums_one)
    sum_rows = jnp.stack(
        [sums_one[0], sums_mid[0], sums_late[0]]
        + [sums_one[2], sums_one[3], sums_mid[2], sums_mid[3], sums_frames[0], sums_late[2], square_rest[2]]
        + [sums_one[1], sums_mid[1], sums_late[1]]
    )
    squares = jnp.stack([square_rest[0], square_self[0], square_cross[0], square_rest[1]])
    stats = jnp.concatenate([jnp.sum(squares, -1), jnp.sum(lengths).astype(WIDE)[None]])
    sums_ff = sums_ff.reshape(mats, count, share)
    sums = jnp.concatenate(
        [
            sum_rows.reshape(13, count, share).transpose(1, 0, 2).reshape(count, 13 * share),
            sums_ff.transpose(1, 0, 2).reshape(count, ff_share),
            jnp.broadcast_to(stats[None], (count, 5)),
        ],
        1,
    )
    sums = jnp.pad(sums, ((0, 0), (0, small_size - sums.shape[1])))
    s_small = Scatter([[sums.reshape(1, count * small_rows, 128)]], count)
    tick([s_small])
    tick([s_small])
    tick([s_small])
    tick([s_self, s_cross, s_small])
    tick([s_self, s_small])
    d_ffn = s_ffn.result()
    d_in_all, d_out_all = d_ffn[:mats], d_ffn[mats:]
    d_cross = s_cross.result()
    d_self = s_self.result()
    small = s_small.result().reshape(-1)
    stats = small[small_count : small_count + 5]
    rms = jnp.sqrt(stats[:4] / (stats[4] * width))
    return (
        result.reshape(hidden_in.shape),
        grad_in.reshape(hidden_in.shape),
        grad_frames.reshape(encoder_states.shape),
        jnp.concatenate([d_self[:3], d_cross[:1], d_cross[2:]]),
        jnp.concatenate([d_self[3:], d_cross[1:2]]),
        d_in_all.reshape(mats, share, count, share).transpose(1, 2, 0, 3).reshape(share, -1),
        d_out_all.reshape(ff_share, width),
        small[: 3 * share].reshape(3, share),
        small[3 * share : 13 * share].reshape(10, share),
        small[13 * share : small_count],
        rms,
    )


def solution(mesh):
    placed = (
        P("fsdp", None, None),
        P("fsdp", None, None),
        P("fsdp"),
        P("fsdp", None, None),
        P(None, "fsdp", None),
        P(None, "fsdp", None),
        P("fsdp", None),
        P("fsdp", None),
        P(None, "fsdp"),
        P(None, "fsdp"),
        P("fsdp"),
    )
    return jax.shard_map(
        functools.partial(shards, mesh.shape["fsdp"]),
        mesh=mesh,
        in_specs=placed,
        out_specs=(
            P("fsdp", None, None),
            P("fsdp", None, None),
            P("fsdp", None, None),
            P(None, "fsdp", None),
            P(None, "fsdp", None),
            P("fsdp", None),
            P("fsdp", None),
            P(None, "fsdp"),
            P(None, "fsdp"),
            P("fsdp"),
            P(),
        ),
        check_vma=False,
    )
```

```python
import functools
import math

import jax
import jax.numpy as jnp
from jax import lax
from jax.experimental import pallas as pl
from jax.experimental.pallas import tpu as pltpu
from jax.sharding import PartitionSpec as P

NORM_EPS = 1e-05
LOW = jnp.bfloat16
WIDE = jnp.float32
HEADS = 12
PAIR = 128
HALF_PAIR = 64
SCALE = 0.125


def dot_nn(left, right):
    return lax.dot_general(left, right, (((1,), (0,)), ((), ())), preferred_element_type=WIDE)


def dot_nt(left, right):
    return lax.dot_general(left, right, (((1,), (1,)), ((), ())), preferred_element_type=WIDE)


def dot_tn(left, right):
    return lax.dot_general(left, right, (((0,), (0,)), ((), ())), preferred_element_type=WIDE)


def spec(block, index, once=False):
    if once:
        return pl.BlockSpec(block, index, pipeline_mode=pl.Buffered(1))
    return pl.BlockSpec(block, index)


def run(body, name, grid, operands, in_specs, outs, scratch=(), flops=0, exps=0, limit=14, far=()):
    moved = sum(o.size * o.dtype.itemsize for o in operands)
    moved += sum(math.prod(s) * jnp.dtype(d).itemsize for s, d, _ in outs)
    return pl.pallas_call(
        body,
        name=name,
        grid=grid,
        in_specs=in_specs,
        out_specs=[o[2] for o in outs],
        out_shape=[
            pltpu.HBM(o[0], o[1]) if i in far else jax.ShapeDtypeStruct(o[0], o[1])
            for i, o in enumerate(outs)
        ],
        scratch_shapes=list(scratch),
        compiler_params=pltpu.CompilerParams(
            dimension_semantics=("arbitrary",) * len(grid), vmem_limit_bytes=limit << 20
        ),
        cost_estimate=pl.CostEstimate(flops=flops, transcendentals=exps, bytes_accessed=moved),
    )(*operands)


def in_hbm(values):
    return pltpu.with_memory_space_constraint(values, pltpu.HBM)


def normalised(values):
    center = values - jnp.mean(values, -1, keepdims=True)
    spread = jnp.mean(center * center, -1, keepdims=True)
    scale = lax.rsqrt(spread + NORM_EPS)
    return center * scale, scale


def norm_backward(values, grad, gain):
    unit, scale = normalised(values)
    inner = grad * gain
    mean_inner = jnp.mean(inner, -1, keepdims=True)
    mean_unit = jnp.mean(inner * unit, -1, keepdims=True)
    return scale * (inner - mean_inner - unit * mean_unit), grad * unit


def col_sum(values):
    return jnp.sum(values.astype(WIDE), 0, keepdims=True)


def add_rows(ref, first, rows):
    @pl.when(first)
    def _():
        ref[...] = jnp.zeros_like(ref)

    for place, row in enumerate(rows):
        ref[place : place + 1, :] += row


def masked_squares(values, length_ref, step, per_seq):
    rows = values.shape[0]
    start = (step % per_seq) * rows
    index = start + lax.broadcasted_iota(jnp.int32, (rows, 1), 0)
    inside = index < length_ref[step // per_seq]
    return col_sum(jnp.where(inside, values * values, 0.0))


def qkv_body(x_ref, vec_ref, wq, wk, wv, n_ref, q_ref, k_ref, v_ref):
    unit, _ = normalised(x_ref[...].astype(WIDE))
    norm = (unit * vec_ref[0:1, :] + vec_ref[10:11, :]).astype(LOW)
    n_ref[...] = norm
    query = (dot_nn(norm, wq[0]) + vec_ref[3:4, :]).astype(LOW)
    q_ref[...] = query * jnp.asarray(SCALE, LOW)
    k_ref[...] = dot_nn(norm, wk[0]).astype(LOW)
    v_ref[...] = (dot_nn(norm, wv[0]) + vec_ref[4:5, :]).astype(LOW)


def whole(shape):
    return spec(shape, lambda *_: (0,) * len(shape), once=True)


def qkv(x, vec, self_a, self_b, block):
    rows, width = x.shape
    row = lambda i: (i, 0)
    weight = lambda which: spec((1, width, width), lambda i: (which, 0, 0), once=True)
    return run(
        qkv_body,
        "qkv",
        (rows // block,),
        (x, vec, self_a, self_a, self_b),
        [spec((block, width), row), whole(vec.shape), weight(0), weight(1), weight(0)],
        [((rows, width), LOW, spec((block, width), row))] * 4,
        flops=6 * rows * width * width,
    )


def head_lanes(values, head):
    lane = lax.broadcasted_iota(jnp.int32, (1, PAIR), 1)
    inside = lane < HALF_PAIR if head == 0 else lane >= HALF_PAIR
    return jnp.where(inside, values, jnp.zeros_like(values))


def attend_cross_body(pairs, q_ref, k_ref, v_ref, o_ref):
    for pair in range(pairs):
        lanes = slice(pair * PAIR, (pair + 1) * PAIR)
        values, keys, queries = v_ref[:, lanes], k_ref[:, lanes], q_ref[:, lanes]
        total = None
        for head in (0, 1):
            scores = dot_nt(head_lanes(queries, head), keys)
            exps = jnp.exp(scores - jnp.max(scores, -1, keepdims=True))
            probs = exps * (1.0 / jnp.sum(exps, -1, keepdims=True))
            part = dot_nn(probs.astype(LOW), head_lanes(values, head))
            total = part if total is None else total + part
        o_ref[:, lanes] = total.astype(LOW)


def attend_body(pairs, step_rows, q_ref, k_ref, v_ref, o_ref):
    length = q_ref.shape[0]
    starts = list(range(0, length, step_rows))
    for pair in range(pairs):
        lanes = slice(pair * PAIR, (pair + 1) * PAIR)
        turned = v_ref[:, lanes].T
        keys = [head_lanes(k_ref[:, lanes], head) for head in (0, 1)]
        work = []
        for start in starts:
            stop = min(start + step_rows, length)
            queries = q_ref[start:stop, lanes]
            cuts = ([(0, start)] if start else []) + [(start, stop)]
            for head in (0, 1):
                parts = []
                for low, high in cuts:
                    scores = dot_nt(keys[head][low:high], queries)
                    if low == start:
                        key_at = lax.broadcasted_iota(jnp.int32, scores.shape, 0)
                        query_at = lax.broadcasted_iota(jnp.int32, scores.shape, 1)
                        scores = jnp.where(key_at <= query_at, scores, -1e30)
                    parts.append(scores)
                work.append((start, stop, head, cuts, parts))
        tops = []
        for start, stop, head, cuts, parts in work:
            top = jnp.max(parts[0], 0, keepdims=True)
            for scores in parts[1:]:
                top = jnp.maximum(top, jnp.max(scores, 0, keepdims=True))
            tops.append(top)
        exps = [[jnp.exp(s - top) for s in item[4]] for item, top in zip(work, tops)]
        totals = [sum(jnp.sum(e, 0, keepdims=True) for e in group) for group in exps]
        outs = []
        for (start, stop, head, cuts, _), group, total in zip(work, exps, totals):
            out = None
            for (low, high), e in zip(cuts, group):
                part = dot_nn(turned[head * HALF_PAIR : (head + 1) * HALF_PAIR, low:high], e.astype(LOW))
                out = part if out is None else out + part
            outs.append(out * (1.0 / total))
        for place, start in enumerate(starts):
            stop = min(start + step_rows, length)
            both = jnp.concatenate(outs[2 * place : 2 * place + 2], 0)
            o_ref[start:stop, lanes] = both.T.astype(LOW)


def attend(q, k, v, batch, causal, pairs=6, step_rows=128):
    rows, width = q.shape
    length, frames = rows // batch, k.shape[0] // batch
    lanes = pairs * PAIR
    at = lambda b, p: (b, p)
    return run(
        functools.partial(attend_body, pairs, step_rows) if causal else functools.partial(attend_cross_body, pairs),
        "attend_self" if causal else "attend_cross",
        (batch, width // lanes),
        (q, k, v),
        [spec((length, lanes), at), spec((frames, lanes), at), spec((frames, lanes), at)],
        [((rows, width), LOW, spec((length, lanes), at))],
        flops=4 * rows * frames * width,
        exps=rows * frames * HEADS,
    )[0]


def attend_back_body(causal, pairs, step_rows, q_ref, k_ref, v_ref, g_ref, gq_ref, gk_ref, gv_ref, dk, dv):
    length = q_ref.shape[0]
    frames = k_ref.shape[0]
    starts = list(range(0, length, step_rows))
    for pair in range(pairs):
        lanes = slice(pair * PAIR, (pair + 1) * PAIR)
        keys = [head_lanes(k_ref[:, lanes], head) for head in (0, 1)]
        values = [head_lanes(v_ref[:, lanes], head) for head in (0, 1)]
        work = []
        for start in starts:
            stop = min(start + step_rows, length)
            cuts = ([(0, start)] if start else []) + [(start, stop)] if causal else [(0, frames)]
            for head in (0, 1):
                queries, grads = q_ref[start:stop, lanes], g_ref[start:stop, lanes]
                parts = []
                for low, high in cuts:
                    scores = dot_nt(keys[head][low:high], queries)
                    if causal and low == start:
                        key_at = lax.broadcasted_iota(jnp.int32, scores.shape, 0)
                        query_at = lax.broadcasted_iota(jnp.int32, scores.shape, 1)
                        scores = jnp.where(key_at <= query_at, scores, -1e30)
                    parts.append(scores)
                grad_parts = [dot_nt(values[head][low:high], grads) for low, high in cuts]
                work.append((start, stop, head, cuts, parts, grad_parts))
        probs = []
        for item in work:
            parts = item[4]
            top = jnp.max(parts[0], 0, keepdims=True)
            for scores in parts[1:]:
                top = jnp.maximum(top, jnp.max(scores, 0, keepdims=True))
            exps = [jnp.exp(scores - top) for scores in parts]
            total = 1.0 / sum(jnp.sum(e, 0, keepdims=True) for e in exps)
            probs.append([e * total for e in exps])
        scores = []
        for item, group in zip(work, probs):
            weighted = [p * g for p, g in zip(group, item[5])]
            inner = sum(jnp.sum(w, 0, keepdims=True) for w in weighted)
            scores.append([(w - p * inner).astype(LOW) for w, p in zip(weighted, group)])
        grad_q = {}
        for (start, stop, head, cuts, _, _), group, low_scores in zip(work, probs, scores):
            queries = head_lanes(q_ref[start:stop, lanes], head)
            grads = head_lanes(g_ref[start:stop, lanes], head)
            for (low, high), p, s in zip(cuts, group, low_scores):
                part_v = dot_nn(p.astype(LOW), grads)
                part_k = dot_nn(s, queries)
                part_q = dot_tn(s, keys[head][low:high])
                grad_q[start] = part_q if start not in grad_q else grad_q[start] + part_q
                if head == 0 and (low == start or not causal and start == 0):
                    dv[low:high, :] = part_v
                    dk[low:high, :] = part_k
                else:
                    dv[low:high, :] += part_v
                    dk[low:high, :] += part_k
        for start, total in grad_q.items():
            gq_ref[start : start + total.shape[0], lanes] = (total * SCALE).astype(LOW)
        gk_ref[:, lanes] = dk[...].astype(LOW)
        gv_ref[:, lanes] = dv[...].astype(LOW)


def attend_back(q, k, v, grad, batch, causal, pairs=6):
    rows, width = q.shape
    length, frames = rows // batch, k.shape[0] // batch
    lanes = pairs * PAIR
    at = lambda b, p: (b, p)
    long, short = spec((length, lanes), at), spec((frames, lanes), at)
    return run(
        functools.partial(attend_back_body, causal, pairs, 128 if causal else length),
        "attend_self_back" if causal else "attend_cross_back",
        (batch, width // lanes),
        (q, k, v, grad),
        [long, short, short, long],
        [((rows, width), LOW, long), (k.shape, LOW, short), (k.shape, LOW, short)],
        [pltpu.VMEM((frames, PAIR), WIDE)] * 2,
        flops=10 * rows * frames * width,
        exps=rows * frames * HEADS,
    )


def mid_body(per_seq, len_ref, a_ref, x_ref, vec_ref, wo, mid_ref, n_ref, s_ref):
    step = pl.program_id(0)
    branch = dot_nn(a_ref[...], wo[0]) + vec_ref[5:6, :]
    mid = x_ref[...].astype(WIDE) + branch
    mid_ref[...] = mid
    unit, _ = normalised(mid)
    n_ref[...] = (unit * vec_ref[1:2, :] + vec_ref[11:12, :]).astype(LOW)
    add_rows(s_ref, step == 0, [masked_squares(branch, len_ref, step, per_seq)])


def smem():
    return pl.BlockSpec(memory_space=pltpu.SMEM)


def mid_stage(lengths, attended, x, vec, self_b, batch, block):
    rows, width = x.shape
    weight = spec((1, width, width), lambda i: (1, 0, 0), once=True)
    tile = spec((block, width), lambda i: (i, 0))
    return run(
        functools.partial(mid_body, rows // batch // block),
        "mid_stage",
        (rows // block,),
        (lengths, attended, x, vec, self_b),
        [smem(), tile, tile, whole(vec.shape), weight],
        [
            ((rows, width), WIDE, tile),
            ((rows, width), LOW, tile),
            ((8, width), WIDE, spec((8, width), lambda i: (0, 0))),
        ],
        flops=2 * rows * width * width,
    )


def cross_body(n_ref, f_ref, vec_ref, wq, wk, wv, q_ref, k_ref, v_ref):
    query = (dot_nn(n_ref[...], wq[0]) + vec_ref[6:7, :]).astype(LOW)
    q_ref[...] = query * jnp.asarray(SCALE, LOW)
    frames = f_ref[...]
    k_ref[...] = dot_nn(frames, wk[0]).astype(LOW)
    v_ref[...] = (dot_nn(frames, wv[0]) + vec_ref[7:8, :]).astype(LOW)


def cross_stage(norm, frames, vec, cross_a, cross_b, batch):
    width = norm.shape[1]
    rows, frame_rows = norm.shape[0], frames.shape[0]
    long = spec((rows // batch, width), lambda i: (i, 0))
    short = spec((frame_rows // batch, width), lambda i: (i, 0))
    weight = lambda which: spec((1, width, width), lambda i: (which, 0, 0), once=True)
    return run(
        cross_body,
        "cross_stage",
        (batch,),
        (norm, frames, vec, cross_a, cross_b, cross_b),
        [long, short, whole(vec.shape), weight(0), weight(0), weight(1)],
        [((rows, width), LOW, long), ((frame_rows, width), LOW, short), ((frame_rows, width), LOW, short)],
        flops=(2 * rows + 4 * frame_rows) * width * width,
    )


def late_body(per_seq, len_ref, a_ref, mid_ref, vec_ref, wo, late_ref, n_ref, s_ref):
    step = pl.program_id(0)
    branch = dot_nn(a_ref[...], wo[0]) + vec_ref[8:9, :]
    late = mid_ref[...] + branch
    late_ref[...] = late
    unit, _ = normalised(late)
    n_ref[...] = (unit * vec_ref[2:3, :] + vec_ref[12:13, :]).astype(LOW)
    add_rows(s_ref, step == 0, [masked_squares(branch, len_ref, step, per_seq)])


def late_stage(lengths, attended, mid, vec, cross_a, batch, block):
    rows, width = mid.shape
    tile = spec((block, width), lambda i: (i, 0))
    return run(
        functools.partial(late_body, rows // batch // block),
        "late_stage",
        (rows // block,),
        (lengths, attended, mid, vec, cross_a),
        [smem(), tile, tile, whole(vec.shape), spec((1, width, width), lambda i: (1, 0, 0), once=True)],
        [
            ((rows, width), WIDE, tile),
            ((rows, width), LOW, tile),
            ((8, width), WIDE, spec((8, width), lambda i: (0, 0))),
        ],
        flops=2 * rows * width * width,
        far=(0,),
    )


def ffn_body(first, last, batch, block, split, len_ref, core_ref, n_ref, g_ref, b_ref, wi_ref, wo_ref, *refs):
    refs = list(refs)
    before = [] if first else [refs.pop(0), refs.pop(0)]
    late_ref, vec_ref = (refs.pop(0), refs.pop(0)) if last else (None, None)
    gn_ref = refs.pop(0)
    di_refs = [refs.pop(0) for _ in range(split)]
    do_refs = [refs.pop(0) for _ in range(split)]
    sf_ref, f_ref = refs[:2]
    rest = refs[2:]
    s_ref = rest.pop(0) if last else None
    hidden_ref, pre_ref = rest[:2]
    acc_ref = rest[2] if last else f_ref
    step = pl.program_id(0)
    rows = n_ref.shape[0]

    @pl.when(step == 0)
    def _():
        if first:
            acc_ref[...] = jnp.zeros_like(acc_ref)
            gn_ref[...] = jnp.zeros_like(gn_ref)
        else:
            acc_ref[...] = before[0][...]
            gn_ref[...] = before[1][...]

    def chunk(place, carry):
        at = pl.ds(pl.multiple_of(place * block, block), block)
        pre = dot_nn(n_ref[at, :], wi_ref[0]) + b_ref[0]
        below = 0.5 + 0.5 * lax.erf(pre * (0.5**0.5))
        density = jnp.exp(-0.5 * pre * pre) * (1.0 / math.sqrt(2.0 * math.pi))
        hidden = (pre * below).astype(LOW)
        hidden_ref[at, :] = hidden
        acc_ref[at, :] += dot_nn(hidden, wo_ref[0])
        grad = dot_nt(g_ref[at, :], wo_ref[0])
        grad = (grad * (below + pre * density)).astype(LOW)
        pre_ref[at, :] = grad
        gn_ref[at, :] += dot_nt(grad, wi_ref[0])
        return carry

    lax.fori_loop(0, rows // block, chunk, 0)
    sf_ref[0] = col_sum(pre_ref[...])
    store_grad(dot_tn(n_ref[...], pre_ref[...]), di_refs, 0, core_ref)
    store_grad(dot_tn(hidden_ref[...], g_ref[...]), do_refs, 0, core_ref)
    if last:
        @pl.when(step == pl.num_programs(0) - 1)
        def _():
            s_ref[...] = jnp.zeros_like(s_ref)

            def finish(place, carry):
                at = pl.ds(pl.multiple_of(place * block, block), block)
                branch = acc_ref[at, :] + vec_ref[9:10, :]
                result = late_ref[at, :] + branch
                f_ref[at, :] = result.astype(LOW)
                per_seq = rows // batch // block
                s_ref[0:1, :] += masked_squares(result, len_ref, place, per_seq)
                s_ref[1:2, :] += masked_squares(branch, len_ref, place, per_seq)
                s_ref[2:3, :] += col_sum(g_ref[at, :])
                return carry

            lax.fori_loop(0, rows // block, finish, 0)


def ffn_stage(lengths, core, count, norm, grad, bias, w_in, w_out, before, late, vec, batch, block):
    rows, width = norm.shape
    mats = w_in.shape[0]
    first, last = before is None, late is not None
    mat = spec((1, width, width), lambda j: (j, 0, 0))
    line = spec((1, 1, width), lambda j: (j, 0, 0))
    operands = [lengths, core, norm, grad, bias, w_in, w_out]
    specs = [smem(), smem(), whole(norm.shape), whole(grad.shape), line, mat, mat]
    if not first:
        operands += list(before)
        specs += [whole((rows, width))] * 2
    if last:
        operands += [late, vec]
        specs += [whole((rows, width)), whole(vec.shape)]
    fixed = whole((rows, width))
    grads = grad_outs(mats, width, count, (1, width), lambda j: (j, 0))
    outs = [
        ((rows, width), WIDE, fixed),
        *grads,
        *grads,
        ((mats, 1, width), WIDE, line),
        ((rows, width), LOW if last else WIDE, fixed),
    ]
    scratch = [pltpu.VMEM((rows, width), LOW)] * 2
    if last:
        outs.append(((8, width), WIDE, whole((8, width))))
        scratch.append(pltpu.VMEM((rows, width), WIDE))
    done = run(
        functools.partial(ffn_body, first, last, batch, block, len(grads)),
        "ffn_stage",
        (mats,),
        tuple(operands),
        specs,
        outs,
        scratch,
        flops=12 * rows * width * width * mats,
        exps=2 * rows * width * mats,
        limit=30,
        far=(0, 2, 4),
    )
    split = len(grads)
    return done[0], done[1 : 1 + split], done[1 + split : 1 + 2 * split], *done[1 + 2 * split :]


def late_back_body(gn_ref, late_ref, og_ref, vec_ref, wo, gl_ref, gc_ref, ga_ref, s_ref):
    grad = gn_ref[...]
    through, for_gain = norm_backward(late_ref[...], grad, vec_ref[2:3, :])
    total = og_ref[...].astype(WIDE) + through
    gl_ref[...] = total
    low = total.astype(LOW)
    gc_ref[...] = low
    ga_ref[...] = dot_nt(low, wo[0]).astype(LOW)
    add_rows(s_ref, pl.program_id(0) == 0, [col_sum(for_gain), col_sum(grad), col_sum(low)])


def late_back(grad_norm, late, grad, vec, cross_a, block):
    rows, width = late.shape
    tile = spec((block, width), lambda i: (i, 0))
    return run(
        late_back_body,
        "late_back",
        (rows // block,),
        (in_hbm(grad_norm), in_hbm(late), grad, vec, cross_a),
        [
            tile,
            tile,
            tile,
            whole(vec.shape),
            spec((1, width, width), lambda i: (1, 0, 0), once=True),
        ],
        [
            ((rows, width), WIDE, tile),
            ((rows, width), LOW, tile),
            ((rows, width), LOW, tile),
            ((8, width), WIDE, spec((8, width), lambda i: (0, 0))),
        ],
        flops=2 * rows * width * width,
    )


def store_grad(grad, outs, place, core_ref):
    if len(outs) == 1:
        outs[0][place] = grad.astype(LOW)
        return
    groups, _, rows, width = outs[0].shape
    pairs = grad.reshape(groups, 2, rows, width)
    for core in (0, 1):

        @pl.when(core_ref[0] == core)
        def _(core=core):
            outs[0][:, place] = pairs[:, 1 - core].astype(LOW)
            outs[1][:, place] = pairs[:, core].astype(LOW)


def grad_outs(mats, width, count, block, index):
    rows = width // count
    if rows % 8 or block[1] % (2 * rows):
        whole_out = spec(block + (width,), lambda i: index(i) + (0,))
        return [((mats, width, width), LOW, whole_out)]
    groups = block[1] // (2 * rows)
    half = spec((groups, block[0], rows, width), lambda i: index(i)[::-1] + (0, 0))
    return [((count // 2, mats, rows, width), LOW, half)] * 2


def weights_body(count, core_ref, *refs):
    outs = refs[2 * count :]
    for place in range(count):
        grad = dot_tn(refs[2 * place][...], refs[2 * place + 1][...])
        store_grad(grad, outs, place, core_ref)


def weight_grads(pairs, core, count):
    width = pairs[0][0].shape[1]
    block = width // 2
    operands, specs = [core], [smem()]
    for left, right in pairs:
        operands += [left, right]
        specs += [spec((left.shape[0], block), lambda j: (0, j)), whole(right.shape)]
    return run(
        functools.partial(weights_body, len(pairs)),
        "weight_grads",
        (width // block,),
        tuple(operands),
        specs,
        grad_outs(len(pairs), width, count, (len(pairs), block), lambda j: (0, j)),
        flops=sum(2 * left.shape[0] * width * width for left, _ in pairs),
    )


def mid_back_body(gq, wq, mid_ref, gl_ref, vec_ref, wo, gm_ref, gs_ref, ga_ref, s_ref):
    query = gq[...]
    grad = dot_nt(query, wq[0])
    through, for_gain = norm_backward(mid_ref[...], grad, vec_ref[1:2, :])
    total = gl_ref[...] + through
    gm_ref[...] = total
    low = total.astype(LOW)
    gs_ref[...] = low
    ga_ref[...] = dot_nt(low, wo[0]).astype(LOW)
    add_rows(
        s_ref,
        pl.program_id(0) == 0,
        [col_sum(for_gain), col_sum(grad), col_sum(low), col_sum(query)],
    )


def mid_back(grad_q, cross_a, mid, grad_late, vec, self_b, block):
    rows, width = mid.shape
    tile = spec((block, width), lambda i: (i, 0))
    weight = lambda which: spec((1, width, width), lambda i: (which, 0, 0), once=True)
    return run(
        mid_back_body,
        "mid_back",
        (rows // block,),
        (grad_q, cross_a, mid, grad_late, vec, self_b),
        [tile, weight(0), tile, tile, whole(vec.shape), weight(1)],
        [
            ((rows, width), WIDE, tile),
            ((rows, width), LOW, tile),
            ((rows, width), LOW, tile),
            ((8, width), WIDE, spec((8, width), lambda i: (0, 0))),
        ],
        flops=4 * rows * width * width,
    )


def frames_back_body(gk, gv, wk, wv, ge_ref, s_ref):
    grad_v = gv[...]
    ge_ref[...] = (dot_nt(gk[...], wk[0]) + dot_nt(grad_v, wv[0])).astype(LOW)
    add_rows(s_ref, pl.program_id(0) == 0, [col_sum(grad_v)])


def frames_back(grad_k, grad_v, cross_b, block):
    rows, width = grad_k.shape
    tile = spec((block, width), lambda i: (i, 0))
    weight = lambda which: spec((1, width, width), lambda i: (which, 0, 0), once=True)
    return run(
        frames_back_body,
        "frames_back",
        (rows // block,),
        (grad_k, grad_v, cross_b, cross_b),
        [tile, tile, weight(0), weight(1)],
        [((rows, width), LOW, tile), ((8, width), WIDE, spec((8, width), lambda i: (0, 0)))],
        flops=4 * rows * width * width,
    )


def in_back_body(gq, gk, gv, wq, wk, wv, x_ref, gm_ref, vec_ref, gi_ref, s_ref):
    query, value = gq[...], gv[...]
    grad = dot_nt(query, wq[0]) + dot_nt(gk[...], wk[0]) + dot_nt(value, wv[0])
    through, for_gain = norm_backward(x_ref[...].astype(WIDE), grad, vec_ref[0:1, :])
    gi_ref[...] = (gm_ref[...] + through).astype(LOW)
    add_rows(
        s_ref,
        pl.program_id(0) == 0,
        [col_sum(for_gain), col_sum(grad), col_sum(query), col_sum(value)],
    )


def in_back(grad_q, grad_k, grad_v, self_a, self_b, x, grad_mid, vec, block):
    rows, width = x.shape
    tile = spec((block, width), lambda i: (i, 0))
    weight = lambda which: spec((1, width, width), lambda i: (which, 0, 0), once=True)
    return run(
        in_back_body,
        "in_back",
        (rows // block,),
        (grad_q, grad_k, grad_v, self_a, self_a, self_b, x, grad_mid, vec),
        [tile, tile, tile, weight(0), weight(1), weight(0), tile, tile, whole(vec.shape)],
        [((rows, width), LOW, tile), ((8, width), WIDE, spec((8, width), lambda i: (0, 0)))],
        flops=6 * rows * width * width,
    )


def axis_bits(count):
    bits = count.bit_length() - 1
    assert 1 << bits == count
    each = (bits - 1) // 3
    x_bits = list(range(1, 1 + each))
    y_bits = list(range(1 + each, 1 + 2 * each))
    z_bits = list(range(1 + 2 * each, bits))
    return x_bits, y_bits, z_bits


def gather_stages(count, parts):
    x_bits, y_bits, z_bits = (list(reversed(b)) for b in axis_bits(count))
    if parts == 1:
        return [[(b,) for b in bits] for bits in (x_bits, y_bits, z_bits[:1], z_bits[1:], [0])]
    return [
        [(z_bits[0],)],
        [(b,) for b in z_bits[1:]],
        list(zip(y_bits, x_bits)),
        list(zip(x_bits, y_bits)),
        [(0, 0)],
    ]


def scatter_stages(count, parts):
    return [list(reversed(stage)) for stage in reversed(gather_stages(count, parts))]


def swap(values, bit, count):
    return lax.ppermute(values, "fsdp", [(i, i ^ (1 << bit)) for i in range(count)])


def own_bit(bit):
    return (lax.axis_index("fsdp") >> bit) & 1


def weave_body(parts, core_ref, *refs):
    for part in range(parts):
        out = refs[2 * parts + part]
        out[0, :, core_ref[0]] = refs[part][:, 0]
        out[0, :, 1 - core_ref[0]] = refs[parts + part][:, 0]


def weave(held, other, core):
    groups, mats, rows, width = held[0].shape
    parts = len(held)
    half = spec((groups, 1, rows, width), lambda i: (0, i, 0, 0))
    both = spec((1, groups, 2, rows, width), lambda i: (i, 0, 0, 0, 0))
    return run(
        functools.partial(weave_body, parts),
        "weave",
        (mats,),
        (core, *held, *other),
        [smem()] + [half] * (2 * parts),
        [((mats, groups, 2, rows, width), held[0].dtype, both)] * parts,
    )


class Gather:
    def __init__(self, piece, count, parts=2):
        self.count = count
        self.bits = count.bit_length() - 1
        mats, rows, width = piece.shape
        self.shape = (rows, width)
        self.parts = [piece.reshape((1,) * self.bits + (mats, rows, width))]
        self.stages = gather_stages(count, parts)
        self.flight = None

    def land(self):
        if self.flight is not None:
            parts = []
            for held, (bit, other) in zip(self.parts, self.flight):
                axis = self.bits - 1 - bit
                parts.append(
                    jnp.where(
                        own_bit(bit) == 0,
                        jnp.concatenate([held, other], axis),
                        jnp.concatenate([other, held], axis),
                    )
                )
            self.parts = parts
            self.flight = None

    def ready(self):
        self.land()
        if len(self.stages[0][0]) == 2 and len(self.parts) == 1:
            self.parts = jnp.split(self.parts[0], 2, self.bits)
        return self.parts

    def launch(self, parts):
        self.parts = parts
        for place, step in enumerate(self.stages.pop(0)):
            if place:
                self.land()
            self.flight = [(bit, swap(part, bit, self.count)) for bit, part in zip(step, self.parts)]

    def result(self):
        rows, width = self.shape
        merged = lambda v: v.reshape((self.count // 2,) + v.shape[self.bits :])
        held = [merged(v) for v in self.parts]
        other = [merged(v) for _, v in self.flight]
        if len(held) == 1:
            self.land()
            return [self.parts[0].reshape(self.count * rows, width)]
        done = weave(held, other, own_bit(0).astype(jnp.int32).reshape(1))
        return [v.reshape(v.shape[0], self.count * rows, width) for v in done]


class Scatter:
    def __init__(self, parts, count):
        self.count = count
        self.bits = count.bit_length() - 1
        self.kind = parts[0][0].dtype
        self.stages = scatter_stages(count, len(parts))
        self.sends, self.pairs = [], []
        for part in parts:
            if len(part) == 1:
                mats, rows, width = part[0].shape
                groups = part[0].reshape(mats, count // 2, 2, rows // count, width)
                part = [
                    jnp.swapaxes(lax.dynamic_index_in_dim(groups, side, 2, False), 0, 1)
                    for side in (1 - own_bit(0), own_bit(0))
                ]
            self.shape = part[0].shape[2:]
            shaped = [v.reshape((2,) * (self.bits - 1) + (1,) + v.shape[1:]) for v in part]
            self.sends.append(shaped[0])
            self.pairs.append((shaped[1], None))

    def pick(self, pair, bit, side):
        axis = self.bits - 1 - bit
        values = [lax.dynamic_slice_in_dim(v, side, 1, axis) for v in pair]
        return self.total(values, self.kind)

    def total(self, pair, kind):
        return (pair[0].astype(WIDE) + pair[1].astype(WIDE)).astype(kind)

    def ready(self):
        if self.sends is not None:
            return self.sends
        step = self.stages[0][0]
        if len(step) == 1 and len(self.pairs) == 2:
            self.pairs = [
                tuple(jnp.concatenate([p[i] for p in self.pairs], self.bits) for i in (0, 1))
            ]
        return [self.pick(pair, bit, 1 - own_bit(bit)) for bit, pair in zip(step, self.pairs)]

    def launch(self, sends):
        for place, step in enumerate(self.stages.pop(0)):
            if place:
                sends = [self.pick(p, b, 1 - own_bit(b)) for b, p in zip(step, self.pairs)]
            flight = [swap(v, bit, self.count) for bit, v in zip(step, sends)]
            if self.sends is None:
                kept = [self.pick(p, bit, own_bit(bit)) for bit, p in zip(step, self.pairs)]
            else:
                kept, self.sends = [p[0] for p in self.pairs], None
            self.pairs = list(zip(kept, flight))

    def result(self):
        total = jnp.concatenate([self.total(p, WIDE) for p in self.pairs], self.bits)
        return total.reshape((-1,) + self.shape)


def tick(chains, values=()):
    ready = [chain.ready() for chain in chains]
    ready, values = lax.optimization_barrier((ready, values))
    for chain, parts in zip(chains, ready):
        chain.launch(parts)
    return values


def shards(
    count,
    hidden_in,
    encoder_states,
    lengths,
    out_grad,
    attn_in,
    attn_out,
    fc_in,
    fc_out,
    gains,
    biases,
    ffn_bias,
):
    batch, length, width = hidden_in.shape
    rows = batch * length
    block = length // 2
    frame_rows = encoder_states.shape[1]
    share = gains.shape[1]
    ff_share = ffn_bias.shape[0]
    mats = ff_share // share

    small = jnp.concatenate([gains.reshape(-1), biases.reshape(-1), ffn_bias])
    small_count = small.shape[0]
    small_rows = -(-(small_count + 5) // 128)
    small_size = small_rows * 128
    small = jnp.pad(small, (0, small_size - small_count)).reshape(1, small_rows, 128)
    fc_in_mats = fc_in.reshape(share, count, mats, share).transpose(2, 0, 1, 3).reshape(mats, share, width)
    fc_out_mats = fc_out.reshape(mats, share, width)
    g_small = Gather(small, count, 1)
    g_self = Gather(jnp.concatenate([attn_in[0:3], attn_out[0:1]]), count)
    g_cross = Gather(jnp.concatenate([attn_in[3:4], attn_out[1:2], attn_in[4:6]]), count)
    g_ffn = Gather(jnp.concatenate([fc_in_mats, fc_out_mats]), count)

    core = own_bit(0).astype(jnp.int32).reshape(1)
    x = hidden_in.reshape(rows, width)
    frames = encoder_states.reshape(-1, width)
    valid = jnp.arange(length)[None, :, None] < lengths[:, None, None]
    grad = jnp.where(valid, out_grad, jnp.zeros_like(out_grad)).reshape(rows, width)

    tick([g_self, g_small])
    tick([g_self, g_small])
    tick([g_self, g_small, g_cross])
    tick([g_self, g_small, g_cross, g_ffn])
    tick([g_self, g_small, g_cross, g_ffn])
    small = g_small.result()[0].astype(jnp.float32).reshape(count, small_size)
    vec = small[:, : 13 * share].reshape(count, 13, share).transpose(1, 0, 2).reshape(13, width)
    vec = jnp.pad(vec, ((0, 3), (0, 0)))
    bias = small[:, 13 * share : small_count].reshape(count, mats, share)
    bias = bias.transpose(1, 0, 2).reshape(mats, 1, width)
    self_a, self_b = g_self.result()
    x = tick([g_cross], x)
    norm_one, query, key, value = qkv(x, vec, self_a, self_b, block)
    query, key, value = tick([g_ffn], (query, key, value))
    attended = attend(query, key, value, batch, True)
    mid, norm_two, square_self = mid_stage(lengths, attended, x, vec, self_b, batch, block)
    norm_two = tick([g_cross], norm_two)
    norm_two = tick([g_ffn], norm_two)
    cross_a, cross_b = g_cross.result()
    cross_q, cross_k, cross_v = cross_stage(norm_two, frames, vec, cross_a, cross_b, batch)
    cross_attended = attend(cross_q, cross_k, cross_v, batch, False)
    late, norm_three, square_cross = late_stage(lengths, cross_attended, mid, vec, cross_a, batch, block)
    norm_three = tick([g_ffn], norm_three)
    w_in, w_out = g_ffn.result()
    grad_norm, d_in, d_out, sums_ff, result, square_rest = ffn_stage(
        lengths, core, count, norm_three, grad, bias, w_in, w_out, None, late, vec, batch, length
    )
    s_ffn = Scatter([d_in, d_out], count)
    grad_norm = tick([s_ffn], grad_norm)
    grad_late, grad_cross, grad_cross_att, sums_late = late_back(
        grad_norm, late, grad, vec, cross_a, block
    )
    grad_cross_att = tick([s_ffn], grad_cross_att)
    grad_cq, grad_ck, grad_cv = attend_back(
        cross_q, cross_k, cross_v, grad_cross_att, batch, False
    )
    d_cross_a = weight_grads([(norm_two, grad_cq), (cross_attended, grad_cross)], core, count)
    d_cross_b = weight_grads([(frames, grad_ck), (frames, grad_cv)], core, count)
    s_cross = Scatter([d_cross_a, d_cross_b], count)
    grad_cq, grad_ck, grad_cv = tick([s_cross], (grad_cq, grad_ck, grad_cv))
    grad_mid, grad_self, grad_att, sums_mid = mid_back(
        grad_cq, cross_a, mid, grad_late, vec, self_b, block
    )
    grad_frames, sums_frames = frames_back(grad_ck, grad_cv, cross_b, frame_rows)
    grad_att, grad_frames = tick([s_cross, s_ffn], (grad_att, grad_frames))
    grad_q, grad_k, grad_v = attend_back(query, key, value, grad_att, batch, True)
    d_self_a = weight_grads([(norm_one, grad_q), (norm_one, grad_k)], core, count)
    d_self_b = weight_grads([(norm_one, grad_v), (attended, grad_self)], core, count)
    s_self = Scatter([d_self_a, d_self_b], count)
    grad_q, grad_k, grad_v = tick([s_self], (grad_q, grad_k, grad_v))
    grad_q, grad_k, grad_v = tick([s_cross, s_ffn], (grad_q, grad_k, grad_v))
    grad_q, grad_k, grad_v = tick([s_self], (grad_q, grad_k, grad_v))
    grad_in, sums_one = in_back(grad_q, grad_k, grad_v, self_a, self_b, x, grad_mid, vec, block)

    sums_one = tick([s_self, s_cross, s_ffn], sums_one)
    sum_rows = jnp.stack(
        [sums_one[0], sums_mid[0], sums_late[0]]
        + [sums_one[2], sums_one[3], sums_mid[2], sums_mid[3], sums_frames[0], sums_late[2], square_rest[2]]
        + [sums_one[1], sums_mid[1], sums_late[1]]
    )
    squares = jnp.stack([square_rest[0], square_self[0], square_cross[0], square_rest[1]])
    stats = jnp.concatenate([jnp.sum(squares, -1), jnp.sum(lengths).astype(WIDE)[None]])
    sums_ff = sums_ff.reshape(mats, count, share)
    sums = jnp.concatenate(
        [
            sum_rows.reshape(13, count, share).transpose(1, 0, 2).reshape(count, 13 * share),
            sums_ff.transpose(1, 0, 2).reshape(count, ff_share),
            jnp.broadcast_to(stats[None], (count, 5)),
        ],
        1,
    )
    sums = jnp.pad(sums, ((0, 0), (0, small_size - sums.shape[1])))
    s_small = Scatter([[sums.reshape(1, count * small_rows, 128)]], count)
    tick([s_small])
    tick([s_small])
    tick([s_small])
    tick([s_self, s_cross, s_small])
    tick([s_self, s_small])
    d_ffn = s_ffn.result()
    d_in_all, d_out_all = d_ffn[:mats], d_ffn[mats:]
    d_cross = s_cross.result()
    d_self = s_self.result()
    small = s_small.result().reshape(-1)
    stats = small[small_count : small_count + 5]
    rms = jnp.sqrt(stats[:4] / (stats[4] * width))
    return (
        result.reshape(hidden_in.shape),
        grad_in.reshape(hidden_in.shape),
        grad_frames.reshape(encoder_states.shape),
        jnp.concatenate([d_self[:3], d_cross[:1], d_cross[2:]]),
        jnp.concatenate([d_self[3:], d_cross[1:2]]),
        d_in_all.reshape(mats, share, count, share).transpose(1, 2, 0, 3).reshape(share, -1),
        d_out_all.reshape(ff_share, width),
        small[: 3 * share].reshape(3, share),
        small[3 * share : 13 * share].reshape(10, share),
        small[13 * share : small_count],
        rms,
    )


def solution(mesh):
    placed = (
        P("fsdp", None, None),
        P("fsdp", None, None),
        P("fsdp"),
        P("fsdp", None, None),
        P(None, "fsdp", None),
        P(None, "fsdp", None),
        P("fsdp", None),
        P("fsdp", None),
        P(None, "fsdp"),
        P(None, "fsdp"),
        P("fsdp"),
    )
    return jax.shard_map(
        functools.partial(shards, mesh.shape["fsdp"]),
        mesh=mesh,
        in_specs=placed,
        out_specs=(
            P("fsdp", None, None),
            P("fsdp", None, None),
            P("fsdp", None, None),
            P(None, "fsdp", None),
            P(None, "fsdp", None),
            P("fsdp", None),
            P("fsdp", None),
            P(None, "fsdp"),
            P(None, "fsdp"),
            P("fsdp"),
            P(),
        ),
        check_vma=False,
    )
```
